32 devices in a mesh: rows: 16 (over z, y, x), inner: 2 (over core).
Axes of the slice: x: 2, y: 2, z: 4, core: 2. Of those that a mesh axis runs over, the one named last changes fastest.
Arguments:
- r_tiles: bfloat16 [128, 16, 128, 128], P('rows', 'inner'), may hold values from -0.5 to 0.5
- r_cols: int32 [128, 16], P('rows', 'inner'), may hold values from 0 to 255, as said below
- a_tiles: bfloat16 [256, 7, 128, 128], P(('rows', 'inner')), may hold values from -6 to 6
- a_cols: int32 [256, 7], replicated, may hold values from 0 to 255, as said below
- c_cols: int32 [128, 8], P('rows'), may hold values from -1 to 255, as said below
- c_counts: int32 [128], P('rows'), may hold values from 4 to 8, as said below
Outputs:
- c_tiles: bfloat16 [128, 8, 128, 128], P('rows', 'inner')
- row_offsets: int32 [128], P('rows')
The draws below stay inside these ranges and needn't reach their ends.
Inputs may be any that keep to these rules, and one draw needn't show every extreme that they name: `r_cols`: the slots g * 8 to (g + 1) * 8 - 1 of block row c name distinct fine block rows k with (k // 8) % 2 == g and k // 16 within one of c // 8. `a_cols`: row k names 7 distinct fine block columns, the first of them k. `c_cols`: the first c_counts[c] entries of row c are distinct block columns, the others are -1. `c_counts`: each aligned group of 8 block rows has one with 8 live slots.
All inputs are finite; a program needn't handle non-finite values.
Results may differ from the reference program's by a relative error of at most 0.001.
Values may be sent and summed in bfloat16 or wider, within the bound.
A program may use at most 64 MiB of HBM per device.

```python
import jax
import jax.numpy as jnp
from jax import lax

TB = 128
RB_DEV = 8
SR_DEV = 8
KA_DEV = 8
SA = 7
CAP = 8
NCB = 128
SR = 16
NK = 256
N_ROWS = 16
N_INNER = 2


def pattern(key):
    span = 3 * KA_DEV
    coarse_owner = jnp.arange(NCB, dtype=jnp.int32) // RB_DEV
    candidate = jnp.arange(span, dtype=jnp.int32)
    shift_rows = candidate // KA_DEV - 1
    neighbour = coarse_owner[:, None, None] + shift_rows[None, None, :]
    usable = (neighbour >= 0) & (neighbour < N_ROWS)
    group_ids = jnp.arange(N_INNER, dtype=jnp.int32)
    noise_r = jax.random.randint(jax.random.fold_in(key, 101), (NCB, N_INNER, span), 0, 65536)
    scores = noise_r * span + candidate[None, None, :]
    scores = jnp.where((candidate == 0)[None, None, :] & usable, -2, scores)
    scores = jnp.where((candidate == 2 * KA_DEV)[None, None, :] & usable, -1, scores)
    scores = jnp.where(usable, scores, 2 ** 30)
    chosen_q = jnp.argsort(scores, axis=-1)[:, :, :SR_DEV].astype(jnp.int32)
    chosen_shift = chosen_q // KA_DEV - 1
    chosen_local = chosen_q % KA_DEV
    fine_rows = ((coarse_owner[:, None, None] + chosen_shift) * N_INNER + group_ids[None, :, None]) * KA_DEV + chosen_local
    r_columns = fine_rows.reshape(NCB, SR).astype(jnp.int32)
    first_stride = jax.random.randint(jax.random.fold_in(key, 606), (), 9, 17).astype(jnp.int32)
    second_raw = jax.random.randint(jax.random.fold_in(key, 707), (), 9, 17).astype(jnp.int32)
    second_stride = jnp.clip(second_raw, 2, (NK // 2 - 1) // first_stride)
    plane_stride = first_stride * second_stride
    stencil = jnp.stack([jnp.int32(1), jnp.int32(-1), first_stride, -first_stride, plane_stride, -plane_stride]).astype(jnp.int32)
    noise_a = jax.random.randint(jax.random.fold_in(key, 202), (NK, 6), 0, 65536)
    order_ids = jnp.argsort(noise_a * 6 + jnp.arange(6, dtype=jnp.int32)[None, :], axis=-1)[:, :SA - 1]
    fine_ids = jnp.arange(NK, dtype=jnp.int32)
    others = jnp.mod(fine_ids[:, None] + stencil[order_ids], NK)
    a_columns = jnp.concatenate([fine_ids[:, None], others], axis=1).astype(jnp.int32)
    base_counts = jax.random.randint(jax.random.fold_in(key, 303), (NCB,), CAP // 2, CAP + 1)
    full_at = jax.random.randint(jax.random.fold_in(key, 404), (N_ROWS,), 0, RB_DEV)
    is_full = jnp.arange(NCB, dtype=jnp.int32) % RB_DEV == jnp.repeat(full_at, RB_DEV)
    counts = jnp.where(is_full, CAP, base_counts).astype(jnp.int32)
    product_columns = a_columns[r_columns]
    slot_ids = jnp.arange(SR, dtype=jnp.int32)
    favoured = ((slot_ids // SR_DEV)[None, :] == (jnp.arange(NCB, dtype=jnp.int32) % N_INNER)[:, None]) & (slot_ids % SR_DEV < 2)[None, :]
    favoured = favoured[:, :, None] & (jnp.arange(SA, dtype=jnp.int32) == 0)[None, None, :]
    noise_c = jax.random.randint(jax.random.fold_in(key, 505), (NCB, SR, SA), 0, 4096)
    weights = jnp.where(favoured, 0, noise_c + 1)
    packed = (product_columns * 8192 + weights).reshape(NCB, SR * SA)
    ordered = jnp.sort(packed, axis=-1)
    values = ordered // 8192
    ranks = ordered % 8192
    leading = jnp.concatenate([jnp.ones((NCB, 1), dtype=bool), values[:, 1:] != values[:, :-1]], axis=1)
    select_key = jnp.where(leading, ranks * (SR * SA) + jnp.arange(SR * SA, dtype=jnp.int32)[None, :], 2 ** 30)
    selected = jnp.argsort(select_key, axis=-1)[:, :CAP]
    taken = jnp.take_along_axis(values, selected, axis=1)
    c_columns = jnp.where(jnp.arange(CAP, dtype=jnp.int32)[None, :] < counts[:, None], taken, -1).astype(jnp.int32)
    return (r_columns, a_columns, c_columns, counts)


def draw_r_cols(key, part):
    return pattern(key)[0]


def draw_a_cols(key, part):
    return pattern(key)[1]


def draw_c_cols(key, part):
    return pattern(key)[2]


def draw_c_counts(key, part):
    return pattern(key)[3]


def block_levels(own_key, dims, split, smallest, top_value):
    factor_of = 1.0
    for position, parts in split:
        steps = jax.random.uniform(jax.random.fold_in(jax.random.fold_in(own_key, 6), position), (parts,), jnp.float32, smallest / len(split), top_value / len(split))
        factor_of = factor_of * jnp.repeat(jnp.exp(steps), dims[position] // parts).reshape((-1,) + (1,) * (len(dims) - 1 - position))
    return factor_of


def scatter_about(rng, dims, spread, most, split=(), kind=jnp.bfloat16):
    loudness = block_levels(rng, dims, split, -0.22, 0.18) if split else 1.0
    drawn = jax.random.normal(rng, dims, jnp.float32) * spread * loudness
    return jnp.minimum(jnp.maximum(drawn, -most), most).astype(kind)


def setup_inputs(seed: int = 0) -> dict:
    streams_of = jax.random.split(jax.random.key(seed), 7)
    r_tiles = scatter_about(streams_of[0], (NCB, SR, TB, TB), TB ** -0.5, 0.5, ((0, 16), (1, 2)))
    r_cols = draw_r_cols(jax.random.fold_in(streams_of[6], 71), 0)
    a_tiles = scatter_about(streams_of[2], (NK, SA, TB, TB), 1.0, 6.0, ((0, 32),))
    a_cols = draw_a_cols(jax.random.fold_in(streams_of[6], 71), 0)
    c_cols = draw_c_cols(jax.random.fold_in(streams_of[6], 71), 0)
    c_counts = draw_c_counts(jax.random.fold_in(streams_of[6], 71), 0)
    return dict(r_tiles=r_tiles, r_cols=r_cols, a_tiles=a_tiles, a_cols=a_cols, c_cols=c_cols, c_counts=c_counts)


def reference(r_tiles, r_cols, a_tiles, a_cols, c_cols, c_counts):
    def one_row(row_data):
        row_tiles, columns, wanted = row_data
        picked = a_tiles[columns].astype(jnp.float32)
        products = jnp.einsum("jxy,jtyz->jtxz", row_tiles.astype(jnp.float32), picked, precision=lax.Precision.HIGHEST)
        matches = (wanted[:, None, None] == a_cols[columns][None]).astype(jnp.float32)
        summed = jnp.einsum("sjt,jtxz->sxz", matches, products, precision=lax.Precision.HIGHEST)
        return summed.astype(jnp.bfloat16)

    c_tiles = lax.map(one_row, (r_tiles, r_cols, c_cols))
    row_offsets = (jnp.cumsum(c_counts) - c_counts).astype(jnp.int32)
    return c_tiles, row_offsets
```

```python
import functools

import jax
import jax.numpy as jnp
from jax import lax
from jax.experimental import pallas as pl
from jax.experimental.pallas import tpu as pltpu
from jax.sharding import PartitionSpec as P

MESH = pl.DeviceIdType.MESH
BATCH = 4


def plan_kernel(
    dims, r_cols_ref, c_cols_ref, counts_ref, columns_ref, code_ref, plan_ref,
    meta_ref, gathered, needs, send_sem, recv_sem,
):
    rows, groups, local_rows, op_slots, r_slots, cap, half = dims
    width = 2 * half
    count = rows * groups
    tiles = local_rows * op_slots
    row = lax.axis_index("rows")
    group = lax.axis_index("inner")
    me = row * groups + group

    barrier = pltpu.get_barrier_semaphore()

    def place(step):
        other = lax.rem(me + step, count)
        return (other // groups, lax.rem(other, groups))

    def greet(step, carry):
        pl.semaphore_signal(barrier, inc=1, device_id=place(step), device_id_type=MESH)
        return carry

    lax.fori_loop(1, count, greet, 0)
    row_count = r_cols_ref.shape[0]
    live = r_slots + cap
    lanes = lax.broadcasted_iota(jnp.int32, (row_count, width), 1)
    above = lax.broadcasted_iota(jnp.int32, (row_count, width), 0)
    small = (row_count, row_count)
    diagonal = lax.broadcasted_iota(jnp.int32, small, 0) == lax.broadcasted_iota(jnp.int32, small, 1)
    spread_counts = jnp.broadcast_to(counts_ref[...], small)
    own_counts = jnp.sum(jnp.where(diagonal, spread_counts, 0), axis=1, keepdims=True)
    meta_ref[...] = jnp.full(meta_ref.shape, -9, jnp.int32)
    meta_ref[:, 0:r_slots] = r_cols_ref[...]
    meta_ref[:, r_slots:live] = c_cols_ref[...]
    meta_ref[:, live : live + 1] = own_counts
    gathered[me] = meta_ref[...]
    pl.semaphore_wait(barrier, count - 1)

    def post(step, carry):
        pltpu.make_async_remote_copy(
            src_ref=meta_ref,
            dst_ref=gathered.at[me],
            send_sem=send_sem,
            recv_sem=recv_sem,
            device_id=place(step),
            device_id_type=MESH,
        ).start()
        return carry

    lax.fori_loop(1, count, post, 0)
    everyone = gathered.at[pl.ds(0, count - 1)]
    pltpu.make_async_copy(everyone, everyone, send_sem).wait()
    pltpu.make_async_copy(everyone, everyone, recv_sem).wait()

    def matches(block, columns, fine_rows):
        named = fine_rows == block[:, 0:1]
        for j in range(1, r_slots):
            named = named | (fine_rows == block[:, j : j + 1])
        slot = jnp.full((row_count, width), -1, jnp.int32)
        for s in range(cap):
            slot = jnp.where(columns == block[:, r_slots + s : r_slots + s + 1], s, slot)
        return jnp.where(named, slot, -1)

    shift = jnp.where(lanes < half, -groups, groups) * local_rows
    tile = jnp.where(lanes < half, lanes, lanes - half)
    lane_rows = jnp.where(tile < tiles, shift + tile // op_slots, -(1 << 24))
    low_lanes = lanes[0:1] < half

    def near_matches(device):
        before = columns_ref[pl.ds(jnp.maximum(device - groups, 0), 1), :]
        after = columns_ref[pl.ds(jnp.minimum(device + groups, count - 1), 1), :]
        columns = jnp.where(low_lanes, before, after)
        return matches(gathered[device], columns, lane_rows + device * local_rows)

    def wanted(found):
        return jnp.max((found >= 0).astype(jnp.int32), axis=0, keepdims=True)

    def gather_needs(device, carry):
        needs[pl.ds(device, 1), :] = wanted(near_matches(device))
        return carry

    lax.fori_loop(0, count, gather_needs, 0, unroll=4)
    every = needs[...]
    low_side = lax.broadcasted_iota(jnp.int32, every.shape, 1) < half
    low = jnp.sum(jnp.where(low_side, every, 0), axis=1, keepdims=True)
    high = jnp.sum(jnp.where(low_side, 0, every), axis=1, keepdims=True)
    most = jnp.max(jnp.maximum(low, high), axis=0, keepdims=True)

    down = lax.broadcasted_iota(jnp.int32, (width, width), 0)
    across = lax.broadcasted_iota(jnp.int32, (width, width), 1)
    same = (down < half) == (across < half)

    def ranks(need):
        spread = jnp.broadcast_to(need, (width, width))
        column = jnp.sum(jnp.where(down == across, spread, 0), axis=1, keepdims=True)
        before = jnp.sum(jnp.where((across < down) & same, spread, 0), axis=1, keepdims=True)
        along = jnp.sum(
            jnp.where((down < across) & same, jnp.broadcast_to(column, (width, width)), 0),
            axis=0,
            keepdims=True,
        )
        return column, before, along

    def send_list(device, high):
        column, before, _ = ranks(needs[pl.ds(device, 1), :])
        first = half if high else 0
        mine = (down >= half) if high else (down < half)
        chosen = mine & (column > 0) & (before == across)
        return jnp.sum(jnp.where(chosen, down - first, 0), axis=0, keepdims=True)

    left = jnp.maximum(row - 1, 0) * groups + group
    right = jnp.minimum(row + 1, rows - 1) * groups + group
    plan_ref[0:1, :] = send_list(left, True)
    plan_ref[1:2, :] = send_list(right, False)

    found = near_matches(me)
    _, _, along = ranks(wanted(found))
    slot_at = along + jnp.where(lanes[0:1] < half, tiles, 2 * tiles)
    code_ref[:, 0:width] = jnp.where(found >= 0, found + cap * slot_at, -1)
    fine = me * local_rows + jnp.where(lanes < tiles, lanes // op_slots, 0)
    fine = jnp.where(lanes < tiles, fine, -5)
    found = matches(gathered[me], columns_ref[pl.ds(me, 1), :], fine)
    code_ref[:, width:] = jnp.where(found >= 0, found + cap * lanes, -1)

    def earlier(index, total):
        block = gathered[index * groups]
        return total + jnp.sum(block[:, live : live + 1], axis=0, keepdims=True)

    first = lax.fori_loop(0, row, earlier, jnp.zeros((1, 1), jnp.int32))
    counts = jnp.broadcast_to(own_counts, (row_count, width))
    inner_sum = jnp.sum(jnp.where(above < lanes, counts, 0), axis=0, keepdims=True)
    plan_ref[2:3, :] = inner_sum + first
    level = jnp.zeros((1, 1), jnp.int32)
    for size in sizes_for(tiles)[:-1]:
        level = level + (most > size).astype(jnp.int32)
    plan_ref[3:4, :] = jnp.broadcast_to(level, (1, width))


def halo_kernel(rows, size, plan_ref, a_ref, out_ref, packed, send_sems, recv_sems):
    row = lax.axis_index("rows")
    group = lax.axis_index("inner")
    barrier = pltpu.get_barrier_semaphore()
    has_left = row > 0
    has_right = row < rows - 1

    @pl.when(has_left)
    def _():
        pl.semaphore_signal(barrier, inc=1, device_id=(row - 1, group), device_id_type=MESH)

    @pl.when(has_right)
    def _():
        pl.semaphore_signal(barrier, inc=1, device_id=(row + 1, group), device_id_type=MESH)

    def pack(index, carry):
        packed[0, index] = a_ref[plan_ref[0, index]]
        packed[1, index] = a_ref[plan_ref[1, index]]
        return carry

    lax.fori_loop(0, size, pack, 0, unroll=2)

    pl.semaphore_wait(barrier, has_left.astype(jnp.int32) + has_right.astype(jnp.int32))

    def copy(side, other):
        return pltpu.make_async_remote_copy(
            src_ref=packed.at[side],
            dst_ref=out_ref.at[1 - side, pl.ds(0, size)],
            send_sem=send_sems.at[side],
            recv_sem=recv_sems.at[1 - side],
            device_id=(other, group),
            device_id_type=MESH,
        )

    @pl.when(has_left)
    def _():
        copy(0, row - 1).start()

    @pl.when(has_right)
    def _():
        copy(1, row + 1).start()

    @pl.when(has_left)
    def _():
        copy(0, row - 1).wait_send()
        copy(1, row - 1).wait_recv()

    @pl.when(has_right)
    def _():
        copy(1, row + 1).wait_send()
        copy(0, row + 1).wait_recv()


def product_kernel(dims, code_ref, cols_ref, r_ref, a_ref, halo_ref, out_ref, tiles_ref, jobs, sems):
    rows, groups, local_rows, op_slots, r_slots, cap, half = dims
    width = 2 * half
    tiles = local_rows * op_slots
    row_count = cols_ref.shape[0]
    own_cap = cap // groups
    row = lax.axis_index("rows")
    group = lax.axis_index("inner")
    own = pltpu.make_async_copy(a_ref, tiles_ref.at[pl.ds(0, tiles)], sems.at[0])
    near = pltpu.make_async_copy(halo_ref, tiles_ref.at[pl.ds(tiles, 2 * tiles)], sems.at[1])
    own.start()
    near.start()
    last = groups * row_count * own_cap
    scale = 1 << (3 * tiles * cap - 1).bit_length()

    def clear(index, carry):
        out_ref[index] = jnp.zeros(out_ref.shape[1:], jnp.float32)
        return carry

    lax.fori_loop(0, last, clear, 0, unroll=4)

    def list_row(c, found):
        def list_slot(j, found):
            fine = cols_ref[c, j]
            side = fine // (local_rows * groups) - row
            base = jnp.where(side == 0, width, jnp.where(side < 0, 0, half))
            base = base + lax.rem(fine, local_rows) * op_slots
            for t in range(op_slots):
                code = code_ref[c, base + t]
                jobs[found] = (c * r_slots + j) * scale + code
                found = found + (code >= 0).astype(jnp.int32)
            return found

        return lax.fori_loop(0, r_slots, list_slot, found)

    found = lax.fori_loop(0, row_count, list_row, jnp.int32(0))
    for extra in range(BATCH):
        jobs[found + extra] = -1
    own.wait()
    near.wait()

    def batch(step, carry):
        results = []
        targets = []
        for extra in range(BATCH):
            job = jobs[step * BATCH + extra]
            valid = job >= 0
            job = jnp.maximum(job, 0)
            pair = job // scale
            code = lax.rem(job, scale)
            slot = lax.rem(code, cap)
            ahead = lax.rem(slot // own_cap + groups - group, groups)
            target = (ahead * row_count + pair // r_slots) * own_cap + lax.rem(slot, own_cap)
            targets.append(jnp.where(valid, target, last))
            results.append(
                jnp.dot(
                    r_ref[pair],
                    tiles_ref[code // cap],
                    preferred_element_type=jnp.float32,
                )
            )
        for extra in range(BATCH):
            target = targets[extra]
            out_ref[target] = out_ref[target] + results[extra]
        return carry

    lax.fori_loop(0, (found + BATCH - 1) // BATCH, batch, 0)


def sum_kernel(groups, own, part_ref, landed, send_sems, recv_sems):
    row = lax.axis_index("rows")
    group = lax.axis_index("inner")
    barrier = pltpu.get_barrier_semaphore()
    for ahead in range(1, groups):
        pl.semaphore_signal(
            barrier, inc=1, device_id=(row, lax.rem(group + ahead, groups)), device_id_type=MESH
        )
    pl.semaphore_wait(barrier, groups - 1)
    copies = []
    for ahead in range(1, groups):
        copy = pltpu.make_async_remote_copy(
            src_ref=part_ref.at[pl.ds(ahead * own, own)],
            dst_ref=landed.at[ahead - 1],
            send_sem=send_sems.at[ahead - 1],
            recv_sem=recv_sems.at[ahead - 1],
            device_id=(row, lax.rem(group + ahead, groups)),
            device_id_type=MESH,
        )
        copy.start()
        copies.append(copy)
    for copy in copies:
        copy.wait()


def sizes_for(tiles):
    steps = [16, 18, 20, 21, 22, 23, 24, 25, 26, 27, 28, 29, 30, 32, 36, 42]
    return [size for size in steps if size < tiles] + [tiles]


def plain_body(rows, groups, r_tiles, r_cols, a_tiles, a_cols, c_cols, c_counts):
    local_rows, op_slots, tile, _ = a_tiles.shape
    row_count, r_slots = r_tiles.shape[:2]
    cap = c_cols.shape[1]
    tiles = local_rows * op_slots
    half = -(-tiles // 64) * 64
    width = 2 * half
    count = rows * groups
    own_cap = cap // groups
    dims = (rows, groups, local_rows, op_slots, r_slots, cap, half)
    vmem = pl.BlockSpec(memory_space=pltpu.VMEM)
    smem = pl.BlockSpec(memory_space=pltpu.SMEM)
    anywhere = pl.BlockSpec(memory_space=pl.ANY)

    flat = a_cols.reshape(count, tiles)
    flat = jnp.pad(flat, ((0, 0), (0, half - tiles)), constant_values=-2)
    columns = jnp.concatenate([flat, flat], axis=1)

    code, plan = pl.pallas_call(
        functools.partial(plan_kernel, dims),
        out_shape=(
            jax.ShapeDtypeStruct((row_count, 2 * width), jnp.int32),
            jax.ShapeDtypeStruct((8, width), jnp.int32),
        ),
        in_specs=[vmem] * 4,
        out_specs=(vmem, vmem),
        scratch_shapes=[
            pltpu.VMEM((row_count, width), jnp.int32),
            pltpu.VMEM((count, row_count, width), jnp.int32),
            pltpu.VMEM((count, width), jnp.int32),
            pltpu.SemaphoreType.DMA,
            pltpu.SemaphoreType.DMA,
        ],
        compiler_params=pltpu.CompilerParams(collective_id=0, has_side_effects=True),
        name="plan",
    )(r_cols, c_cols, c_counts[None, :], columns)

    flat_a = a_tiles.reshape(tiles, tile, tile)
    sizes = sizes_for(tiles)

    def exchange(number, size, plan, flat_a):
        return pl.pallas_call(
            functools.partial(halo_kernel, rows, size),
            out_shape=jax.ShapeDtypeStruct((2, tiles, tile, tile), a_tiles.dtype),
            in_specs=[smem, vmem],
            out_specs=anywhere,
            scratch_shapes=[
                pltpu.VMEM((2, size, tile, tile), a_tiles.dtype),
                pltpu.SemaphoreType.DMA((2,)),
                pltpu.SemaphoreType.DMA((2,)),
            ],
            compiler_params=pltpu.CompilerParams(collective_id=number + 2, has_side_effects=True),
            name=f"halo{size}",
        )(plan, flat_a)

    halo = lax.switch(
        plan[3, 0],
        [functools.partial(exchange, number, size) for number, size in enumerate(sizes)],
        plan,
        flat_a,
    )

    slots = row_count * r_slots * op_slots + BATCH
    partial_value = pl.pallas_call(
        functools.partial(product_kernel, dims),
        out_shape=jax.ShapeDtypeStruct((row_count * cap + 1, tile, tile), jnp.float32),
        in_specs=[smem, smem, vmem, anywhere, anywhere],
        out_specs=vmem,
        scratch_shapes=[
            pltpu.VMEM((3 * tiles, tile, tile), a_tiles.dtype),
            pltpu.SMEM((slots,), jnp.int32),
            pltpu.SemaphoreType.DMA((2,)),
        ],
        name="products",
    )(
        code,
        r_cols,
        r_tiles.reshape(row_count * r_slots, tile, tile),
        flat_a,
        halo.reshape(2 * tiles, tile, tile),
    )

    own_count = row_count * own_cap
    landed = pl.pallas_call(
        functools.partial(sum_kernel, groups, own_count),
        out_shape=jax.ShapeDtypeStruct((groups - 1, own_count, tile, tile), jnp.float32),
        in_specs=[anywhere],
        out_specs=anywhere,
        scratch_shapes=[
            pltpu.SemaphoreType.DMA((groups - 1,)),
            pltpu.SemaphoreType.DMA((groups - 1,)),
        ],
        compiler_params=pltpu.CompilerParams(collective_id=1, has_side_effects=True),
        name="sums",
    )(partial_value)
    c_tiles = partial_value[:own_count]
    for ahead in range(groups - 1):
        c_tiles = c_tiles + landed[ahead]
    c_tiles = c_tiles.astype(jnp.bfloat16)
    return (c_tiles.reshape(row_count, own_cap, tile, tile), plan[2, :row_count])

NEAR_SLOTS = 30
FAR_SLOTS = 21
CHUNK = 3
REMOTE = 1 << 14


def fused_kernel(
    dims, r_cols_ref, c_cols_ref, counts_ref, columns_ref, a_ref, r_ref,
    out_ref, offsets_ref, flag_ref,
    meta, gathered, close, pair_a, pair_r, packed, landed, sums, done, tables, codes, picks,
    local_sems, gather_sems, close_sems, pair_sems, near_sems, near_pair_sems, far_sems,
    far_pair_sems, table_sems, out_sems,
):
    (rows, groups, local_rows, op_slots, r_slots, cap, width, near_slots, far_slots, chunk) = dims
    count = rows * groups
    pairs = groups // 2
    tiles = local_rows * op_slots
    span = 2 * local_rows
    own_cap = cap // groups
    half_cap = cap // 2
    row_count = r_cols_ref.shape[0]
    live = r_slots + cap
    near_chunks = near_slots // chunk
    far_chunks = far_slots // chunk
    far_base = 2 * near_slots
    zero_near = 2 * (near_slots + far_slots)
    zero_own = 2 * tiles

    row = lax.axis_index("rows")
    group = lax.axis_index("inner")
    me = row * groups + group
    part = lax.rem(group, 2)
    first_group = group - part
    mate = first_group + 1 - part
    odd = lax.rem(row, 2)
    near = row + 1 - 2 * odd
    far = row - 1 + 2 * odd
    has_far = (far >= 0) & (far < rows)
    onward = near + 1 - 2 * odd
    has_onward = (onward >= 0) & (onward < rows)

    def remote(src, dst, send_sem, recv_sem, place):
        return pltpu.make_async_remote_copy(
            src_ref=src, dst_ref=dst, send_sem=send_sem, recv_sem=recv_sem,
            device_id=place, device_id_type=MESH,
        )

    own_a = pltpu.make_async_copy(
        a_ref, pair_a.at[pl.ds(part * tiles, tiles)], local_sems.at[0]
    )
    own_r = pltpu.make_async_copy(r_ref, pair_r.at[part], local_sems.at[1])
    own_a.start()
    own_r.start()

    barrier = pltpu.get_barrier_semaphore()

    def place(step):
        other = lax.rem(me + step, count)
        return (other // groups, lax.rem(other, groups))

    def greet(step, carry):
        pl.semaphore_signal(barrier, inc=1, device_id=place(step), device_id_type=MESH)
        return carry

    lax.fori_loop(1, count, greet, 0)

    small = (row_count, row_count)
    diagonal = lax.broadcasted_iota(jnp.int32, small, 0) == lax.broadcasted_iota(jnp.int32, small, 1)
    spread_counts = jnp.broadcast_to(counts_ref[...], small)
    own_counts = jnp.sum(jnp.where(diagonal, spread_counts, 0), axis=1, keepdims=True)
    meta[...] = jnp.full(meta.shape, -9, jnp.int32)
    meta[:, 0:r_slots] = r_cols_ref[...]
    meta[:, r_slots:live] = c_cols_ref[...]
    meta[:, live : live + 1] = own_counts
    gathered[me] = meta[...]
    pair_a[zero_own] = jnp.zeros(pair_a.shape[1:], pair_a.dtype)
    landed[zero_near] = jnp.zeros(landed.shape[1:], landed.dtype)

    pl.semaphore_wait(barrier, count - 1)

    mate_place = (row, mate)

    def to_close(slot, place):
        return remote(meta, close.at[slot], close_sems.at[0, slot], close_sems.at[1, slot], place)

    def start_close(target, first):
        for core in range(2):
            pltpu.make_async_remote_copy(
                src_ref=meta, dst_ref=close.at[first + part],
                send_sem=close_sems.at[0, first + core], recv_sem=close_sems.at[1, first + part],
                device_id=(target, first_group + core), device_id_type=MESH,
            ).start()

    def wait_close_recv(first):
        for core in range(2):
            to_close(first + core, mate_place).wait_recv()

    def wait_close_send(first):
        for core in range(2):
            to_close(first + core, mate_place).wait_send()

    start_close(near, 0)

    @pl.when(has_far)
    def _():
        start_close(far, 2)

    mate_a = remote(
        a_ref, pair_a.at[pl.ds(part * tiles, tiles)], pair_sems.at[0, 0], pair_sems.at[1, 0], mate_place
    )
    mate_a.start()

    def post(step, carry):
        remote(meta, gathered.at[me], gather_sems.at[0], gather_sems.at[1], place(step)).start()
        return carry

    lax.fori_loop(1, count, post, 0)
    mate_r = remote(r_ref, pair_r.at[part], pair_sems.at[0, 1], pair_sems.at[1, 1], mate_place)
    mate_r.start()

    lanes = lax.broadcasted_iota(jnp.int32, (1, width), 1)
    deep = lax.broadcasted_iota(jnp.int32, (op_slots, width), 0)
    wide = lax.broadcasted_iota(jnp.int32, (op_slots, width), 1)
    real = lanes < op_slots * span
    lane_fine = jnp.where(real, lax.rem(lanes, span), -(1 << 24))
    lane_core = lax.rem(lanes, span) // local_rows
    lane_tile = lane_core * tiles + lax.rem(lanes, local_rows) * op_slots + lanes // span

    def pair_columns(which_row):
        return pair_columns_at((which_row * groups + first_group) * local_rows)

    def pair_columns_at(start):
        block = start // 128
        values = columns_ref[:, pl.ds(pl.multiple_of(block * 128, 128), 128)]
        if width > 128:
            values = jnp.concatenate([values] * (width // 128), axis=1)
        offset = start - block * 128
        total = jnp.zeros((1, width), jnp.int32)
        for t in range(op_slots):
            moved = pltpu.roll(values[t : t + 1, :], lax.rem(t * span - offset + 128 * width, width), 1)
            total = jnp.where(lanes // span == t, moved, total)
        return jnp.where(real, total, -2)

    def pair_fine(which_row):
        return lane_fine + (which_row * groups + first_group) * local_rows

    def need_of(meta_low, meta_high, columns, fine):
        named = fine == meta_low[:, 0:1]
        for j in range(1, r_slots):
            named = named | (fine == meta_low[:, j : j + 1])
        for j in range(r_slots):
            named = named | (fine == meta_high[:, j : j + 1])
        wanted = columns == meta_low[:, r_slots : r_slots + 1]
        for s in range(1, cap):
            wanted = wanted | (columns == meta_low[:, r_slots + s : r_slots + s + 1])
        return jnp.max((named & wanted).astype(jnp.int32), axis=0, keepdims=True)

    def before(need):
        total = need
        step = 1
        while step < width:
            total = total + jnp.where(lanes >= step, pltpu.roll(total, step, 1), 0)
            step *= 2
        return total - need

    def list_places(need_far, need_near):
        only = need_near * (1 - need_far)
        first = before(need_far)
        second = before(only) + jnp.sum(need_far, axis=1, keepdims=True)
        return jnp.where(need_far > 0, first, jnp.where(only > 0, second, -1))

    own_columns = pair_columns(row)
    own_fine = pair_fine(row)
    wait_close_recv(0)

    @pl.when(has_far)
    def _():
        wait_close_recv(2)

    @pl.when(jnp.logical_not(has_far))
    def _():
        close[2] = jnp.full(close.shape[1:], -9, jnp.int32)
        close[3] = jnp.full(close.shape[1:], -9, jnp.int32)

    need_near = need_of(close[0], close[1], own_columns, own_fine)
    need_far = need_of(close[2], close[3], own_columns, own_fine)
    places = list_places(need_far, need_near)
    pick_rows = -(-near_slots // 8) * 8
    slot_down = lax.broadcasted_iota(jnp.int32, (pick_rows, width), 0)
    chosen = jnp.broadcast_to(places, (pick_rows, width)) == 2 * slot_down + part
    picked = jnp.sum(
        jnp.where(chosen, jnp.broadcast_to(lane_tile, (pick_rows, width)), 0), axis=1, keepdims=True
    )
    across = lax.broadcasted_iota(jnp.int32, (pick_rows, width), 1)
    pick_row = jnp.sum(
        jnp.where(slot_down == across, jnp.broadcast_to(picked, (pick_rows, width)), 0),
        axis=0, keepdims=True,
    )
    tables[0:8, :] = jnp.broadcast_to(pick_row, (8, width))
    pick_copy = pltpu.make_async_copy(tables.at[pl.ds(0, 8)], picks, table_sems.at[0])
    pick_copy.start()
    own_a.wait()
    mate_a.wait_recv()
    pick_copy.wait()

    def near_copy(index):
        return remote(
            packed.at[pl.ds(index * chunk, chunk)],
            landed.at[pl.ds(part * near_slots + index * chunk, chunk)],
            near_sems.at[0, index], near_sems.at[1, index], (near, group),
        )

    def pack(index):
        for extra in range(chunk):
            packed[index * chunk + extra] = pair_a[picks[0, index * chunk + extra]]

    pack(0)
    for index in range(near_chunks):
        if index + 1 < near_chunks:
            pack(index + 1)
        near_copy(index).start()

    everyone = gathered.at[pl.ds(0, count - 1)]
    gather_all = pltpu.make_async_copy(everyone, everyone, gather_sems.at[1])
    gather_all.wait()

    def gathered_pair(which_row):
        safe = jnp.clip(which_row, 0, rows - 1)
        base = safe * groups + first_group
        return gathered[base], gathered[base + 1]

    my_low, my_high = gathered_pair(row)
    near_columns = pair_columns(near)
    near_fine = pair_fine(near)
    far_row = jnp.clip(far, 0, rows - 1)
    far_columns = pair_columns(far_row)
    far_fine = jnp.where(has_far, pair_fine(far_row), -(1 << 24))
    past_low, past_high = gathered_pair(onward)
    past = need_of(past_low, past_high, near_columns, near_fine)
    past = jnp.where(has_onward, past, 0)
    near_places = list_places(past, need_of(my_low, my_high, near_columns, near_fine))
    far_need = need_of(my_low, my_high, far_columns, far_fine)
    far_places = jnp.where(far_need > 0, before(far_need), -1)

    def landing(places, slots, base):
        fits = (places >= 0) & (places < 2 * slots)
        at = base + lax.rem(places, 2) * slots + places // 2
        return jnp.where(fits, REMOTE + at, -1)

    near_at = landing(near_places, near_slots, 0)
    far_at = landing(far_places, far_slots, far_base)

    above = (row_count, width)
    table_lanes = lax.broadcasted_iota(jnp.int32, above, 1)
    own_at, near_at, far_at = [jnp.broadcast_to(x, above) for x in (lane_tile, near_at, far_at)]
    slot_own, slot_near, slot_far = [], [], []
    for index in range(half_cap):
        even = (2 * (index // own_cap)) * own_cap + index % own_cap
        low = my_low[:, r_slots + even : r_slots + even + 1]
        high = my_low[:, r_slots + even + own_cap : r_slots + even + own_cap + 1]
        column = jnp.where(part == 0, low, high)
        slot_own.append(jnp.where(own_columns == column, own_at, -1))
        slot_near.append(jnp.where(near_columns == column, near_at, -1))
        slot_far.append(jnp.where(far_columns == column, far_at, -1))
    code = jnp.full(above, -1, jnp.int32)
    for j in range(2 * r_slots):
        block = my_low if j < r_slots else my_high
        named = block[:, j % r_slots : j % r_slots + 1]
        in_own = own_fine == named
        in_near = near_fine == named
        in_far = far_fine == named
        for index in range(half_cap):
            found = jnp.where(in_own, slot_own[index], -1)
            found = jnp.where(in_near, slot_near[index], found)
            found = jnp.where(in_far, slot_far[index], found)
            best = jnp.max(found, axis=1, keepdims=True)
            code = jnp.where(table_lanes == index * 2 * r_slots + j, best, code)
    tables[0:row_count, :] = jnp.where((code >= 0) & (code < REMOTE), code, zero_own)
    tables[row_count : 2 * row_count, :] = jnp.where(code >= REMOTE, code - REMOTE, zero_near)
    code_copy = pltpu.make_async_copy(tables, codes, table_sems.at[1])
    code_copy.start()

    def earlier(index, total):
        block = gathered[index * groups]
        return total + jnp.sum(block[:, live : live + 1], axis=0, keepdims=True)

    first = lax.fori_loop(0, row, earlier, jnp.zeros((1, 1), jnp.int32))
    counts = jnp.broadcast_to(own_counts, small)
    inner_sum = jnp.sum(
        jnp.where(
            lax.broadcasted_iota(jnp.int32, small, 0) < lax.broadcasted_iota(jnp.int32, small, 1),
            counts, 0,
        ),
        axis=0, keepdims=True,
    )
    offsets_ref[...] = inner_sum + first
    code_copy.wait()
    own_r.wait()
    mate_r.wait_recv()

    tile = pair_a.shape[1:]

    def multiply(c, stage, index, source):
        total = None
        for j in range(0, 2 * r_slots, 2):
            left = jnp.concatenate(
                [pair_r[x // r_slots, c * r_slots + x % r_slots] for x in (j, j + 1)], axis=1
            )
            right = jnp.concatenate(
                [
                    jnp.concatenate(
                        [
                            source[codes[stage * row_count + c, slot * 2 * r_slots + x]]
                            for slot in (index, index + 1)
                        ],
                        axis=1,
                    )
                    for x in (j, j + 1)
                ],
                axis=0,
            )
            term = jnp.dot(left, right, preferred_element_type=jnp.float32)
            total = term if total is None else total + term
        return total

    def own_stage(c, carry):
        for index in range(0, half_cap, 2):
            sums[c * half_cap // 2 + index // 2] = multiply(c, 0, index, pair_a)
        return carry

    lax.fori_loop(0, row_count, own_stage, 0)

    def near_mate(index):
        view = landed.at[pl.ds(part * near_slots + index * chunk, chunk)]
        return remote(view, view, near_pair_sems.at[0, index], near_pair_sems.at[1, index], mate_place)

    def far_view(index):
        return landed.at[pl.ds(far_base + part * far_slots + index * chunk, chunk)]

    def far_copy(index):
        return remote(
            landed.at[pl.ds(part * near_slots + index * chunk, chunk)], far_view(index),
            far_sems.at[0, index], far_sems.at[1, index], (onward, group),
        )

    def far_mate(index):
        view = far_view(index)
        return remote(
            view, view, far_pair_sems.at[0, index], far_pair_sems.at[1, index], mate_place
        )

    def take_far(index):
        @pl.when(has_far)
        def _():
            far_copy(index).wait_recv()
            far_mate(index).start()

    lag = 2
    for index in range(near_chunks):
        near_copy(index).wait_recv()
        if index < far_chunks:
            @pl.when(has_onward)
            def _():
                far_copy(index).start()
        near_mate(index).start()
        if 0 <= index - lag < far_chunks:
            take_far(index - lag)
    for index in range(max(near_chunks - lag, 0), far_chunks):
        take_far(index)

    pair_count = rows * pairs

    def crowd(which, most):
        which_row = which // pairs
        base_group = 2 * lax.rem(which, pairs)
        parity = lax.rem(which_row, 2)
        which_near = which_row + 1 - 2 * parity
        which_far = which_row - 1 + 2 * parity
        far_there = (which_far >= 0) & (which_far < rows)
        start = (which_row * groups + base_group) * local_rows
        columns = pair_columns_at(start)
        fine = lane_fine + start
        near_base = which_near * groups + base_group
        far_base_at = jnp.clip(which_far, 0, rows - 1) * groups + base_group
        by_near = need_of(gathered[near_base], gathered[near_base + 1], columns, fine)
        by_far = need_of(gathered[far_base_at], gathered[far_base_at + 1], columns, fine)
        by_far = jnp.where(far_there, by_far, 0)
        sends = jnp.sum(jnp.maximum(by_near, by_far), axis=1, keepdims=True)
        passes = jnp.sum(by_far, axis=1, keepdims=True)
        over = jnp.maximum(sends - 2 * near_slots, passes - 2 * far_slots)
        return jnp.maximum(most, over)

    worst_over = lax.fori_loop(0, pair_count, crowd, jnp.full((1, 1), -1, jnp.int32))
    flag_ref[...] = (worst_over > 0).astype(jnp.int32)

    for index in range(near_chunks):
        near_mate(index).wait_recv()

    @pl.when(has_far)
    def _():
        for index in range(far_chunks):
            far_mate(index).wait_recv()

    ahead_of = [lax.rem(index // own_cap + pairs - group // 2, pairs) for index in range(half_cap)]

    def out_copy(c, index):
        return pltpu.make_async_copy(
            done.at[c * half_cap + index],
            out_ref.at[ahead_of[index] * row_count * own_cap + c * own_cap + index % own_cap],
            out_sems.at[c * half_cap + index],
        )

    def near_stage(c, carry):
        for index in range(0, half_cap, 2):
            total = sums[c * half_cap // 2 + index // 2] + multiply(c, 1, index, landed)
            total = total.astype(done.dtype)
            done[c * half_cap + index] = total[:, : tile[1]]
            done[c * half_cap + index + 1] = total[:, tile[1] :]
        for index in range(half_cap):
            out_copy(c, index).start()
        return carry

    lax.fori_loop(0, row_count, near_stage, 0)

    sent = gathered.at[pl.ds(0, count - 1)]
    pltpu.make_async_copy(sent, sent, gather_sems.at[0]).wait()
    wait_close_send(0)

    @pl.when(has_far)
    def _():
        wait_close_send(2)

    mate_a.wait_send()
    mate_r.wait_send()
    for index in range(near_chunks):
        near_copy(index).wait_send()
        near_mate(index).wait_send()

    @pl.when(has_onward)
    def _():
        for index in range(far_chunks):
            far_copy(index).wait_send()

    @pl.when(has_far)
    def _():
        for index in range(far_chunks):
            far_mate(index).wait_send()

    def finish(c, carry):
        for index in range(half_cap):
            out_copy(c, index).wait()
        return carry

    lax.fori_loop(0, row_count, finish, 0)


def pair_sum_kernel(pairs, own, part_ref, landed, send_sems, recv_sems):
    row = lax.axis_index("rows")
    group = lax.axis_index("inner")
    core = lax.rem(group, 2)
    barrier = pltpu.get_barrier_semaphore()

    def place(ahead):
        return (row, 2 * lax.rem(group // 2 + ahead, pairs) + core)

    for ahead in range(1, pairs):
        pl.semaphore_signal(barrier, inc=1, device_id=place(ahead), device_id_type=MESH)
    pl.semaphore_wait(barrier, pairs - 1)
    copies = []
    for ahead in range(1, pairs):
        copy = pltpu.make_async_remote_copy(
            src_ref=part_ref.at[pl.ds(ahead * own, own)],
            dst_ref=landed.at[ahead - 1],
            send_sem=send_sems.at[ahead - 1],
            recv_sem=recv_sems.at[ahead - 1],
            device_id=place(ahead),
            device_id_type=MESH,
        )
        copy.start()
        copies.append(copy)
    for copy in copies:
        copy.wait()


def fused_body(rows, groups, r_tiles, r_cols, a_tiles, a_cols, c_cols, c_counts):
    local_rows, op_slots, tile, _ = a_tiles.shape
    row_count, r_slots = r_tiles.shape[:2]
    cap = c_cols.shape[1]
    tiles = local_rows * op_slots
    pairs = groups // 2
    count = rows * groups
    own_cap = cap // groups
    half_cap = cap // 2
    width = -(-2 * tiles // 128) * 128
    near_slots = min(NEAR_SLOTS, -(-tiles // CHUNK) * CHUNK)
    far_slots = min(FAR_SLOTS, near_slots)
    dims = (rows, groups, local_rows, op_slots, r_slots, cap, width, near_slots, far_slots, CHUNK)
    near_chunks = near_slots // CHUNK
    far_chunks = far_slots // CHUNK
    dtype = a_tiles.dtype
    out_dtype = jnp.bfloat16 if pairs == 1 else jnp.float32
    own = row_count * own_cap
    vmem = pl.BlockSpec(memory_space=pltpu.VMEM)
    anywhere = pl.BlockSpec(memory_space=pl.ANY)
    dma = pltpu.SemaphoreType.DMA
    part, offsets, flag = pl.pallas_call(
        functools.partial(fused_kernel, dims),
        out_shape=(
            jax.ShapeDtypeStruct((pairs * own, tile, tile), out_dtype),
            jax.ShapeDtypeStruct((1, row_count), jnp.int32),
            jax.ShapeDtypeStruct((1, 1), jnp.int32),
        ),
        in_specs=[vmem] * 4 + [anywhere] * 2,
        out_specs=(anywhere, vmem, vmem),
        scratch_shapes=[
            pltpu.VMEM((row_count, 128), jnp.int32),
            pltpu.VMEM((count, row_count, 128), jnp.int32),
            pltpu.VMEM((4, row_count, 128), jnp.int32),
            pltpu.VMEM((2 * tiles + 1, tile, tile), dtype),
            pltpu.VMEM((2, row_count * r_slots, tile, tile), dtype),
            pltpu.VMEM((near_slots, tile, tile), dtype),
            pltpu.VMEM((2 * (near_slots + far_slots) + 1, tile, tile), dtype),
            pltpu.VMEM((row_count * half_cap // 2, tile, 2 * tile), jnp.float32),
            pltpu.VMEM((row_count * half_cap, tile, tile), out_dtype),
            pltpu.VMEM((2 * row_count, width), jnp.int32),
            pltpu.SMEM((2 * row_count, width), jnp.int32),
            pltpu.SMEM((8, width), jnp.int32),
            dma((2,)),
            dma((2,)),
            dma((2, 4)),
            dma((2, 2)),
            dma((2, near_chunks)),
            dma((2, near_chunks)),
            dma((2, far_chunks)),
            dma((2, far_chunks)),
            dma((2,)),
            dma((row_count * half_cap,)),
        ],
        compiler_params=pltpu.CompilerParams(collective_id=40, has_side_effects=True),
        name="fused",
    )(
        r_cols,
        c_cols,
        c_counts[None, :],
        a_cols.T,
        a_tiles.reshape(tiles, tile, tile),
        r_tiles.reshape(row_count * r_slots, tile, tile),
    )
    if pairs == 1:
        c_tiles = part
    else:
        landed = pl.pallas_call(
            functools.partial(pair_sum_kernel, pairs, own),
            out_shape=jax.ShapeDtypeStruct((pairs - 1, own, tile, tile), jnp.float32),
            in_specs=[anywhere],
            out_specs=anywhere,
            scratch_shapes=[dma((pairs - 1,)), dma((pairs - 1,))],
            compiler_params=pltpu.CompilerParams(collective_id=41, has_side_effects=True),
            name="pair_sums",
        )(part)
        c_tiles = part[:own]
        for ahead in range(pairs - 1):
            c_tiles = c_tiles + landed[ahead]
        c_tiles = c_tiles.astype(jnp.bfloat16)
    return c_tiles.reshape(row_count, own_cap, tile, tile), offsets[0], flag[0, 0]


def body(rows, groups, *args):
    if rows % 2 or groups % 2:
        return plain_body(rows, groups, *args)
    c_tiles, offsets, flag = fused_body(rows, groups, *args)

    def again(c_tiles, offsets, *args):
        return plain_body(rows, groups, *args)

    def keep(c_tiles, offsets, *args):
        return c_tiles, offsets

    return lax.cond(flag > 0, again, keep, c_tiles, offsets, *args)


def solution(mesh):
    rows = mesh.shape["rows"]
    groups = mesh.shape["inner"]
    return jax.shard_map(
        functools.partial(body, rows, groups),
        mesh=mesh,
        in_specs=(
            P("rows", "inner", None, None),
            P("rows", "inner"),
            P(("rows", "inner"), None, None, None),
            P(),
            P("rows", None),
            P("rows"),
        ),
        out_specs=(P("rows", "inner", None, None), P("rows")),
        check_vma=False,
    )
```

```python
import functools

import jax
import jax.numpy as jnp
from jax import lax
from jax.experimental import pallas as pl
from jax.experimental.pallas import tpu as pltpu
from jax.sharding import PartitionSpec as P

MESH = pl.DeviceIdType.MESH
BATCH = 4


def plan_kernel(
    dims, r_cols_ref, c_cols_ref, counts_ref, columns_ref, code_ref, plan_ref,
    meta_ref, gathered, needs, send_sem, recv_sem,
):
    rows, groups, local_rows, op_slots, r_slots, cap, half = dims
    width = 2 * half
    count = rows * groups
    tiles = local_rows * op_slots
    row = lax.axis_index("rows")
    group = lax.axis_index("inner")
    me = row * groups + group

    barrier = pltpu.get_barrier_semaphore()

    def place(step):
        other = lax.rem(me + step, count)
        return (other // groups, lax.rem(other, groups))

    def greet(step, carry):
        pl.semaphore_signal(barrier, inc=1, device_id=place(step), device_id_type=MESH)
        return carry

    lax.fori_loop(1, count, greet, 0)
    row_count = r_cols_ref.shape[0]
    live = r_slots + cap
    lanes = lax.broadcasted_iota(jnp.int32, (row_count, width), 1)
    above = lax.broadcasted_iota(jnp.int32, (row_count, width), 0)
    small = (row_count, row_count)
    diagonal = lax.broadcasted_iota(jnp.int32, small, 0) == lax.broadcasted_iota(jnp.int32, small, 1)
    spread_counts = jnp.broadcast_to(counts_ref[...], small)
    own_counts = jnp.sum(jnp.where(diagonal, spread_counts, 0), axis=1, keepdims=True)
    meta_ref[...] = jnp.full(meta_ref.shape, -9, jnp.int32)
    meta_ref[:, 0:r_slots] = r_cols_ref[...]
    meta_ref[:, r_slots:live] = c_cols_ref[...]
    meta_ref[:, live : live + 1] = own_counts
    gathered[me] = meta_ref[...]
    pl.semaphore_wait(barrier, count - 1)

    def post(step, carry):
        pltpu.make_async_remote_copy(
            src_ref=meta_ref,
            dst_ref=gathered.at[me],
            send_sem=send_sem,
            recv_sem=recv_sem,
            device_id=place(step),
            device_id_type=MESH,
        ).start()
        return carry

    lax.fori_loop(1, count, post, 0)
    everyone = gathered.at[pl.ds(0, count - 1)]
    pltpu.make_async_copy(everyone, everyone, send_sem).wait()
    pltpu.make_async_copy(everyone, everyone, recv_sem).wait()

    def matches(block, columns, fine_rows):
        named = fine_rows == block[:, 0:1]
        for j in range(1, r_slots):
            named = named | (fine_rows == block[:, j : j + 1])
        slot = jnp.full((row_count, width), -1, jnp.int32)
        for s in range(cap):
            slot = jnp.where(columns == block[:, r_slots + s : r_slots + s + 1], s, slot)
        return jnp.where(named, slot, -1)

    shift = jnp.where(lanes < half, -groups, groups) * local_rows
    tile = jnp.where(lanes < half, lanes, lanes - half)
    lane_rows = jnp.where(tile < tiles, shift + tile // op_slots, -(1 << 24))
    low_lanes = lanes[0:1] < half

    def near_matches(device):
        before = columns_ref[pl.ds(jnp.maximum(device - groups, 0), 1), :]
        after = columns_ref[pl.ds(jnp.minimum(device + groups, count - 1), 1), :]
        columns = jnp.where(low_lanes, before, after)
        return matches(gathered[device], columns, lane_rows + device * local_rows)

    def wanted(found):
        return jnp.max((found >= 0).astype(jnp.int32), axis=0, keepdims=True)

    def gather_needs(device, carry):
        needs[pl.ds(device, 1), :] = wanted(near_matches(device))
        return carry

    lax.fori_loop(0, count, gather_needs, 0, unroll=4)
    every = needs[...]
    low_side = lax.broadcasted_iota(jnp.int32, every.shape, 1) < half
    low = jnp.sum(jnp.where(low_side, every, 0), axis=1, keepdims=True)
    high = jnp.sum(jnp.where(low_side, 0, every), axis=1, keepdims=True)
    most = jnp.max(jnp.maximum(low, high), axis=0, keepdims=True)

    down = lax.broadcasted_iota(jnp.int32, (width, width), 0)
    across = lax.broadcasted_iota(jnp.int32, (width, width), 1)
    same = (down < half) == (across < half)

    def ranks(need):
        spread = jnp.broadcast_to(need, (width, width))
        column = jnp.sum(jnp.where(down == across, spread, 0), axis=1, keepdims=True)
        before = jnp.sum(jnp.where((across < down) & same, spread, 0), axis=1, keepdims=True)
        along = jnp.sum(
            jnp.where((down < across) & same, jnp.broadcast_to(column, (width, width)), 0),
            axis=0,
            keepdims=True,
        )
        return column, before, along

    def send_list(device, high):
        column, before, _ = ranks(needs[pl.ds(device, 1), :])
        first = half if high else 0
        mine = (down >= half) if high else (down < half)
        chosen = mine & (column > 0) & (before == across)
        return jnp.sum(jnp.where(chosen, down - first, 0), axis=0, keepdims=True)

    left = jnp.maximum(row - 1, 0) * groups + group
    right = jnp.minimum(row + 1, rows - 1) * groups + group
    plan_ref[0:1, :] = send_list(left, True)
    plan_ref[1:2, :] = send_list(right, False)

    found = near_matches(me)
    _, _, along = ranks(wanted(found))
    slot_at = along + jnp.where(lanes[0:1] < half, tiles, 2 * tiles)
    code_ref[:, 0:width] = jnp.where(found >= 0, found + cap * slot_at, -1)
    fine = me * local_rows + jnp.where(lanes < tiles, lanes // op_slots, 0)
    fine = jnp.where(lanes < tiles, fine, -5)
    found = matches(gathered[me], columns_ref[pl.ds(me, 1), :], fine)
    code_ref[:, width:] = jnp.where(found >= 0, found + cap * lanes, -1)

    def earlier(index, total):
        block = gathered[index * groups]
        return total + jnp.sum(block[:, live : live + 1], axis=0, keepdims=True)

    first = lax.fori_loop(0, row, earlier, jnp.zeros((1, 1), jnp.int32))
    counts = jnp.broadcast_to(own_counts, (row_count, width))
    inner_sum = jnp.sum(jnp.where(above < lanes, counts, 0), axis=0, keepdims=True)
    plan_ref[2:3, :] = inner_sum + first
    level = jnp.zeros((1, 1), jnp.int32)
    for size in sizes_for(tiles)[:-1]:
        level = level + (most > size).astype(jnp.int32)
    plan_ref[3:4, :] = jnp.broadcast_to(level, (1, width))


def halo_kernel(rows, size, plan_ref, a_ref, out_ref, packed, send_sems, recv_sems):
    row = lax.axis_index("rows")
    group = lax.axis_index("inner")
    barrier = pltpu.get_barrier_semaphore()
    has_left = row > 0
    has_right = row < rows - 1

    @pl.when(has_left)
    def _():
        pl.semaphore_signal(barrier, inc=1, device_id=(row - 1, group), device_id_type=MESH)

    @pl.when(has_right)
    def _():
        pl.semaphore_signal(barrier, inc=1, device_id=(row + 1, group), device_id_type=MESH)

    def pack(index, carry):
        packed[0, index] = a_ref[plan_ref[0, index]]
        packed[1, index] = a_ref[plan_ref[1, index]]
        return carry

    lax.fori_loop(0, size, pack, 0, unroll=2)

    pl.semaphore_wait(barrier, has_left.astype(jnp.int32) + has_right.astype(jnp.int32))

    def copy(side, other):
        return pltpu.make_async_remote_copy(
            src_ref=packed.at[side],
            dst_ref=out_ref.at[1 - side, pl.ds(0, size)],
            send_sem=send_sems.at[side],
            recv_sem=recv_sems.at[1 - side],
            device_id=(other, group),
            device_id_type=MESH,
        )

    @pl.when(has_left)
    def _():
        copy(0, row - 1).start()

    @pl.when(has_right)
    def _():
        copy(1, row + 1).start()

    @pl.when(has_left)
    def _():
        copy(0, row - 1).wait_send()
        copy(1, row - 1).wait_recv()

    @pl.when(has_right)
    def _():
        copy(1, row + 1).wait_send()
        copy(0, row + 1).wait_recv()


def product_kernel(dims, code_ref, cols_ref, r_ref, a_ref, halo_ref, out_ref, tiles_ref, jobs, sems):
    rows, groups, local_rows, op_slots, r_slots, cap, half = dims
    width = 2 * half
    tiles = local_rows * op_slots
    row_count = cols_ref.shape[0]
    own_cap = cap // groups
    row = lax.axis_index("rows")
    group = lax.axis_index("inner")
    own = pltpu.make_async_copy(a_ref, tiles_ref.at[pl.ds(0, tiles)], sems.at[0])
    near = pltpu.make_async_copy(halo_ref, tiles_ref.at[pl.ds(tiles, 2 * tiles)], sems.at[1])
    own.start()
    near.start()
    last = groups * row_count * own_cap
    scale = 1 << (3 * tiles * cap - 1).bit_length()

    def clear(index, carry):
        out_ref[index] = jnp.zeros(out_ref.shape[1:], jnp.float32)
        return carry

    lax.fori_loop(0, last, clear, 0, unroll=4)

    def list_row(c, found):
        def list_slot(j, found):
            fine = cols_ref[c, j]
            side = fine // (local_rows * groups) - row
            base = jnp.where(side == 0, width, jnp.where(side < 0, 0, half))
            base = base + lax.rem(fine, local_rows) * op_slots
            for t in range(op_slots):
                code = code_ref[c, base + t]
                jobs[found] = (c * r_slots + j) * scale + code
                found = found + (code >= 0).astype(jnp.int32)
            return found

        return lax.fori_loop(0, r_slots, list_slot, found)

    found = lax.fori_loop(0, row_count, list_row, jnp.int32(0))
    for extra in range(BATCH):
        jobs[found + extra] = -1
    own.wait()
    near.wait()

    def batch(step, carry):
        results = []
        targets = []
        for extra in range(BATCH):
            job = jobs[step * BATCH + extra]
            valid = job >= 0
            job = jnp.maximum(job, 0)
            pair = job // scale
            code = lax.rem(job, scale)
            slot = lax.rem(code, cap)
            ahead = lax.rem(slot // own_cap + groups - group, groups)
            target = (ahead * row_count + pair // r_slots) * own_cap + lax.rem(slot, own_cap)
            targets.append(jnp.where(valid, target, last))
            results.append(
                jnp.dot(
                    r_ref[pair],
                    tiles_ref[code // cap],
                    preferred_element_type=jnp.float32,
                )
            )
        for extra in range(BATCH):
            target = targets[extra]
            out_ref[target] = out_ref[target] + results[extra]
        return carry

    lax.fori_loop(0, (found + BATCH - 1) // BATCH, batch, 0)


def sum_kernel(groups, own, part_ref, landed, send_sems, recv_sems):
    row = lax.axis_index("rows")
    group = lax.axis_index("inner")
    barrier = pltpu.get_barrier_semaphore()
    for ahead in range(1, groups):
        pl.semaphore_signal(
            barrier, inc=1, device_id=(row, lax.rem(group + ahead, groups)), device_id_type=MESH
        )
    pl.semaphore_wait(barrier, groups - 1)
    copies = []
    for ahead in range(1, groups):
        copy = pltpu.make_async_remote_copy(
            src_ref=part_ref.at[pl.ds(ahead * own, own)],
            dst_ref=landed.at[ahead - 1],
            send_sem=send_sems.at[ahead - 1],
            recv_sem=recv_sems.at[ahead - 1],
            device_id=(row, lax.rem(group + ahead, groups)),
            device_id_type=MESH,
        )
        copy.start()
        copies.append(copy)
    for copy in copies:
        copy.wait()


def sizes_for(tiles):
    steps = [16, 18, 20, 21, 22, 23, 24, 25, 26, 27, 28, 29, 30, 32, 36, 42]
    return [size for size in steps if size < tiles] + [tiles]


def plain_body(rows, groups, r_tiles, r_cols, a_tiles, a_cols, c_cols, c_counts):
    local_rows, op_slots, tile, _ = a_tiles.shape
    row_count, r_slots = r_tiles.shape[:2]
    cap = c_cols.shape[1]
    tiles = local_rows * op_slots
    half = -(-tiles // 64) * 64
    width = 2 * half
    count = rows * groups
    own_cap = cap // groups
    dims = (rows, groups, local_rows, op_slots, r_slots, cap, half)
    vmem = pl.BlockSpec(memory_space=pltpu.VMEM)
    smem = pl.BlockSpec(memory_space=pltpu.SMEM)
    anywhere = pl.BlockSpec(memory_space=pl.ANY)

    flat = a_cols.reshape(count, tiles)
    flat = jnp.pad(flat, ((0, 0), (0, half - tiles)), constant_values=-2)
    columns = jnp.concatenate([flat, flat], axis=1)

    code, plan = pl.pallas_call(
        functools.partial(plan_kernel, dims),
        out_shape=(
            jax.ShapeDtypeStruct((row_count, 2 * width), jnp.int32),
            jax.ShapeDtypeStruct((8, width), jnp.int32),
        ),
        in_specs=[vmem] * 4,
        out_specs=(vmem, vmem),
        scratch_shapes=[
            pltpu.VMEM((row_count, width), jnp.int32),
            pltpu.VMEM((count, row_count, width), jnp.int32),
            pltpu.VMEM((count, width), jnp.int32),
            pltpu.SemaphoreType.DMA,
            pltpu.SemaphoreType.DMA,
        ],
        compiler_params=pltpu.CompilerParams(collective_id=0, has_side_effects=True),
        name="plan",
    )(r_cols, c_cols, c_counts[None, :], columns)

    flat_a = a_tiles.reshape(tiles, tile, tile)
    sizes = sizes_for(tiles)

    def exchange(number, size, plan, flat_a):
        return pl.pallas_call(
            functools.partial(halo_kernel, rows, size),
            out_shape=jax.ShapeDtypeStruct((2, tiles, tile, tile), a_tiles.dtype),
            in_specs=[smem, vmem],
            out_specs=anywhere,
            scratch_shapes=[
                pltpu.VMEM((2, size, tile, tile), a_tiles.dtype),
                pltpu.SemaphoreType.DMA((2,)),
                pltpu.SemaphoreType.DMA((2,)),
            ],
            compiler_params=pltpu.CompilerParams(collective_id=number + 2, has_side_effects=True),
            name=f"halo{size}",
        )(plan, flat_a)

    halo = lax.switch(
        plan[3, 0],
        [functools.partial(exchange, number, size) for number, size in enumerate(sizes)],
        plan,
        flat_a,
    )

    slots = row_count * r_slots * op_slots + BATCH
    partial_value = pl.pallas_call(
        functools.partial(product_kernel, dims),
        out_shape=jax.ShapeDtypeStruct((row_count * cap + 1, tile, tile), jnp.float32),
        in_specs=[smem, smem, vmem, anywhere, anywhere],
        out_specs=vmem,
        scratch_shapes=[
            pltpu.VMEM((3 * tiles, tile, tile), a_tiles.dtype),
            pltpu.SMEM((slots,), jnp.int32),
            pltpu.SemaphoreType.DMA((2,)),
        ],
        name="products",
    )(
        code,
        r_cols,
        r_tiles.reshape(row_count * r_slots, tile, tile),
        flat_a,
        halo.reshape(2 * tiles, tile, tile),
    )

    own_count = row_count * own_cap
    landed = pl.pallas_call(
        functools.partial(sum_kernel, groups, own_count),
        out_shape=jax.ShapeDtypeStruct((groups - 1, own_count, tile, tile), jnp.float32),
        in_specs=[anywhere],
        out_specs=anywhere,
        scratch_shapes=[
            pltpu.SemaphoreType.DMA((groups - 1,)),
            pltpu.SemaphoreType.DMA((groups - 1,)),
        ],
        compiler_params=pltpu.CompilerParams(collective_id=1, has_side_effects=True),
        name="sums",
    )(partial_value)
    c_tiles = partial_value[:own_count]
    for ahead in range(groups - 1):
        c_tiles = c_tiles + landed[ahead]
    c_tiles = c_tiles.astype(jnp.bfloat16)
    return (c_tiles.reshape(row_count, own_cap, tile, tile), plan[2, :row_count])

LIST_SLOTS = 27
PASS_SLOTS = 15
CHUNK = 3
JOBS = 6
REMOTE = 1 << 14


def fused_kernel(
    dims, r_cols_hbm, c_cols_hbm, counts_hbm, columns_hbm, a_ref, r_ref,
    out_ref, offsets_ref, flag_ref,
    r_cols_ref, c_cols_ref, counts_ref, columns_ref,
    meta, close, placing, pair_a, pair_r, packed, landed, sums, tables, codes, picks,
    told, scan_out, scan_in,
    local_sems, close_sems, pair_sems, place_sems, early_sems, near_sems, near_send,
    near_pair_sems, far_sems, far_send, far_pair_sems, table_sems, told_sems, scan_sems,
):
    (rows, groups, local_rows, op_slots, r_slots, cap, width, list_slots, pass_slots, chunk) = dims
    pairs = groups // 2
    tiles = local_rows * op_slots
    span = 2 * local_rows
    own_cap = cap // groups
    half_cap = cap // 2
    both = 2 * r_slots
    row_count = r_cols_ref.shape[0]
    live = r_slots + cap
    early = op_slots
    near_slots = early + list_slots
    far_slots = early + pass_slots
    near_chunks = list_slots // chunk
    far_chunks = pass_slots // chunk
    far_base = 2 * near_slots
    zero_near = 2 * (near_slots + far_slots)
    zero_own = 2 * tiles
    rounds = (rows - 1).bit_length()

    row = lax.axis_index("rows")
    group = lax.axis_index("inner")
    part = lax.rem(group, 2)
    first_group = group - part
    mate = first_group + 1 - part
    odd = lax.rem(row, 2)
    near = row + 1 - 2 * odd
    far = row - 1 + 2 * odd
    has_far = (far >= 0) & (far < rows)
    onward = near + 1 - 2 * odd
    has_onward = (onward >= 0) & (onward < rows)
    mate_place = (row, mate)

    barrier = pltpu.get_barrier_semaphore()

    def greet(place):
        pl.semaphore_signal(barrier, inc=1, device_id=place, device_id_type=MESH)

    for core in range(2):
        greet((near, first_group + core))

    @pl.when(has_far)
    def _():
        for core in range(2):
            greet((far, first_group + core))

    for ahead in range(1, groups):
        greet((row, lax.rem(group + ahead, groups)))

    small_copies = [
        pltpu.make_async_copy(src, dst, local_sems.at[2 + index])
        for index, (src, dst) in enumerate(
            [
                (r_cols_hbm, r_cols_ref),
                (c_cols_hbm, c_cols_ref),
                (counts_hbm, counts_ref),
                (columns_hbm, columns_ref),
            ]
        )
    ]
    for copy in small_copies:
        copy.start()
    own_a = pltpu.make_async_copy(
        a_ref, pair_a.at[pl.ds(part * tiles, tiles)], local_sems.at[0]
    )
    own_r = pltpu.make_async_copy(r_ref, pair_r.at[part], local_sems.at[1])
    own_a.start()
    own_r.start()

    def remote(src, dst, send_sem, recv_sem, place):
        return pltpu.make_async_remote_copy(
            src_ref=src, dst_ref=dst, send_sem=send_sem, recv_sem=recv_sem,
            device_id=place, device_id_type=MESH,
        )

    def wait_bytes(view, sem):
        pltpu.make_async_copy(view, view, sem).wait()

    small = (row_count, row_count)
    diagonal = lax.broadcasted_iota(jnp.int32, small, 0) == lax.broadcasted_iota(jnp.int32, small, 1)
    meta[...] = jnp.full(meta.shape, -9, jnp.int32)
    pair_a[zero_own] = jnp.zeros(pair_a.shape[1:], pair_a.dtype)
    landed[zero_near] = jnp.zeros(landed.shape[1:], landed.dtype)
    for copy in small_copies:
        copy.wait()
    spread_counts = jnp.broadcast_to(counts_ref[...], small)
    own_counts = jnp.sum(jnp.where(diagonal, spread_counts, 0), axis=1, keepdims=True)
    meta[:, 0:r_slots] = r_cols_ref[...]
    meta[:, r_slots:live] = c_cols_ref[...]
    own_a.wait()

    pl.semaphore_wait(barrier, groups + 1 + 2 * has_far.astype(jnp.int32))

    def start_close(target, first, which):
        for core in range(2):
            remote(
                meta, close.at[first + part], close_sems.at[0, which], close_sems.at[1, which],
                (target, first_group + core),
            ).start()

    @pl.when(has_far)
    def _():
        start_close(far, 2, 1)

    start_close(near, 0, 0)
    to_mate = remote(meta, close.at[4], close_sems.at[0, 2], close_sems.at[1, 2], mate_place)
    to_mate.start()
    mate_a = remote(
        a_ref, pair_a.at[pl.ds(part * tiles, tiles)], pair_sems.at[0, 0], pair_sems.at[1, 0], mate_place
    )
    mate_a.start()

    early_copy = remote(
        pair_a.at[pl.ds(part * tiles, early)], landed.at[pl.ds(part * near_slots, early)],
        early_sems.at[0], early_sems.at[1], (near, group),
    )
    early_copy.start()
    mate_r = remote(r_ref, pair_r.at[part], pair_sems.at[0, 1], pair_sems.at[1, 1], mate_place)
    mate_r.start()

    lanes = lax.broadcasted_iota(jnp.int32, (1, width), 1)
    real = lanes < op_slots * span
    lane_slot = lanes // span
    lane_fine = jnp.where(real, lax.rem(lanes, span), -(1 << 24))
    lane_core = lax.rem(lanes, span) // local_rows
    lane_local = lax.rem(lanes, local_rows)
    lane_tile = lane_core * tiles + lane_local * op_slots + lane_slot
    late = jnp.where(lane_local > 0, 1, 0)

    def pair_columns(which_row):
        start = (which_row * groups + first_group) * local_rows
        block = start // 128
        values = columns_ref[:, pl.ds(pl.multiple_of(block * 128, 128), 128)]
        if width > 128:
            values = jnp.concatenate([values] * (width // 128), axis=1)
        offset = start - block * 128
        total = jnp.zeros((1, width), jnp.int32)
        for t in range(op_slots):
            moved = pltpu.roll(values[t : t + 1, :], lax.rem(t * span - offset + 128 * width, width), 1)
            total = jnp.where(lane_slot == t, moved, total)
        return jnp.where(real, total, -2)

    def pair_fine(which_row):
        return lane_fine + (which_row * groups + first_group) * local_rows

    def need_of(meta_low, meta_high, columns, fine):
        named = fine == meta_low[:, 0:1]
        for j in range(1, r_slots):
            named = named | (fine == meta_low[:, j : j + 1])
        for j in range(r_slots):
            named = named | (fine == meta_high[:, j : j + 1])
        wanted = columns == meta_low[:, r_slots : r_slots + 1]
        for s in range(1, cap):
            wanted = wanted | (columns == meta_low[:, r_slots + s : r_slots + s + 1])
        return jnp.max((named & wanted).astype(jnp.int32), axis=0, keepdims=True)

    def before(need):
        total = need
        step = 1
        while step < width:
            total = total + jnp.where(lanes >= step, pltpu.roll(total, step, 1), 0)
            step *= 2
        return total - need

    def landing(places, count, base, slots):
        fits = (places >= 0) & (places < 2 * count)
        at = lax.rem(places, 2) * slots + early + places // 2
        at = jnp.where(late > 0, jnp.where(fits, at, -1), lane_core * slots + lane_slot)
        return jnp.where(real & (at >= 0), REMOTE + base + at, -1)

    own_columns = pair_columns(row)
    own_fine = pair_fine(row)

    @pl.when(has_far)
    def _():
        wait_bytes(close.at[pl.ds(2, 2)], close_sems.at[1, 1])

    @pl.when(jnp.logical_not(has_far))
    def _():
        close[2] = jnp.full(close.shape[1:], -9, jnp.int32)
        close[3] = jnp.full(close.shape[1:], -9, jnp.int32)

    need_far = need_of(close[2], close[3], own_columns, own_fine) * late
    far_before = before(need_far)
    far_total = jnp.sum(need_far, axis=1, keepdims=True)
    wait_bytes(close.at[pl.ds(0, 2)], close_sems.at[1, 0])
    need_near = need_of(close[0], close[1], own_columns, own_fine) * late
    need_only = need_near * (1 - need_far)
    near_total = far_total + jnp.sum(need_only, axis=1, keepdims=True)
    places = jnp.where(
        need_far > 0, far_before, jnp.where(need_only > 0, before(need_only) + far_total, -1)
    )
    pick_rows = -(-list_slots // 8) * 8
    slot_down = lax.broadcasted_iota(jnp.int32, (pick_rows, width), 0)
    chosen = jnp.broadcast_to(places, (pick_rows, width)) == 2 * slot_down + part
    picked = jnp.sum(
        jnp.where(chosen, jnp.broadcast_to(lane_tile, (pick_rows, width)), 0), axis=1, keepdims=True
    )
    across = lax.broadcasted_iota(jnp.int32, (pick_rows, width), 1)
    pick_row = jnp.sum(
        jnp.where(slot_down == across, jnp.broadcast_to(picked, (pick_rows, width)), 0),
        axis=0, keepdims=True,
    )
    tables[0:8, :] = jnp.broadcast_to(pick_row, (8, width))
    pick_copy = pltpu.make_async_copy(tables.at[pl.ds(0, 8)], picks, table_sems.at[0])
    pick_copy.start()
    placing[0] = jnp.broadcast_to(landing(places, list_slots, 0, near_slots), placing.shape[1:])
    place_copy = remote(placing.at[0], placing.at[1], place_sems.at[0], place_sems.at[1], (near, group))
    place_copy.start()
    mate_a.wait_recv()
    pick_copy.wait()

    def near_view(index):
        return landed.at[pl.ds(part * near_slots + early + index * chunk, chunk)]

    def near_copy(index):
        return remote(
            packed.at[pl.ds(index * chunk, chunk)], near_view(index),
            near_send.at[0], near_sems.at[index], (near, group),
        )

    def pack(index):
        for extra in range(chunk):
            packed[index * chunk + extra] = pair_a[picks[0, index * chunk + extra]]

    pack(0)
    for index in range(near_chunks):
        if index + 1 < near_chunks:
            pack(index + 1)
        near_copy(index).start()

    near_columns = pair_columns(near)
    near_fine = pair_fine(near)
    far_row = jnp.clip(far, 0, rows - 1)
    far_columns = pair_columns(far_row)
    far_fine = jnp.where(has_far, pair_fine(far_row), -(1 << 24))
    to_mate.wait_recv()
    mine, other = meta[...], close[4]
    my_low = jnp.where(part == 0, mine, other)
    my_high = jnp.where(part == 0, other, mine)
    far_need = need_of(my_low, my_high, far_columns, far_fine) * late
    far_places = jnp.where(far_need > 0, before(far_need), -1)
    far_at = landing(far_places, pass_slots, far_base, far_slots)
    place_copy.wait_recv()
    near_at = placing[1][0:1, :]

    above = (row_count, width)
    table_lanes = lax.broadcasted_iota(jnp.int32, above, 1)
    own_at, near_at, far_at = [jnp.broadcast_to(x, above) for x in (lane_tile, near_at, far_at)]
    slot_own, slot_near, slot_far = [], [], []
    for index in range(half_cap):
        even = (2 * (index // own_cap)) * own_cap + index % own_cap
        low = my_low[:, r_slots + even : r_slots + even + 1]
        high = my_low[:, r_slots + even + own_cap : r_slots + even + own_cap + 1]
        column = jnp.where(part == 0, low, high)
        slot_own.append(jnp.where(own_columns == column, own_at, -1))
        slot_near.append(jnp.where(near_columns == column, near_at, -1))
        slot_far.append(jnp.where(far_columns == column, far_at, -1))
    code = jnp.full(above, -1, jnp.int32)
    for j in range(both):
        block = my_low if j < r_slots else my_high
        named = block[:, j % r_slots : j % r_slots + 1]
        in_own = own_fine == named
        in_near = near_fine == named
        in_far = far_fine == named
        for index in range(half_cap):
            found = jnp.where(in_own, slot_own[index], -1)
            found = jnp.where(in_near, slot_near[index], found)
            found = jnp.where(in_far, slot_far[index], found)
            best = jnp.max(found, axis=1, keepdims=True)
            code = jnp.where(table_lanes == index * both + j, best, code)
    tables[0:row_count, :] = jnp.where((code >= 0) & (code < REMOTE), code, zero_own)
    away = code >= REMOTE
    rank = away.astype(jnp.int32)
    table_j = lax.rem(table_lanes, both)
    step = 1
    while step < both:
        rank = rank + jnp.where(table_j >= step, pltpu.roll(rank, step, 1), 0)
        step *= 2
    crowded = jnp.max(jnp.max(rank, axis=1, keepdims=True), axis=0, keepdims=True)
    job = jnp.where(away, (code - REMOTE) * both + table_j, -1)
    rank = jnp.where(away, rank - 1 + (table_lanes // both) * JOBS, -1)
    short = jnp.full(above, -1, jnp.int32)
    for at in range(half_cap * JOBS):
        best = jnp.max(jnp.where(rank == at, job, -1), axis=1, keepdims=True)
        short = jnp.where(table_lanes == at, best, short)
    job_j = lax.rem(jnp.maximum(short, 0), both)
    job_c = lax.broadcasted_iota(jnp.int32, above, 0)
    job_r = (job_j // r_slots) * (row_count * r_slots) + job_c * r_slots + lax.rem(job_j, r_slots)
    tables[row_count : 2 * row_count, :] = jnp.where(short >= 0, short // both, zero_near)
    tables[2 * row_count : 3 * row_count, :] = job_r
    code_copy = pltpu.make_async_copy(tables, codes, table_sems.at[1])
    code_copy.start()

    over = jnp.maximum(near_total - 2 * list_slots, far_total - 2 * pass_slots)
    over = jnp.maximum(over, crowded - JOBS)
    over = (over > 0).astype(jnp.int32)
    told[group] = jnp.broadcast_to(over, told.shape[1:])

    def tell(ahead):
        return remote(
            told.at[group], told.at[group], told_sems.at[0], told_sems.at[1],
            (row, lax.rem(group + ahead, groups)),
        )

    for ahead in range(1, groups):
        tell(ahead).start()

    tile = pair_a.shape[1]
    total_count = jnp.sum(own_counts, axis=0, keepdims=True)

    def scan_copy(k, side):
        other = row + (1 << k) if side == 0 else row - (1 << k)
        return remote(
            scan_out.at[k], scan_in.at[k, side], scan_sems.at[0, k, side], scan_sems.at[1, k, side],
            (other, group),
        )

    scan_shape = scan_out.shape[1:]
    scan_lane = lax.broadcasted_iota(jnp.int32, scan_shape, 1)
    above_there = [row + (1 << k) < rows for k in range(rounds)]
    below_there = [row - (1 << k) >= 0 for k in range(rounds)]

    def scan_send(k, state):
        scan_out[k] = state

        @pl.when(above_there[k])
        def _():
            scan_copy(k, 0).start()

        @pl.when(below_there[k])
        def _():
            scan_copy(k, 1).start()

    def scan_take(k, state):
        @pl.when(below_there[k])
        def _():
            scan_copy(k, 0).wait_recv()

        @pl.when(above_there[k])
        def _():
            scan_copy(k, 1).wait_recv()

        below = jnp.where((scan_lane < 2) & below_there[k], scan_in[k, 0], 0)
        beyond = jnp.where((scan_lane == 2) & above_there[k], scan_in[k, 1], 0)
        return state + below + beyond

    wait_bytes(told.at[pl.ds(0, groups - 1)], told_sems.at[1])
    over = told[0]
    for other_group in range(1, groups):
        over = over + told[other_group]
    state = jnp.where(
        scan_lane == 0, jnp.broadcast_to(total_count, scan_shape),
        jnp.where(scan_lane < 3, over, 0),
    )
    scan_send(0, state)

    def mate_copy(view, sems):
        return remote(view, view, sems.at[0], sems.at[1], mate_place)

    early_view = landed.at[pl.ds(part * near_slots, early)]
    early_far_view = landed.at[pl.ds(far_base + part * far_slots, early)]

    def far_view(index):
        return landed.at[pl.ds(far_base + part * far_slots + early + index * chunk, chunk)]

    early_far = remote(early_view, early_far_view, far_send.at[0], far_sems.at[far_chunks], (onward, group))

    def far_copy(index):
        return remote(
            near_view(index), far_view(index), far_send.at[0], far_sems.at[index], (onward, group)
        )

    def take_far(index):
        @pl.when(has_far)
        def _():
            if index < 0:
                early_far.wait_recv()
                mate_copy(early_far_view, far_pair_sems).start()
            else:
                far_copy(index).wait_recv()
                mate_copy(far_view(index), far_pair_sems).start()

    early_copy.wait_recv()

    @pl.when(has_onward)
    def _():
        early_far.start()

    mate_copy(early_view, near_pair_sems).start()
    code_copy.wait()
    own_r.wait()
    mate_r.wait_recv()

    def flat_r(index):
        return pair_r[index // (row_count * r_slots), lax.rem(index, row_count * r_slots)]

    def own_stage(c, carry):
        for index in range(0, half_cap, 2):
            total = None
            for j in range(0, both, 2):
                left = jnp.concatenate(
                    [pair_r[x // r_slots, c * r_slots + x % r_slots] for x in (j, j + 1)], axis=1
                )
                right = jnp.concatenate(
                    [
                        jnp.concatenate(
                            [pair_a[codes[c, slot * both + x]] for slot in (index, index + 1)], axis=1
                        )
                        for x in (j, j + 1)
                    ],
                    axis=0,
                )
                term = jnp.dot(left, right, preferred_element_type=jnp.float32)
                total = term if total is None else total + term
            sums[c * half_cap + index] = total[:, :tile]
            sums[c * half_cap + index + 1] = total[:, tile:]
        return carry

    lag = 2
    scans = 0
    for index in range(near_chunks):
        near_copy(index).wait_recv()
        if index < far_chunks:
            @pl.when(has_onward)
            def _():
                far_copy(index).start()
        mate_copy(near_view(index), near_pair_sems).start()
        if -1 <= index - lag < far_chunks:
            take_far(index - lag)
        lax.fori_loop(
            index * row_count // near_chunks, (index + 1) * row_count // near_chunks, own_stage, 0
        )
        if index > 0 and scans < rounds:
            state = scan_take(scans, state)
            scans += 1
            if scans < rounds:
                scan_send(scans, state)
    for index in range(max(near_chunks - lag, -1), far_chunks):
        take_far(index)
    while scans < rounds:
        state = scan_take(scans, state)
        scans += 1
        if scans < rounds:
            scan_send(scans, state)

    flags = jnp.where((scan_lane == 1) | (scan_lane == 2), state, 0)
    flags = jnp.max(jnp.max(flags, axis=1, keepdims=True), axis=0, keepdims=True)
    flag_ref[...] = (flags > 0).astype(jnp.int32)
    reached = jnp.where(scan_lane == 0, state, 0)
    reached = jnp.max(jnp.max(reached, axis=1, keepdims=True), axis=0, keepdims=True)
    earlier = lax.broadcasted_iota(jnp.int32, small, 0) < lax.broadcasted_iota(jnp.int32, small, 1)
    counts = jnp.broadcast_to(own_counts, small)
    inner_sum = jnp.sum(jnp.where(earlier, counts, 0), axis=0, keepdims=True)
    offsets_ref[...] = inner_sum + (reached - total_count)

    wait_bytes(landed.at[pl.ds(0, near_slots)], near_pair_sems.at[1])

    @pl.when(has_far)
    def _():
        wait_bytes(landed.at[pl.ds(0, far_slots)], far_pair_sems.at[1])

    ahead_of = [lax.rem(index // own_cap + pairs - group // 2, pairs) for index in range(half_cap)]

    def near_stage(c, carry):
        for index in range(half_cap):
            total = sums[c * half_cap + index]
            for at in range(index * JOBS, (index + 1) * JOBS, 2):
                left = jnp.concatenate(
                    [flat_r(codes[2 * row_count + c, x]) for x in (at, at + 1)], axis=1
                )
                right = jnp.concatenate(
                    [landed[codes[row_count + c, x]] for x in (at, at + 1)], axis=0
                )
                total = total + jnp.dot(left, right, preferred_element_type=jnp.float32)
            place = ahead_of[index] * row_count * own_cap + c * own_cap + index % own_cap
            out_ref[place] = total.astype(out_ref.dtype)
        return carry

    lax.fori_loop(0, row_count, near_stage, 0)

    wait_bytes(close.at[pl.ds(0, 2)], close_sems.at[0, 0])
    to_mate.wait_send()
    mate_a.wait_send()
    mate_r.wait_send()
    early_copy.wait_send()
    place_copy.wait_send()
    wait_bytes(packed, near_send.at[0])
    wait_bytes(told.at[pl.ds(0, groups - 1)], told_sems.at[0])
    wait_bytes(landed.at[pl.ds(0, near_slots)], near_pair_sems.at[0])

    @pl.when(has_onward)
    def _():
        wait_bytes(landed.at[pl.ds(0, far_slots)], far_send.at[0])

    @pl.when(has_far)
    def _():
        wait_bytes(close.at[pl.ds(2, 2)], close_sems.at[0, 1])
        wait_bytes(landed.at[pl.ds(0, far_slots)], far_pair_sems.at[0])

    for k in range(rounds):
        @pl.when(above_there[k])
        def _():
            scan_copy(k, 0).wait_send()

        @pl.when(below_there[k])
        def _():
            scan_copy(k, 1).wait_send()


def pair_sum_kernel(pairs, own, part_ref, landed, send_sems, recv_sems):
    row = lax.axis_index("rows")
    group = lax.axis_index("inner")
    core = lax.rem(group, 2)
    barrier = pltpu.get_barrier_semaphore()

    def place(ahead):
        return (row, 2 * lax.rem(group // 2 + ahead, pairs) + core)

    for ahead in range(1, pairs):
        pl.semaphore_signal(barrier, inc=1, device_id=place(ahead), device_id_type=MESH)
    pl.semaphore_wait(barrier, pairs - 1)
    copies = []
    for ahead in range(1, pairs):
        copy = pltpu.make_async_remote_copy(
            src_ref=part_ref.at[pl.ds(ahead * own, own)],
            dst_ref=landed.at[ahead - 1],
            send_sem=send_sems.at[ahead - 1],
            recv_sem=recv_sems.at[ahead - 1],
            device_id=place(ahead),
            device_id_type=MESH,
        )
        copy.start()
        copies.append(copy)
    for copy in copies:
        copy.wait()


def fused_body(rows, groups, r_tiles, r_cols, a_tiles, a_cols, c_cols, c_counts):
    local_rows, op_slots, tile, _ = a_tiles.shape
    row_count, r_slots = r_tiles.shape[:2]
    cap = c_cols.shape[1]
    tiles = local_rows * op_slots
    pairs = groups // 2
    own_cap = cap // groups
    half_cap = cap // 2
    width = -(-2 * tiles // 128) * 128
    list_slots = min(LIST_SLOTS, -(-tiles // CHUNK) * CHUNK)
    pass_slots = min(PASS_SLOTS, list_slots)
    dims = (rows, groups, local_rows, op_slots, r_slots, cap, width, list_slots, pass_slots, CHUNK)
    near_chunks = list_slots // CHUNK
    far_chunks = pass_slots // CHUNK
    near_slots = op_slots + list_slots
    far_slots = op_slots + pass_slots
    rounds = (rows - 1).bit_length()
    dtype = a_tiles.dtype
    out_dtype = jnp.bfloat16 if pairs == 1 else jnp.float32
    own = row_count * own_cap
    vmem = pl.BlockSpec(memory_space=pltpu.VMEM)
    anywhere = pl.BlockSpec(memory_space=pl.ANY)
    dma = pltpu.SemaphoreType.DMA
    block = (row_count, 128)
    part, offsets, flag = pl.pallas_call(
        functools.partial(fused_kernel, dims),
        out_shape=(
            jax.ShapeDtypeStruct((pairs * own, tile, tile), out_dtype),
            jax.ShapeDtypeStruct((1, row_count), jnp.int32),
            jax.ShapeDtypeStruct((1, 1), jnp.int32),
        ),
        in_specs=[anywhere] * 6,
        out_specs=(vmem, vmem, vmem),
        scratch_shapes=[
            pltpu.VMEM(r_cols.shape, jnp.int32),
            pltpu.VMEM(c_cols.shape, jnp.int32),
            pltpu.VMEM((1, row_count), jnp.int32),
            pltpu.VMEM((op_slots, a_cols.shape[0]), jnp.int32),
            pltpu.VMEM(block, jnp.int32),
            pltpu.VMEM((5,) + block, jnp.int32),
            pltpu.VMEM((2, 8, width), jnp.int32),
            pltpu.VMEM((2 * tiles + 1, tile, tile), dtype),
            pltpu.VMEM((2, row_count * r_slots, tile, tile), dtype),
            pltpu.VMEM((list_slots, tile, tile), dtype),
            pltpu.VMEM((2 * (near_slots + far_slots) + 1, tile, tile), dtype),
            pltpu.VMEM((row_count * half_cap, tile, tile), jnp.float32),
            pltpu.VMEM((3 * row_count, width), jnp.int32),
            pltpu.SMEM((3 * row_count, width), jnp.int32),
            pltpu.SMEM((8, width), jnp.int32),
            pltpu.VMEM((groups, 8, 128), jnp.int32),
            pltpu.VMEM((rounds, 8, 128), jnp.int32),
            pltpu.VMEM((rounds, 2, 8, 128), jnp.int32),
            dma((6,)),
            dma((2, 3)),
            dma((2, 2)),
            dma((2,)),
            dma((2,)),
            dma((near_chunks,)),
            dma((1,)),
            dma((2,)),
            dma((far_chunks + 1,)),
            dma((1,)),
            dma((2,)),
            dma((2,)),
            dma((2,)),
            dma((2, rounds, 2)),
        ],
        compiler_params=pltpu.CompilerParams(collective_id=40, has_side_effects=True),
        name="fused",
    )(
        r_cols,
        c_cols,
        c_counts[None, :],
        a_cols.T,
        a_tiles.reshape(tiles, tile, tile),
        r_tiles.reshape(row_count * r_slots, tile, tile),
    )
    if pairs == 1:
        c_tiles = part
    else:
        landed = pl.pallas_call(
            functools.partial(pair_sum_kernel, pairs, own),
            out_shape=jax.ShapeDtypeStruct((pairs - 1, own, tile, tile), jnp.float32),
            in_specs=[anywhere],
            out_specs=anywhere,
            scratch_shapes=[dma((pairs - 1,)), dma((pairs - 1,))],
            compiler_params=pltpu.CompilerParams(collective_id=41, has_side_effects=True),
            name="pair_sums",
        )(part)
        c_tiles = part[:own]
        for ahead in range(pairs - 1):
            c_tiles = c_tiles + landed[ahead]
        c_tiles = c_tiles.astype(jnp.bfloat16)
    return c_tiles.reshape(row_count, own_cap, tile, tile), offsets[0], flag[0, 0]


def body(rows, groups, *args):
    if rows % 2 or groups % 2:
        return plain_body(rows, groups, *args)
    c_tiles, offsets, flag = fused_body(rows, groups, *args)

    def again(c_tiles, offsets, *args):
        return plain_body(rows, groups, *args)

    def keep(c_tiles, offsets, *args):
        return c_tiles, offsets

    return lax.cond(flag > 0, again, keep, c_tiles, offsets, *args)


def solution(mesh):
    rows = mesh.shape["rows"]
    groups = mesh.shape["inner"]
    return jax.shard_map(
        functools.partial(body, rows, groups),
        mesh=mesh,
        in_specs=(
            P("rows", "inner", None, None),
            P("rows", "inner"),
            P(("rows", "inner"), None, None, None),
            P(),
            P("rows", None),
            P("rows"),
        ),
        out_specs=(P("rows", "inner", None, None), P("rows")),
        check_vma=False,
    )
```

```python
import functools

import jax
import jax.numpy as jnp
from jax import lax
from jax.experimental import pallas as pl
from jax.experimental.pallas import tpu as pltpu
from jax.sharding import PartitionSpec as P

MESH = pl.DeviceIdType.MESH
BATCH = 4


def plan_kernel(
    dims, r_cols_ref, c_cols_ref, counts_ref, columns_ref, code_ref, plan_ref,
    meta_ref, gathered, needs, send_sem, recv_sem,
):
    rows, groups, local_rows, op_slots, r_slots, cap, half = dims
    width = 2 * half
    count = rows * groups
    tiles = local_rows * op_slots
    row = lax.axis_index("rows")
    group = lax.axis_index("inner")
    me = row * groups + group

    barrier = pltpu.get_barrier_semaphore()

    def place(step):
        other = lax.rem(me + step, count)
        return (other // groups, lax.rem(other, groups))

    def greet(step, carry):
        pl.semaphore_signal(barrier, inc=1, device_id=place(step), device_id_type=MESH)
        return carry

    lax.fori_loop(1, count, greet, 0)
    row_count = r_cols_ref.shape[0]
    live = r_slots + cap
    lanes = lax.broadcasted_iota(jnp.int32, (row_count, width), 1)
    above = lax.broadcasted_iota(jnp.int32, (row_count, width), 0)
    small = (row_count, row_count)
    diagonal = lax.broadcasted_iota(jnp.int32, small, 0) == lax.broadcasted_iota(jnp.int32, small, 1)
    spread_counts = jnp.broadcast_to(counts_ref[...], small)
    own_counts = jnp.sum(jnp.where(diagonal, spread_counts, 0), axis=1, keepdims=True)
    meta_ref[...] = jnp.full(meta_ref.shape, -9, jnp.int32)
    meta_ref[:, 0:r_slots] = r_cols_ref[...]
    meta_ref[:, r_slots:live] = c_cols_ref[...]
    meta_ref[:, live : live + 1] = own_counts
    gathered[me] = meta_ref[...]
    pl.semaphore_wait(barrier, count - 1)

    def post(step, carry):
        pltpu.make_async_remote_copy(
            src_ref=meta_ref,
            dst_ref=gathered.at[me],
            send_sem=send_sem,
            recv_sem=recv_sem,
            device_id=place(step),
            device_id_type=MESH,
        ).start()
        return carry

    lax.fori_loop(1, count, post, 0)
    everyone = gathered.at[pl.ds(0, count - 1)]
    pltpu.make_async_copy(everyone, everyone, send_sem).wait()
    pltpu.make_async_copy(everyone, everyone, recv_sem).wait()

    def matches(block, columns, fine_rows):
        named = fine_rows == block[:, 0:1]
        for j in range(1, r_slots):
            named = named | (fine_rows == block[:, j : j + 1])
        slot = jnp.full((row_count, width), -1, jnp.int32)
        for s in range(cap):
            slot = jnp.where(columns == block[:, r_slots + s : r_slots + s + 1], s, slot)
        return jnp.where(named, slot, -1)

    shift = jnp.where(lanes < half, -groups, groups) * local_rows
    tile = jnp.where(lanes < half, lanes, lanes - half)
    lane_rows = jnp.where(tile < tiles, shift + tile // op_slots, -(1 << 24))
    low_lanes = lanes[0:1] < half

    def near_matches(device):
        before = columns_ref[pl.ds(jnp.maximum(device - groups, 0), 1), :]
        after = columns_ref[pl.ds(jnp.minimum(device + groups, count - 1), 1), :]
        columns = jnp.where(low_lanes, before, after)
        return matches(gathered[device], columns, lane_rows + device * local_rows)

    def wanted(found):
        return jnp.max((found >= 0).astype(jnp.int32), axis=0, keepdims=True)

    def gather_needs(device, carry):
        needs[pl.ds(device, 1), :] = wanted(near_matches(device))
        return carry

    lax.fori_loop(0, count, gather_needs, 0, unroll=4)
    every = needs[...]
    low_side = lax.broadcasted_iota(jnp.int32, every.shape, 1) < half
    low = jnp.sum(jnp.where(low_side, every, 0), axis=1, keepdims=True)
    high = jnp.sum(jnp.where(low_side, 0, every), axis=1, keepdims=True)
    most = jnp.max(jnp.maximum(low, high), axis=0, keepdims=True)

    down = lax.broadcasted_iota(jnp.int32, (width, width), 0)
    across = lax.broadcasted_iota(jnp.int32, (width, width), 1)
    same = (down < half) == (across < half)

    def ranks(need):
        spread = jnp.broadcast_to(need, (width, width))
        column = jnp.sum(jnp.where(down == across, spread, 0), axis=1, keepdims=True)
        before = jnp.sum(jnp.where((across < down) & same, spread, 0), axis=1, keepdims=True)
        along = jnp.sum(
            jnp.where((down < across) & same, jnp.broadcast_to(column, (width, width)), 0),
            axis=0,
            keepdims=True,
        )
        return column, before, along

    def send_list(device, high):
        column, before, _ = ranks(needs[pl.ds(device, 1), :])
        first = half if high else 0
        mine = (down >= half) if high else (down < half)
        chosen = mine & (column > 0) & (before == across)
        return jnp.sum(jnp.where(chosen, down - first, 0), axis=0, keepdims=True)

    left = jnp.maximum(row - 1, 0) * groups + group
    right = jnp.minimum(row + 1, rows - 1) * groups + group
    plan_ref[0:1, :] = send_list(left, True)
    plan_ref[1:2, :] = send_list(right, False)

    found = near_matches(me)
    _, _, along = ranks(wanted(found))
    slot_at = along + jnp.where(lanes[0:1] < half, tiles, 2 * tiles)
    code_ref[:, 0:width] = jnp.where(found >= 0, found + cap * slot_at, -1)
    fine = me * local_rows + jnp.where(lanes < tiles, lanes // op_slots, 0)
    fine = jnp.where(lanes < tiles, fine, -5)
    found = matches(gathered[me], columns_ref[pl.ds(me, 1), :], fine)
    code_ref[:, width:] = jnp.where(found >= 0, found + cap * lanes, -1)

    def earlier(index, total):
        block = gathered[index * groups]
        return total + jnp.sum(block[:, live : live + 1], axis=0, keepdims=True)

    first = lax.fori_loop(0, row, earlier, jnp.zeros((1, 1), jnp.int32))
    counts = jnp.broadcast_to(own_counts, (row_count, width))
    inner_sum = jnp.sum(jnp.where(above < lanes, counts, 0), axis=0, keepdims=True)
    plan_ref[2:3, :] = inner_sum + first
    level = jnp.zeros((1, 1), jnp.int32)
    for size in sizes_for(tiles)[:-1]:
        level = level + (most > size).astype(jnp.int32)
    plan_ref[3:4, :] = jnp.broadcast_to(level, (1, width))


def halo_kernel(rows, size, plan_ref, a_ref, out_ref, packed, send_sems, recv_sems):
    row = lax.axis_index("rows")
    group = lax.axis_index("inner")
    barrier = pltpu.get_barrier_semaphore()
    has_left = row > 0
    has_right = row < rows - 1

    @pl.when(has_left)
    def _():
        pl.semaphore_signal(barrier, inc=1, device_id=(row - 1, group), device_id_type=MESH)

    @pl.when(has_right)
    def _():
        pl.semaphore_signal(barrier, inc=1, device_id=(row + 1, group), device_id_type=MESH)

    def pack(index, carry):
        packed[0, index] = a_ref[plan_ref[0, index]]
        packed[1, index] = a_ref[plan_ref[1, index]]
        return carry

    lax.fori_loop(0, size, pack, 0, unroll=2)

    pl.semaphore_wait(barrier, has_left.astype(jnp.int32) + has_right.astype(jnp.int32))

    def copy(side, other):
        return pltpu.make_async_remote_copy(
            src_ref=packed.at[side],
            dst_ref=out_ref.at[1 - side, pl.ds(0, size)],
            send_sem=send_sems.at[side],
            recv_sem=recv_sems.at[1 - side],
            device_id=(other, group),
            device_id_type=MESH,
        )

    @pl.when(has_left)
    def _():
        copy(0, row - 1).start()

    @pl.when(has_right)
    def _():
        copy(1, row + 1).start()

    @pl.when(has_left)
    def _():
        copy(0, row - 1).wait_send()
        copy(1, row - 1).wait_recv()

    @pl.when(has_right)
    def _():
        copy(1, row + 1).wait_send()
        copy(0, row + 1).wait_recv()


def product_kernel(dims, code_ref, cols_ref, r_ref, a_ref, halo_ref, out_ref, tiles_ref, jobs, sems):
    rows, groups, local_rows, op_slots, r_slots, cap, half = dims
    width = 2 * half
    tiles = local_rows * op_slots
    row_count = cols_ref.shape[0]
    own_cap = cap // groups
    row = lax.axis_index("rows")
    group = lax.axis_index("inner")
    own = pltpu.make_async_copy(a_ref, tiles_ref.at[pl.ds(0, tiles)], sems.at[0])
    near = pltpu.make_async_copy(halo_ref, tiles_ref.at[pl.ds(tiles, 2 * tiles)], sems.at[1])
    own.start()
    near.start()
    last = groups * row_count * own_cap
    scale = 1 << (3 * tiles * cap - 1).bit_length()

    def clear(index, carry):
        out_ref[index] = jnp.zeros(out_ref.shape[1:], jnp.float32)
        return carry

    lax.fori_loop(0, last, clear, 0, unroll=4)

    def list_row(c, found):
        def list_slot(j, found):
            fine = cols_ref[c, j]
            side = fine // (local_rows * groups) - row
            base = jnp.where(side == 0, width, jnp.where(side < 0, 0, half))
            base = base + lax.rem(fine, local_rows) * op_slots
            for t in range(op_slots):
                code = code_ref[c, base + t]
                jobs[found] = (c * r_slots + j) * scale + code
                found = found + (code >= 0).astype(jnp.int32)
            return found

        return lax.fori_loop(0, r_slots, list_slot, found)

    found = lax.fori_loop(0, row_count, list_row, jnp.int32(0))
    for extra in range(BATCH):
        jobs[found + extra] = -1
    own.wait()
    near.wait()

    def batch(step, carry):
        results = []
        targets = []
        for extra in range(BATCH):
            job = jobs[step * BATCH + extra]
            valid = job >= 0
            job = jnp.maximum(job, 0)
            pair = job // scale
            code = lax.rem(job, scale)
            slot = lax.rem(code, cap)
            ahead = lax.rem(slot // own_cap + groups - group, groups)
            target = (ahead * row_count + pair // r_slots) * own_cap + lax.rem(slot, own_cap)
            targets.append(jnp.where(valid, target, last))
            results.append(
                jnp.dot(
                    r_ref[pair],
                    tiles_ref[code // cap],
                    preferred_element_type=jnp.float32,
                )
            )
        for extra in range(BATCH):
            target = targets[extra]
            out_ref[target] = out_ref[target] + results[extra]
        return carry

    lax.fori_loop(0, (found + BATCH - 1) // BATCH, batch, 0)


def sum_kernel(groups, own, part_ref, landed, send_sems, recv_sems):
    row = lax.axis_index("rows")
    group = lax.axis_index("inner")
    barrier = pltpu.get_barrier_semaphore()
    for ahead in range(1, groups):
        pl.semaphore_signal(
            barrier, inc=1, device_id=(row, lax.rem(group + ahead, groups)), device_id_type=MESH
        )
    pl.semaphore_wait(barrier, groups - 1)
    copies = []
    for ahead in range(1, groups):
        copy = pltpu.make_async_remote_copy(
            src_ref=part_ref.at[pl.ds(ahead * own, own)],
            dst_ref=landed.at[ahead - 1],
            send_sem=send_sems.at[ahead - 1],
            recv_sem=recv_sems.at[ahead - 1],
            device_id=(row, lax.rem(group + ahead, groups)),
            device_id_type=MESH,
        )
        copy.start()
        copies.append(copy)
    for copy in copies:
        copy.wait()


def sizes_for(tiles):
    steps = [16, 18, 20, 21, 22, 23, 24, 25, 26, 27, 28, 29, 30, 32, 36, 42]
    return [size for size in steps if size < tiles] + [tiles]


def plain_body(rows, groups, r_tiles, r_cols, a_tiles, a_cols, c_cols, c_counts):
    local_rows, op_slots, tile, _ = a_tiles.shape
    row_count, r_slots = r_tiles.shape[:2]
    cap = c_cols.shape[1]
    tiles = local_rows * op_slots
    half = -(-tiles // 64) * 64
    width = 2 * half
    count = rows * groups
    own_cap = cap // groups
    dims = (rows, groups, local_rows, op_slots, r_slots, cap, half)
    vmem = pl.BlockSpec(memory_space=pltpu.VMEM)
    smem = pl.BlockSpec(memory_space=pltpu.SMEM)
    anywhere = pl.BlockSpec(memory_space=pl.ANY)

    flat = a_cols.reshape(count, tiles)
    flat = jnp.pad(flat, ((0, 0), (0, half - tiles)), constant_values=-2)
    columns = jnp.concatenate([flat, flat], axis=1)

    code, plan = pl.pallas_call(
        functools.partial(plan_kernel, dims),
        out_shape=(
            jax.ShapeDtypeStruct((row_count, 2 * width), jnp.int32),
            jax.ShapeDtypeStruct((8, width), jnp.int32),
        ),
        in_specs=[vmem] * 4,
        out_specs=(vmem, vmem),
        scratch_shapes=[
            pltpu.VMEM((row_count, width), jnp.int32),
            pltpu.VMEM((count, row_count, width), jnp.int32),
            pltpu.VMEM((count, width), jnp.int32),
            pltpu.SemaphoreType.DMA,
            pltpu.SemaphoreType.DMA,
        ],
        compiler_params=pltpu.CompilerParams(collective_id=0, has_side_effects=True),
        name="plan",
    )(r_cols, c_cols, c_counts[None, :], columns)

    flat_a = a_tiles.reshape(tiles, tile, tile)
    sizes = sizes_for(tiles)

    def exchange(number, size, plan, flat_a):
        return pl.pallas_call(
            functools.partial(halo_kernel, rows, size),
            out_shape=jax.ShapeDtypeStruct((2, tiles, tile, tile), a_tiles.dtype),
            in_specs=[smem, vmem],
            out_specs=anywhere,
            scratch_shapes=[
                pltpu.VMEM((2, size, tile, tile), a_tiles.dtype),
                pltpu.SemaphoreType.DMA((2,)),
                pltpu.SemaphoreType.DMA((2,)),
            ],
            compiler_params=pltpu.CompilerParams(collective_id=number + 2, has_side_effects=True),
            name=f"halo{size}",
        )(plan, flat_a)

    halo = lax.switch(
        plan[3, 0],
        [functools.partial(exchange, number, size) for number, size in enumerate(sizes)],
        plan,
        flat_a,
    )

    slots = row_count * r_slots * op_slots + BATCH
    partial_value = pl.pallas_call(
        functools.partial(product_kernel, dims),
        out_shape=jax.ShapeDtypeStruct((row_count * cap + 1, tile, tile), jnp.float32),
        in_specs=[smem, smem, vmem, anywhere, anywhere],
        out_specs=vmem,
        scratch_shapes=[
            pltpu.VMEM((3 * tiles, tile, tile), a_tiles.dtype),
            pltpu.SMEM((slots,), jnp.int32),
            pltpu.SemaphoreType.DMA((2,)),
        ],
        name="products",
    )(
        code,
        r_cols,
        r_tiles.reshape(row_count * r_slots, tile, tile),
        flat_a,
        halo.reshape(2 * tiles, tile, tile),
    )

    own_count = row_count * own_cap
    landed = pl.pallas_call(
        functools.partial(sum_kernel, groups, own_count),
        out_shape=jax.ShapeDtypeStruct((groups - 1, own_count, tile, tile), jnp.float32),
        in_specs=[anywhere],
        out_specs=anywhere,
        scratch_shapes=[
            pltpu.SemaphoreType.DMA((groups - 1,)),
            pltpu.SemaphoreType.DMA((groups - 1,)),
        ],
        compiler_params=pltpu.CompilerParams(collective_id=1, has_side_effects=True),
        name="sums",
    )(partial_value)
    c_tiles = partial_value[:own_count]
    for ahead in range(groups - 1):
        c_tiles = c_tiles + landed[ahead]
    c_tiles = c_tiles.astype(jnp.bfloat16)
    return (c_tiles.reshape(row_count, own_cap, tile, tile), plan[2, :row_count])

LIST_SLOTS = 27
PASS_SLOTS = 15
CHUNK = 3
JOBS = 6
REMOTE = 1 << 14


def fused_kernel(
    dims, r_cols_hbm, c_cols_hbm, counts_hbm, columns_hbm, a_ref, r_ref,
    out_ref, offsets_ref, flag_ref,
    r_cols_ref, c_cols_ref, counts_ref, columns_ref,
    meta, close, placing, pair_a, pair_r, packed, landed, sums, tables, codes, picks,
    told, scan_out, scan_in,
    local_sems, close_sems, pair_sems, place_sems, early_sems, near_sems, near_send,
    near_pair_sems, far_sems, far_send, far_pair_sems, table_sems, told_sems, scan_sems,
):
    (rows, groups, local_rows, op_slots, r_slots, cap, width, list_slots, pass_slots, chunk) = dims
    pairs = groups // 2
    tiles = local_rows * op_slots
    span = 2 * local_rows
    own_cap = cap // groups
    half_cap = cap // 2
    both = 2 * r_slots
    row_count = r_cols_ref.shape[0]
    live = r_slots + cap
    early = op_slots
    near_slots = early + list_slots
    far_slots = early + pass_slots
    near_chunks = list_slots // chunk
    far_chunks = pass_slots // chunk
    far_base = 2 * near_slots
    zero_near = 2 * (near_slots + far_slots)
    zero_own = 2 * tiles
    rounds = (rows - 1).bit_length()
    order = [*range(1, rounds), 0]

    row = lax.axis_index("rows")
    group = lax.axis_index("inner")
    part = lax.rem(group, 2)
    first_group = group - part
    mate = first_group + 1 - part
    odd = lax.rem(row, 2)
    near = row + 1 - 2 * odd
    far = row - 1 + 2 * odd
    has_far = (far >= 0) & (far < rows)
    onward = near + 1 - 2 * odd
    has_onward = (onward >= 0) & (onward < rows)
    mate_place = (row, mate)

    barrier = pltpu.get_barrier_semaphore()

    def greet(place):
        pl.semaphore_signal(barrier, inc=1, device_id=place, device_id_type=MESH)

    for core in range(2):
        greet((near, first_group + core))

    @pl.when(has_far)
    def _():
        for core in range(2):
            greet((far, first_group + core))

    for ahead in range(1, groups):
        greet((row, lax.rem(group + ahead, groups)))

    small_copies = [
        pltpu.make_async_copy(src, dst, local_sems.at[2 + index])
        for index, (src, dst) in enumerate(
            [
                (r_cols_hbm, r_cols_ref),
                (c_cols_hbm, c_cols_ref),
                (counts_hbm, counts_ref),
                (columns_hbm, columns_ref),
            ]
        )
    ]
    for copy in small_copies:
        copy.start()
    own_a = pltpu.make_async_copy(
        a_ref, pair_a.at[pl.ds(part * tiles, tiles)], local_sems.at[0]
    )
    own_r = pltpu.make_async_copy(r_ref, pair_r.at[pl.ds(part * row_count * r_slots, row_count * r_slots)], local_sems.at[1])
    own_a.start()
    own_r.start()

    def remote(src, dst, send_sem, recv_sem, place):
        return pltpu.make_async_remote_copy(
            src_ref=src, dst_ref=dst, send_sem=send_sem, recv_sem=recv_sem,
            device_id=place, device_id_type=MESH,
        )

    def wait_bytes(view, sem):
        pltpu.make_async_copy(view, view, sem).wait()

    small = (row_count, row_count)
    diagonal = lax.broadcasted_iota(jnp.int32, small, 0) == lax.broadcasted_iota(jnp.int32, small, 1)
    meta[...] = jnp.full(meta.shape, -9, jnp.int32)
    pair_a[zero_own] = jnp.zeros(pair_a.shape[1:], pair_a.dtype)
    landed[zero_near] = jnp.zeros(landed.shape[1:], landed.dtype)
    for copy in small_copies:
        copy.wait()
    spread_counts = jnp.broadcast_to(counts_ref[...], small)
    own_counts = jnp.sum(jnp.where(diagonal, spread_counts, 0), axis=1, keepdims=True)
    meta[:, 0:r_slots] = r_cols_ref[...]
    meta[:, r_slots:live] = c_cols_ref[...]
    pl.semaphore_wait(barrier, groups + 1 + 2 * has_far.astype(jnp.int32))

    def start_close(target, first, which):
        for core in range(2):
            remote(
                meta, close.at[first + part], close_sems.at[0, which], close_sems.at[1, which],
                (target, first_group + core),
            ).start()

    @pl.when(has_far)
    def _():
        start_close(far, 2, 1)

    start_close(near, 0, 0)
    to_mate = remote(meta, close.at[4], close_sems.at[0, 2], close_sems.at[1, 2], mate_place)
    to_mate.start()
    mate_a = remote(
        a_ref, pair_a.at[pl.ds(part * tiles, tiles)], pair_sems.at[0, 0], pair_sems.at[1, 0], mate_place
    )
    mate_a.start()

    own_a.wait()
    early_copy = remote(
        pair_a.at[pl.ds(part * tiles, early)], landed.at[pl.ds(part * near_slots, early)],
        early_sems.at[0], early_sems.at[1], (near, group),
    )
    early_copy.start()
    mate_r = remote(r_ref, pair_r.at[pl.ds(part * row_count * r_slots, row_count * r_slots)], pair_sems.at[0, 1], pair_sems.at[1, 1], mate_place)
    mate_r.start()

    lanes = lax.broadcasted_iota(jnp.int32, (1, width), 1)
    real = lanes < op_slots * span
    lane_slot = lanes // span
    lane_fine = jnp.where(real, lax.rem(lanes, span), -(1 << 24))
    lane_core = lax.rem(lanes, span) // local_rows
    lane_local = lax.rem(lanes, local_rows)
    lane_tile = lane_core * tiles + lane_local * op_slots + lane_slot
    late = jnp.where(lane_local > 0, 1, 0)

    def pair_columns(which_row):
        start = (which_row * groups + first_group) * local_rows
        block = start // 128
        values = columns_ref[:, pl.ds(pl.multiple_of(block * 128, 128), 128)]
        if width > 128:
            values = jnp.concatenate([values] * (width // 128), axis=1)
        offset = start - block * 128
        total = jnp.zeros((1, width), jnp.int32)
        for t in range(op_slots):
            moved = pltpu.roll(values[t : t + 1, :], lax.rem(t * span - offset + 128 * width, width), 1)
            total = jnp.where(lane_slot == t, moved, total)
        return jnp.where(real, total, -2)

    def pair_fine(which_row):
        return lane_fine + (which_row * groups + first_group) * local_rows

    def need_of(meta_low, meta_high, columns, fine):
        named = fine == meta_low[:, 0:1]
        for j in range(1, r_slots):
            named = named | (fine == meta_low[:, j : j + 1])
        for j in range(r_slots):
            named = named | (fine == meta_high[:, j : j + 1])
        wanted = columns == meta_low[:, r_slots : r_slots + 1]
        for s in range(1, cap):
            wanted = wanted | (columns == meta_low[:, r_slots + s : r_slots + s + 1])
        return jnp.max((named & wanted).astype(jnp.int32), axis=0, keepdims=True)

    def before(need):
        total = need
        step = 1
        while step < width:
            total = total + jnp.where(lanes >= step, pltpu.roll(total, step, 1), 0)
            step *= 2
        return total - need

    def landing(places, count, base, slots):
        fits = (places >= 0) & (places < 2 * count)
        at = lax.rem(places, 2) * slots + early + places // 2
        at = jnp.where(late > 0, jnp.where(fits, at, -1), lane_core * slots + lane_slot)
        return jnp.where(real & (at >= 0), REMOTE + base + at, -1)

    own_columns = pair_columns(row)
    own_fine = pair_fine(row)

    @pl.when(has_far)
    def _():
        wait_bytes(close.at[pl.ds(2, 2)], close_sems.at[1, 1])

    @pl.when(jnp.logical_not(has_far))
    def _():
        close[2] = jnp.full(close.shape[1:], -9, jnp.int32)
        close[3] = jnp.full(close.shape[1:], -9, jnp.int32)

    need_far = need_of(close[2], close[3], own_columns, own_fine) * late
    far_before = before(need_far)
    far_total = jnp.sum(need_far, axis=1, keepdims=True)
    wait_bytes(close.at[pl.ds(0, 2)], close_sems.at[1, 0])
    need_near = need_of(close[0], close[1], own_columns, own_fine) * late
    need_only = need_near * (1 - need_far)
    near_total = far_total + jnp.sum(need_only, axis=1, keepdims=True)
    places = jnp.where(
        need_far > 0, far_before, jnp.where(need_only > 0, before(need_only) + far_total, -1)
    )
    pick_rows = -(-list_slots // 8) * 8
    slot_down = lax.broadcasted_iota(jnp.int32, (pick_rows, width), 0)
    chosen = jnp.broadcast_to(places, (pick_rows, width)) == 2 * slot_down + part
    picked = jnp.sum(
        jnp.where(chosen, jnp.broadcast_to(lane_tile, (pick_rows, width)), 0), axis=1, keepdims=True
    )
    across = lax.broadcasted_iota(jnp.int32, (pick_rows, width), 1)
    pick_row = jnp.sum(
        jnp.where(slot_down == across, jnp.broadcast_to(picked, (pick_rows, width)), 0),
        axis=0, keepdims=True,
    )
    tables[0:8, :] = jnp.broadcast_to(pick_row, (8, width))
    pick_copy = pltpu.make_async_copy(tables.at[pl.ds(0, 8)], picks, table_sems.at[0])
    pick_copy.start()
    placing[0] = jnp.broadcast_to(landing(places, list_slots, 0, near_slots), placing.shape[1:])
    place_copy = remote(placing.at[0], placing.at[1], place_sems.at[0], place_sems.at[1], (near, group))
    place_copy.start()
    mate_a.wait_recv()
    pick_copy.wait()

    def near_view(index):
        return landed.at[pl.ds(part * near_slots + early + index * chunk, chunk)]

    def near_copy(index):
        return remote(
            packed.at[pl.ds(index * chunk, chunk)], near_view(index),
            near_send.at[0], near_sems.at[index], (near, group),
        )

    def pack(index):
        for extra in range(chunk):
            packed[index * chunk + extra] = pair_a[picks[0, index * chunk + extra]]

    pack(0)
    for index in range(near_chunks):
        if index + 1 < near_chunks:
            pack(index + 1)
        near_copy(index).start()

    def mate_copy(view, sems):
        return remote(view, view, sems.at[0], sems.at[1], mate_place)

    early_view = landed.at[pl.ds(part * near_slots, early)]
    early_far_view = landed.at[pl.ds(far_base + part * far_slots, early)]

    def far_view(index):
        return landed.at[pl.ds(far_base + part * far_slots + early + index * chunk, chunk)]

    early_far = remote(early_view, early_far_view, far_send.at[0], far_sems.at[far_chunks], (onward, group))

    def far_copy(index):
        return remote(
            near_view(index), far_view(index), far_send.at[0], far_sems.at[index], (onward, group)
        )

    def take_far(index):
        @pl.when(has_far)
        def _():
            if index < 0:
                early_far.wait_recv()
                mate_copy(early_far_view, far_pair_sems).start()
            else:
                far_copy(index).wait_recv()
                mate_copy(far_view(index), far_pair_sems).start()

    near_columns = pair_columns(near)
    near_fine = pair_fine(near)
    far_row = jnp.clip(far, 0, rows - 1)
    far_columns = pair_columns(far_row)
    far_fine = jnp.where(has_far, pair_fine(far_row), -(1 << 24))
    early_copy.wait_recv()

    @pl.when(has_onward)
    def _():
        early_far.start()

    mate_copy(early_view, near_pair_sems).start()
    to_mate.wait_recv()
    mine, other = meta[...], close[4]
    my_low = jnp.where(part == 0, mine, other)
    my_high = jnp.where(part == 0, other, mine)
    far_need = need_of(my_low, my_high, far_columns, far_fine) * late
    far_places = jnp.where(far_need > 0, before(far_need), -1)
    far_at = landing(far_places, pass_slots, far_base, far_slots)
    place_copy.wait_recv()
    near_at = placing[1][0:1, :]

    above = (row_count, width)
    table_lanes = lax.broadcasted_iota(jnp.int32, above, 1)
    own_at, near_at, far_at = [jnp.broadcast_to(x, above) for x in (lane_tile, near_at, far_at)]
    slot_own, slot_near, slot_far = [], [], []
    for index in range(half_cap):
        even = (2 * (index // own_cap)) * own_cap + index % own_cap
        low = my_low[:, r_slots + even : r_slots + even + 1]
        high = my_low[:, r_slots + even + own_cap : r_slots + even + own_cap + 1]
        column = jnp.where(part == 0, low, high)
        slot_own.append(jnp.where(own_columns == column, own_at, -1))
        slot_near.append(jnp.where(near_columns == column, near_at, -1))
        slot_far.append(jnp.where(far_columns == column, far_at, -1))
    code = jnp.full(above, -1, jnp.int32)
    for j in range(both):
        block = my_low if j < r_slots else my_high
        named = block[:, j % r_slots : j % r_slots + 1]
        in_own = own_fine == named
        in_near = near_fine == named
        in_far = far_fine == named
        for index in range(half_cap):
            found = jnp.where(in_own, slot_own[index], -1)
            found = jnp.where(in_near, slot_near[index], found)
            found = jnp.where(in_far, slot_far[index], found)
            best = jnp.max(found, axis=1, keepdims=True)
            code = jnp.where(table_lanes == index * both + j, best, code)
    tables[0:row_count, :] = jnp.where((code >= 0) & (code < REMOTE), code, zero_own)
    away = code >= REMOTE
    rank = away.astype(jnp.int32)
    table_j = lax.rem(table_lanes, both)
    step = 1
    while step < both:
        rank = rank + jnp.where(table_j >= step, pltpu.roll(rank, step, 1), 0)
        step *= 2
    crowded = jnp.max(jnp.max(rank, axis=1, keepdims=True), axis=0, keepdims=True)
    job = jnp.where(away, (code - REMOTE) * both + table_j, -1)
    rank = jnp.where(away, rank - 1 + (table_lanes // both) * JOBS, -1)
    short = jnp.full(above, -1, jnp.int32)
    for at in range(half_cap * JOBS):
        best = jnp.max(jnp.where(rank == at, job, -1), axis=1, keepdims=True)
        short = jnp.where(table_lanes == at, best, short)
    job_j = lax.rem(jnp.maximum(short, 0), both)
    job_c = lax.broadcasted_iota(jnp.int32, above, 0)
    job_r = (job_j // r_slots) * (row_count * r_slots) + job_c * r_slots + lax.rem(job_j, r_slots)
    tables[row_count : 2 * row_count, :] = jnp.where(short >= 0, short // both, zero_near)
    tables[2 * row_count : 3 * row_count, :] = job_r
    code_copy = pltpu.make_async_copy(tables, codes, table_sems.at[1])
    code_copy.start()

    over = jnp.maximum(near_total - 2 * list_slots, far_total - 2 * pass_slots)
    over = jnp.maximum(over, crowded - JOBS)
    over = (over > 0).astype(jnp.int32)
    told[group] = jnp.broadcast_to(over, told.shape[1:])

    def tell(ahead):
        return remote(
            told.at[group], told.at[group], told_sems.at[0], told_sems.at[1],
            (row, lax.rem(group + ahead, groups)),
        )

    for ahead in range(1, groups):
        tell(ahead).start()

    tile = pair_a.shape[1]
    total_count = jnp.sum(own_counts, axis=0, keepdims=True)

    def scan_copy(k, side):
        other = row + (1 << k) if side == 0 else row - (1 << k)
        return remote(
            scan_out.at[k], scan_in.at[k, side], scan_sems.at[0, k, side], scan_sems.at[1, k, side],
            (other, group),
        )

    scan_shape = scan_out.shape[1:]
    scan_lane = lax.broadcasted_iota(jnp.int32, scan_shape, 1)
    above_there = [row + (1 << k) < rows for k in range(rounds)]
    below_there = [row - (1 << k) >= 0 for k in range(rounds)]

    def scan_send(k, state):
        scan_out[k] = state

        @pl.when(above_there[k])
        def _():
            scan_copy(k, 0).start()

        @pl.when(below_there[k])
        def _():
            scan_copy(k, 1).start()

    def scan_take(k, state):
        @pl.when(below_there[k])
        def _():
            scan_copy(k, 0).wait_recv()

        @pl.when(above_there[k])
        def _():
            scan_copy(k, 1).wait_recv()

        below = jnp.where((scan_lane < 2) & below_there[k], scan_in[k, 0], 0)
        beyond = jnp.where((scan_lane == 2) & above_there[k], scan_in[k, 1], 0)
        return state + below + beyond

    wait_bytes(told.at[pl.ds(0, groups - 1)], told_sems.at[1])
    over = told[0]
    for other_group in range(1, groups):
        over = over + told[other_group]
    state = jnp.where(
        scan_lane == 0, jnp.broadcast_to(total_count, scan_shape),
        jnp.where(scan_lane < 3, over, 0),
    )
    scan_send(order[0], state)

    code_copy.wait()
    own_r.wait()
    mate_r.wait_recv()

    def own_stage(c, carry):
        for index in range(0, half_cap, 2):
            total = None
            for j in range(0, both, 2):
                left = jnp.concatenate(
                    [pair_r[x // r_slots * row_count * r_slots + c * r_slots + x % r_slots] for x in (j, j + 1)], axis=1
                )
                right = jnp.concatenate(
                    [
                        jnp.concatenate(
                            [pair_a[codes[c, slot * both + x]] for slot in (index, index + 1)], axis=1
                        )
                        for x in (j, j + 1)
                    ],
                    axis=0,
                )
                term = jnp.dot(left, right, preferred_element_type=jnp.float32)
                total = term if total is None else total + term
            sums[c * half_cap + index] = total[:, :tile]
            sums[c * half_cap + index + 1] = total[:, tile:]
        return carry

    lag = 3
    scans = 0
    for index in range(near_chunks):
        near_copy(index).wait_recv()
        if index < far_chunks:
            @pl.when(has_onward)
            def _():
                far_copy(index).start()
        mate_copy(near_view(index), near_pair_sems).start()
        if -1 <= index - lag < far_chunks:
            take_far(index - lag)
        lax.fori_loop(
            index * row_count // near_chunks, (index + 1) * row_count // near_chunks, own_stage, 0
        )
        if index > 0 and scans < rounds - 1:
            state = scan_take(order[scans], state)
            scans += 1
            scan_send(order[scans], state)
    for index in range(max(near_chunks - lag, -1), far_chunks):
        take_far(index)
    while scans < rounds:
        state = scan_take(order[scans], state)
        scans += 1
        if scans < rounds:
            scan_send(order[scans], state)

    flags = jnp.where((scan_lane == 1) | (scan_lane == 2), state, 0)
    flags = jnp.max(jnp.max(flags, axis=1, keepdims=True), axis=0, keepdims=True)
    flag_ref[...] = (flags > 0).astype(jnp.int32)
    reached = jnp.where(scan_lane == 0, state, 0)
    reached = jnp.max(jnp.max(reached, axis=1, keepdims=True), axis=0, keepdims=True)
    earlier = lax.broadcasted_iota(jnp.int32, small, 0) < lax.broadcasted_iota(jnp.int32, small, 1)
    counts = jnp.broadcast_to(own_counts, small)
    inner_sum = jnp.sum(jnp.where(earlier, counts, 0), axis=0, keepdims=True)
    offsets_ref[...] = inner_sum + (reached - total_count)

    wait_bytes(landed.at[pl.ds(0, near_slots)], near_pair_sems.at[1])

    @pl.when(has_far)
    def _():
        wait_bytes(landed.at[pl.ds(0, far_slots)], far_pair_sems.at[1])

    ahead_of = [lax.rem(index // own_cap + pairs - group // 2, pairs) for index in range(half_cap)]

    def near_stage(c, carry):
        for index in range(half_cap):
            jobs = range(index * JOBS, (index + 1) * JOBS)
            left = jnp.concatenate([pair_r[codes[2 * row_count + c, x]] for x in jobs], axis=1)
            right = jnp.concatenate([landed[codes[row_count + c, x]] for x in jobs], axis=0)
            total = sums[c * half_cap + index] + jnp.dot(
                left, right, preferred_element_type=jnp.float32
            )
            place = ahead_of[index] * row_count * own_cap + c * own_cap + index % own_cap
            out_ref[place] = total.astype(out_ref.dtype)
        return carry

    lax.fori_loop(0, row_count, near_stage, 0)

    wait_bytes(close.at[pl.ds(0, 2)], close_sems.at[0, 0])
    to_mate.wait_send()
    mate_a.wait_send()
    mate_r.wait_send()
    early_copy.wait_send()
    place_copy.wait_send()
    wait_bytes(packed, near_send.at[0])
    wait_bytes(told.at[pl.ds(0, groups - 1)], told_sems.at[0])
    wait_bytes(landed.at[pl.ds(0, near_slots)], near_pair_sems.at[0])

    @pl.when(has_onward)
    def _():
        wait_bytes(landed.at[pl.ds(0, far_slots)], far_send.at[0])

    @pl.when(has_far)
    def _():
        wait_bytes(close.at[pl.ds(2, 2)], close_sems.at[0, 1])
        wait_bytes(landed.at[pl.ds(0, far_slots)], far_pair_sems.at[0])

    for k in range(rounds):
        @pl.when(above_there[k])
        def _():
            scan_copy(k, 0).wait_send()

        @pl.when(below_there[k])
        def _():
            scan_copy(k, 1).wait_send()


def pair_sum_kernel(pairs, own, part_ref, landed, send_sems, recv_sems):
    row = lax.axis_index("rows")
    group = lax.axis_index("inner")
    core = lax.rem(group, 2)
    barrier = pltpu.get_barrier_semaphore()

    def place(ahead):
        return (row, 2 * lax.rem(group // 2 + ahead, pairs) + core)

    for ahead in range(1, pairs):
        pl.semaphore_signal(barrier, inc=1, device_id=place(ahead), device_id_type=MESH)
    pl.semaphore_wait(barrier, pairs - 1)
    copies = []
    for ahead in range(1, pairs):
        copy = pltpu.make_async_remote_copy(
            src_ref=part_ref.at[pl.ds(ahead * own, own)],
            dst_ref=landed.at[ahead - 1],
            send_sem=send_sems.at[ahead - 1],
            recv_sem=recv_sems.at[ahead - 1],
            device_id=place(ahead),
            device_id_type=MESH,
        )
        copy.start()
        copies.append(copy)
    for copy in copies:
        copy.wait()


def fused_body(rows, groups, r_tiles, r_cols, a_tiles, a_cols, c_cols, c_counts):
    local_rows, op_slots, tile, _ = a_tiles.shape
    row_count, r_slots = r_tiles.shape[:2]
    cap = c_cols.shape[1]
    tiles = local_rows * op_slots
    pairs = groups // 2
    own_cap = cap // groups
    half_cap = cap // 2
    width = -(-2 * tiles // 128) * 128
    list_slots = min(LIST_SLOTS, -(-tiles // CHUNK) * CHUNK)
    pass_slots = min(PASS_SLOTS, list_slots)
    dims = (rows, groups, local_rows, op_slots, r_slots, cap, width, list_slots, pass_slots, CHUNK)
    near_chunks = list_slots // CHUNK
    far_chunks = pass_slots // CHUNK
    near_slots = op_slots + list_slots
    far_slots = op_slots + pass_slots
    rounds = (rows - 1).bit_length()
    dtype = a_tiles.dtype
    out_dtype = jnp.bfloat16 if pairs == 1 else jnp.float32
    own = row_count * own_cap
    vmem = pl.BlockSpec(memory_space=pltpu.VMEM)
    anywhere = pl.BlockSpec(memory_space=pl.ANY)
    dma = pltpu.SemaphoreType.DMA
    block = (row_count, 128)
    part, offsets, flag = pl.pallas_call(
        functools.partial(fused_kernel, dims),
        out_shape=(
            jax.ShapeDtypeStruct((pairs * own, tile, tile), out_dtype),
            jax.ShapeDtypeStruct((1, row_count), jnp.int32),
            jax.ShapeDtypeStruct((1, 1), jnp.int32),
        ),
        in_specs=[anywhere] * 6,
        out_specs=(vmem, vmem, vmem),
        scratch_shapes=[
            pltpu.VMEM(r_cols.shape, jnp.int32),
            pltpu.VMEM(c_cols.shape, jnp.int32),
            pltpu.VMEM((1, row_count), jnp.int32),
            pltpu.VMEM((op_slots, a_cols.shape[0]), jnp.int32),
            pltpu.VMEM(block, jnp.int32),
            pltpu.VMEM((5,) + block, jnp.int32),
            pltpu.VMEM((2, 8, width), jnp.int32),
            pltpu.VMEM((2 * tiles + 1, tile, tile), dtype),
            pltpu.VMEM((2 * row_count * r_slots, tile, tile), dtype),
            pltpu.VMEM((list_slots, tile, tile), dtype),
            pltpu.VMEM((2 * (near_slots + far_slots) + 1, tile, tile), dtype),
            pltpu.VMEM((row_count * half_cap, tile, tile), jnp.float32),
            pltpu.VMEM((3 * row_count, width), jnp.int32),
            pltpu.SMEM((3 * row_count, width), jnp.int32),
            pltpu.SMEM((8, width), jnp.int32),
            pltpu.VMEM((groups, 8, 128), jnp.int32),
            pltpu.VMEM((rounds, 8, 128), jnp.int32),
            pltpu.VMEM((rounds, 2, 8, 128), jnp.int32),
            dma((6,)),
            dma((2, 3)),
            dma((2, 2)),
            dma((2,)),
            dma((2,)),
            dma((near_chunks,)),
            dma((1,)),
            dma((2,)),
            dma((far_chunks + 1,)),
            dma((1,)),
            dma((2,)),
            dma((2,)),
            dma((2,)),
            dma((2, rounds, 2)),
        ],
        compiler_params=pltpu.CompilerParams(collective_id=40, has_side_effects=True),
        name="fused",
    )(
        r_cols,
        c_cols,
        c_counts[None, :],
        a_cols.T,
        a_tiles.reshape(tiles, tile, tile),
        r_tiles.reshape(row_count * r_slots, tile, tile),
    )
    if pairs == 1:
        c_tiles = part
    else:
        landed = pl.pallas_call(
            functools.partial(pair_sum_kernel, pairs, own),
            out_shape=jax.ShapeDtypeStruct((pairs - 1, own, tile, tile), jnp.float32),
            in_specs=[anywhere],
            out_specs=anywhere,
            scratch_shapes=[dma((pairs - 1,)), dma((pairs - 1,))],
            compiler_params=pltpu.CompilerParams(collective_id=41, has_side_effects=True),
            name="pair_sums",
        )(part)
        c_tiles = part[:own]
        for ahead in range(pairs - 1):
            c_tiles = c_tiles + landed[ahead]
        c_tiles = c_tiles.astype(jnp.bfloat16)
    return c_tiles.reshape(row_count, own_cap, tile, tile), offsets[0], flag[0, 0]


def body(rows, groups, *args):
    if rows % 2 or groups % 2:
        return plain_body(rows, groups, *args)
    c_tiles, offsets, flag = fused_body(rows, groups, *args)

    def again(c_tiles, offsets, *args):
        return plain_body(rows, groups, *args)

    def keep(c_tiles, offsets, *args):
        return c_tiles, offsets

    return lax.cond(flag > 0, again, keep, c_tiles, offsets, *args)


def solution(mesh):
    rows = mesh.shape["rows"]
    groups = mesh.shape["inner"]
    return jax.shard_map(
        functools.partial(body, rows, groups),
        mesh=mesh,
        in_specs=(
            P("rows", "inner", None, None),
            P("rows", "inner"),
            P(("rows", "inner"), None, None, None),
            P(),
            P("rows", None),
            P("rows"),
        ),
        out_specs=(P("rows", "inner", None, None), P("rows")),
        check_vma=False,
    )
```

```python
import functools

import jax
import jax.numpy as jnp
from jax import lax
from jax.experimental import pallas as pl
from jax.experimental.pallas import tpu as pltpu
from jax.sharding import PartitionSpec as P

MESH = pl.DeviceIdType.MESH
BATCH = 4


def plan_kernel(
    dims, r_cols_ref, c_cols_ref, counts_ref, columns_ref, code_ref, plan_ref,
    meta_ref, gathered, needs, send_sem, recv_sem,
):
    rows, groups, local_rows, op_slots, r_slots, cap, half = dims
    width = 2 * half
    count = rows * groups
    tiles = local_rows * op_slots
    row = lax.axis_index("rows")
    group = lax.axis_index("inner")
    me = row * groups + group

    barrier = pltpu.get_barrier_semaphore()

    def place(step):
        other = lax.rem(me + step, count)
        return (other // groups, lax.rem(other, groups))

    def greet(step, carry):
        pl.semaphore_signal(barrier, inc=1, device_id=place(step), device_id_type=MESH)
        return carry

    lax.fori_loop(1, count, greet, 0)
    row_count = r_cols_ref.shape[0]
    live = r_slots + cap
    lanes = lax.broadcasted_iota(jnp.int32, (row_count, width), 1)
    above = lax.broadcasted_iota(jnp.int32, (row_count, width), 0)
    small = (row_count, row_count)
    diagonal = lax.broadcasted_iota(jnp.int32, small, 0) == lax.broadcasted_iota(jnp.int32, small, 1)
    spread_counts = jnp.broadcast_to(counts_ref[...], small)
    own_counts = jnp.sum(jnp.where(diagonal, spread_counts, 0), axis=1, keepdims=True)
    meta_ref[...] = jnp.full(meta_ref.shape, -9, jnp.int32)
    meta_ref[:, 0:r_slots] = r_cols_ref[...]
    meta_ref[:, r_slots:live] = c_cols_ref[...]
    meta_ref[:, live : live + 1] = own_counts
    gathered[me] = meta_ref[...]
    pl.semaphore_wait(barrier, count - 1)

    def post(step, carry):
        pltpu.make_async_remote_copy(
            src_ref=meta_ref,
            dst_ref=gathered.at[me],
            send_sem=send_sem,
            recv_sem=recv_sem,
            device_id=place(step),
            device_id_type=MESH,
        ).start()
        return carry

    lax.fori_loop(1, count, post, 0)
    everyone = gathered.at[pl.ds(0, count - 1)]
    pltpu.make_async_copy(everyone, everyone, send_sem).wait()
    pltpu.make_async_copy(everyone, everyone, recv_sem).wait()

    def matches(block, columns, fine_rows):
        named = fine_rows == block[:, 0:1]
        for j in range(1, r_slots):
            named = named | (fine_rows == block[:, j : j + 1])
        slot = jnp.full((row_count, width), -1, jnp.int32)
        for s in range(cap):
            slot = jnp.where(columns == block[:, r_slots + s : r_slots + s + 1], s, slot)
        return jnp.where(named, slot, -1)

    shift = jnp.where(lanes < half, -groups, groups) * local_rows
    tile = jnp.where(lanes < half, lanes, lanes - half)
    lane_rows = jnp.where(tile < tiles, shift + tile // op_slots, -(1 << 24))
    low_lanes = lanes[0:1] < half

    def near_matches(device):
        before = columns_ref[pl.ds(jnp.maximum(device - groups, 0), 1), :]
        after = columns_ref[pl.ds(jnp.minimum(device + groups, count - 1), 1), :]
        columns = jnp.where(low_lanes, before, after)
        return matches(gathered[device], columns, lane_rows + device * local_rows)

    def wanted(found):
        return jnp.max((found >= 0).astype(jnp.int32), axis=0, keepdims=True)

    def gather_needs(device, carry):
        needs[pl.ds(device, 1), :] = wanted(near_matches(device))
        return carry

    lax.fori_loop(0, count, gather_needs, 0, unroll=4)
    every = needs[...]
    low_side = lax.broadcasted_iota(jnp.int32, every.shape, 1) < half
    low = jnp.sum(jnp.where(low_side, every, 0), axis=1, keepdims=True)
    high = jnp.sum(jnp.where(low_side, 0, every), axis=1, keepdims=True)
    most = jnp.max(jnp.maximum(low, high), axis=0, keepdims=True)

    down = lax.broadcasted_iota(jnp.int32, (width, width), 0)
    across = lax.broadcasted_iota(jnp.int32, (width, width), 1)
    same = (down < half) == (across < half)

    def ranks(need):
        spread = jnp.broadcast_to(need, (width, width))
        column = jnp.sum(jnp.where(down == across, spread, 0), axis=1, keepdims=True)
        before = jnp.sum(jnp.where((across < down) & same, spread, 0), axis=1, keepdims=True)
        along = jnp.sum(
            jnp.where((down < across) & same, jnp.broadcast_to(column, (width, width)), 0),
            axis=0,
            keepdims=True,
        )
        return column, before, along

    def send_list(device, high):
        column, before, _ = ranks(needs[pl.ds(device, 1), :])
        first = half if high else 0
        mine = (down >= half) if high else (down < half)
        chosen = mine & (column > 0) & (before == across)
        return jnp.sum(jnp.where(chosen, down - first, 0), axis=0, keepdims=True)

    left = jnp.maximum(row - 1, 0) * groups + group
    right = jnp.minimum(row + 1, rows - 1) * groups + group
    plan_ref[0:1, :] = send_list(left, True)
    plan_ref[1:2, :] = send_list(right, False)

    found = near_matches(me)
    _, _, along = ranks(wanted(found))
    slot_at = along + jnp.where(lanes[0:1] < half, tiles, 2 * tiles)
    code_ref[:, 0:width] = jnp.where(found >= 0, found + cap * slot_at, -1)
    fine = me * local_rows + jnp.where(lanes < tiles, lanes // op_slots, 0)
    fine = jnp.where(lanes < tiles, fine, -5)
    found = matches(gathered[me], columns_ref[pl.ds(me, 1), :], fine)
    code_ref[:, width:] = jnp.where(found >= 0, found + cap * lanes, -1)

    def earlier(index, total):
        block = gathered[index * groups]
        return total + jnp.sum(block[:, live : live + 1], axis=0, keepdims=True)

    first = lax.fori_loop(0, row, earlier, jnp.zeros((1, 1), jnp.int32))
    counts = jnp.broadcast_to(own_counts, (row_count, width))
    inner_sum = jnp.sum(jnp.where(above < lanes, counts, 0), axis=0, keepdims=True)
    plan_ref[2:3, :] = inner_sum + first
    level = jnp.zeros((1, 1), jnp.int32)
    for size in sizes_for(tiles)[:-1]:
        level = level + (most > size).astype(jnp.int32)
    plan_ref[3:4, :] = jnp.broadcast_to(level, (1, width))


def halo_kernel(rows, size, plan_ref, a_ref, out_ref, packed, send_sems, recv_sems):
    row = lax.axis_index("rows")
    group = lax.axis_index("inner")
    barrier = pltpu.get_barrier_semaphore()
    has_left = row > 0
    has_right = row < rows - 1

    @pl.when(has_left)
    def _():
        pl.semaphore_signal(barrier, inc=1, device_id=(row - 1, group), device_id_type=MESH)

    @pl.when(has_right)
    def _():
        pl.semaphore_signal(barrier, inc=1, device_id=(row + 1, group), device_id_type=MESH)

    def pack(index, carry):
        packed[0, index] = a_ref[plan_ref[0, index]]
        packed[1, index] = a_ref[plan_ref[1, index]]
        return carry

    lax.fori_loop(0, size, pack, 0, unroll=2)

    pl.semaphore_wait(barrier, has_left.astype(jnp.int32) + has_right.astype(jnp.int32))

    def copy(side, other):
        return pltpu.make_async_remote_copy(
            src_ref=packed.at[side],
            dst_ref=out_ref.at[1 - side, pl.ds(0, size)],
            send_sem=send_sems.at[side],
            recv_sem=recv_sems.at[1 - side],
            device_id=(other, group),
            device_id_type=MESH,
        )

    @pl.when(has_left)
    def _():
        copy(0, row - 1).start()

    @pl.when(has_right)
    def _():
        copy(1, row + 1).start()

    @pl.when(has_left)
    def _():
        copy(0, row - 1).wait_send()
        copy(1, row - 1).wait_recv()

    @pl.when(has_right)
    def _():
        copy(1, row + 1).wait_send()
        copy(0, row + 1).wait_recv()


def product_kernel(dims, code_ref, cols_ref, r_ref, a_ref, halo_ref, out_ref, tiles_ref, jobs, sems):
    rows, groups, local_rows, op_slots, r_slots, cap, half = dims
    width = 2 * half
    tiles = local_rows * op_slots
    row_count = cols_ref.shape[0]
    own_cap = cap // groups
    row = lax.axis_index("rows")
    group = lax.axis_index("inner")
    own = pltpu.make_async_copy(a_ref, tiles_ref.at[pl.ds(0, tiles)], sems.at[0])
    near = pltpu.make_async_copy(halo_ref, tiles_ref.at[pl.ds(tiles, 2 * tiles)], sems.at[1])
    own.start()
    near.start()
    last = groups * row_count * own_cap
    scale = 1 << (3 * tiles * cap - 1).bit_length()

    def clear(index, carry):
        out_ref[index] = jnp.zeros(out_ref.shape[1:], jnp.float32)
        return carry

    lax.fori_loop(0, last, clear, 0, unroll=4)

    def list_row(c, found):
        def list_slot(j, found):
            fine = cols_ref[c, j]
            side = fine // (local_rows * groups) - row
            base = jnp.where(side == 0, width, jnp.where(side < 0, 0, half))
            base = base + lax.rem(fine, local_rows) * op_slots
            for t in range(op_slots):
                code = code_ref[c, base + t]
                jobs[found] = (c * r_slots + j) * scale + code
                found = found + (code >= 0).astype(jnp.int32)
            return found

        return lax.fori_loop(0, r_slots, list_slot, found)

    found = lax.fori_loop(0, row_count, list_row, jnp.int32(0))
    for extra in range(BATCH):
        jobs[found + extra] = -1
    own.wait()
    near.wait()

    def batch(step, carry):
        results = []
        targets = []
        for extra in range(BATCH):
            job = jobs[step * BATCH + extra]
            valid = job >= 0
            job = jnp.maximum(job, 0)
            pair = job // scale
            code = lax.rem(job, scale)
            slot = lax.rem(code, cap)
            ahead = lax.rem(slot // own_cap + groups - group, groups)
            target = (ahead * row_count + pair // r_slots) * own_cap + lax.rem(slot, own_cap)
            targets.append(jnp.where(valid, target, last))
            results.append(
                jnp.dot(
                    r_ref[pair],
                    tiles_ref[code // cap],
                    preferred_element_type=jnp.float32,
                )
            )
        for extra in range(BATCH):
            target = targets[extra]
            out_ref[target] = out_ref[target] + results[extra]
        return carry

    lax.fori_loop(0, (found + BATCH - 1) // BATCH, batch, 0)


def sum_kernel(groups, own, part_ref, landed, send_sems, recv_sems):
    row = lax.axis_index("rows")
    group = lax.axis_index("inner")
    barrier = pltpu.get_barrier_semaphore()
    for ahead in range(1, groups):
        pl.semaphore_signal(
            barrier, inc=1, device_id=(row, lax.rem(group + ahead, groups)), device_id_type=MESH
        )
    pl.semaphore_wait(barrier, groups - 1)
    copies = []
    for ahead in range(1, groups):
        copy = pltpu.make_async_remote_copy(
            src_ref=part_ref.at[pl.ds(ahead * own, own)],
            dst_ref=landed.at[ahead - 1],
            send_sem=send_sems.at[ahead - 1],
            recv_sem=recv_sems.at[ahead - 1],
            device_id=(row, lax.rem(group + ahead, groups)),
            device_id_type=MESH,
        )
        copy.start()
        copies.append(copy)
    for copy in copies:
        copy.wait()


def sizes_for(tiles):
    steps = [16, 18, 20, 21, 22, 23, 24, 25, 26, 27, 28, 29, 30, 32, 36, 42]
    return [size for size in steps if size < tiles] + [tiles]


def plain_body(rows, groups, r_tiles, r_cols, a_tiles, a_cols, c_cols, c_counts):
    local_rows, op_slots, tile, _ = a_tiles.shape
    row_count, r_slots = r_tiles.shape[:2]
    cap = c_cols.shape[1]
    tiles = local_rows * op_slots
    half = -(-tiles // 64) * 64
    width = 2 * half
    count = rows * groups
    own_cap = cap // groups
    dims = (rows, groups, local_rows, op_slots, r_slots, cap, half)
    vmem = pl.BlockSpec(memory_space=pltpu.VMEM)
    smem = pl.BlockSpec(memory_space=pltpu.SMEM)
    anywhere = pl.BlockSpec(memory_space=pl.ANY)

    flat = a_cols.reshape(count, tiles)
    flat = jnp.pad(flat, ((0, 0), (0, half - tiles)), constant_values=-2)
    columns = jnp.concatenate([flat, flat], axis=1)

    code, plan = pl.pallas_call(
        functools.partial(plan_kernel, dims),
        out_shape=(
            jax.ShapeDtypeStruct((row_count, 2 * width), jnp.int32),
            jax.ShapeDtypeStruct((8, width), jnp.int32),
        ),
        in_specs=[vmem] * 4,
        out_specs=(vmem, vmem),
        scratch_shapes=[
            pltpu.VMEM((row_count, width), jnp.int32),
            pltpu.VMEM((count, row_count, width), jnp.int32),
            pltpu.VMEM((count, width), jnp.int32),
            pltpu.SemaphoreType.DMA,
            pltpu.SemaphoreType.DMA,
        ],
        compiler_params=pltpu.CompilerParams(collective_id=0, has_side_effects=True),
        name="plan",
    )(r_cols, c_cols, c_counts[None, :], columns)

    flat_a = a_tiles.reshape(tiles, tile, tile)
    sizes = sizes_for(tiles)

    def exchange(number, size, plan, flat_a):
        return pl.pallas_call(
            functools.partial(halo_kernel, rows, size),
            out_shape=jax.ShapeDtypeStruct((2, tiles, tile, tile), a_tiles.dtype),
            in_specs=[smem, vmem],
            out_specs=anywhere,
            scratch_shapes=[
                pltpu.VMEM((2, size, tile, tile), a_tiles.dtype),
                pltpu.SemaphoreType.DMA((2,)),
                pltpu.SemaphoreType.DMA((2,)),
            ],
            compiler_params=pltpu.CompilerParams(collective_id=number + 2, has_side_effects=True),
            name=f"halo{size}",
        )(plan, flat_a)

    halo = lax.switch(
        plan[3, 0],
        [functools.partial(exchange, number, size) for number, size in enumerate(sizes)],
        plan,
        flat_a,
    )

    slots = row_count * r_slots * op_slots + BATCH
    partial_value = pl.pallas_call(
        functools.partial(product_kernel, dims),
        out_shape=jax.ShapeDtypeStruct((row_count * cap + 1, tile, tile), jnp.float32),
        in_specs=[smem, smem, vmem, anywhere, anywhere],
        out_specs=vmem,
        scratch_shapes=[
            pltpu.VMEM((3 * tiles, tile, tile), a_tiles.dtype),
            pltpu.SMEM((slots,), jnp.int32),
            pltpu.SemaphoreType.DMA((2,)),
        ],
        name="products",
    )(
        code,
        r_cols,
        r_tiles.reshape(row_count * r_slots, tile, tile),
        flat_a,
        halo.reshape(2 * tiles, tile, tile),
    )

    own_count = row_count * own_cap
    landed = pl.pallas_call(
        functools.partial(sum_kernel, groups, own_count),
        out_shape=jax.ShapeDtypeStruct((groups - 1, own_count, tile, tile), jnp.float32),
        in_specs=[anywhere],
        out_specs=anywhere,
        scratch_shapes=[
            pltpu.SemaphoreType.DMA((groups - 1,)),
            pltpu.SemaphoreType.DMA((groups - 1,)),
        ],
        compiler_params=pltpu.CompilerParams(collective_id=1, has_side_effects=True),
        name="sums",
    )(partial_value)
    c_tiles = partial_value[:own_count]
    for ahead in range(groups - 1):
        c_tiles = c_tiles + landed[ahead]
    c_tiles = c_tiles.astype(jnp.bfloat16)
    return (c_tiles.reshape(row_count, own_cap, tile, tile), plan[2, :row_count])

LIST_SLOTS = 27
PASS_SLOTS = 15
CHUNK = 3
JOBS = 4
REMOTE = 1 << 14


def fused_kernel(
    dims, r_cols_hbm, c_cols_hbm, counts_hbm, columns_hbm, a_ref, r_ref,
    out_ref, offsets_ref, flag_ref,
    r_cols_ref, c_cols_ref, counts_ref, columns_ref,
    meta, close, placing, pair_a, pair_r, packed, landed, sums, tables, codes, picks,
    told, scan_out, scan_in,
    local_sems, close_sems, pair_sems, place_sems, early_sems, near_sems, near_send,
    near_pair_sems, far_sems, far_send, far_pair_sems, table_sems, told_sems, scan_sems,
):
    (rows, groups, local_rows, op_slots, r_slots, cap, width, list_slots, pass_slots, chunk) = dims
    pairs = groups // 2
    tiles = local_rows * op_slots
    span = 2 * local_rows
    own_cap = cap // groups
    half_cap = cap // 2
    both = 2 * r_slots
    row_count = r_cols_ref.shape[0]
    live = r_slots + cap
    early = op_slots
    near_slots = early + list_slots
    far_slots = early + pass_slots
    near_chunks = list_slots // chunk
    far_chunks = pass_slots // chunk
    far_base = 2 * near_slots
    zero_near = 2 * (near_slots + far_slots)
    zero_own = 2 * tiles
    rounds = (rows - 1).bit_length()

    row = lax.axis_index("rows")
    group = lax.axis_index("inner")
    part = lax.rem(group, 2)
    first_group = group - part
    mate = first_group + 1 - part
    odd = lax.rem(row, 2)
    near = row + 1 - 2 * odd
    far = row - 1 + 2 * odd
    has_far = (far >= 0) & (far < rows)
    onward = near + 1 - 2 * odd
    has_onward = (onward >= 0) & (onward < rows)
    mate_place = (row, mate)

    barrier = pltpu.get_barrier_semaphore()

    def greet(place):
        pl.semaphore_signal(barrier, inc=1, device_id=place, device_id_type=MESH)

    for core in range(2):
        greet((near, first_group + core))

    @pl.when(has_far)
    def _():
        for core in range(2):
            greet((far, first_group + core))

    for ahead in range(1, groups):
        greet((row, lax.rem(group + ahead, groups)))

    small_copies = [
        pltpu.make_async_copy(src, dst, local_sems.at[2 + index])
        for index, (src, dst) in enumerate(
            [
                (r_cols_hbm, r_cols_ref),
                (c_cols_hbm, c_cols_ref),
                (counts_hbm, counts_ref),
                (columns_hbm, columns_ref),
            ]
        )
    ]
    for copy in small_copies:
        copy.start()
    own_a = pltpu.make_async_copy(
        a_ref, pair_a.at[pl.ds(part * tiles, tiles)], local_sems.at[0]
    )
    own_r = pltpu.make_async_copy(r_ref, pair_r.at[pl.ds(part * row_count * r_slots, row_count * r_slots)], local_sems.at[1])
    own_a.start()
    own_r.start()

    def remote(src, dst, send_sem, recv_sem, place):
        return pltpu.make_async_remote_copy(
            src_ref=src, dst_ref=dst, send_sem=send_sem, recv_sem=recv_sem,
            device_id=place, device_id_type=MESH,
        )

    def wait_bytes(view, sem):
        pltpu.make_async_copy(view, view, sem).wait()

    small = (row_count, row_count)
    diagonal = lax.broadcasted_iota(jnp.int32, small, 0) == lax.broadcasted_iota(jnp.int32, small, 1)
    meta[...] = jnp.full(meta.shape, -9, jnp.int32)
    pair_a[zero_own] = jnp.zeros(pair_a.shape[1:], pair_a.dtype)
    landed[zero_near] = jnp.zeros(landed.shape[1:], landed.dtype)
    for copy in small_copies:
        copy.wait()
    spread_counts = jnp.broadcast_to(counts_ref[...], small)
    own_counts = jnp.sum(jnp.where(diagonal, spread_counts, 0), axis=1, keepdims=True)
    meta[:, 0:r_slots] = r_cols_ref[...]
    meta[:, r_slots:live] = c_cols_ref[...]
    pl.semaphore_wait(barrier, groups + 1 + 2 * has_far.astype(jnp.int32))

    def start_close(target, first, which):
        for core in range(2):
            remote(
                meta, close.at[first + part], close_sems.at[0, which], close_sems.at[1, which],
                (target, first_group + core),
            ).start()

    @pl.when(has_far)
    def _():
        start_close(far, 2, 1)

    start_close(near, 0, 0)
    to_mate = remote(meta, close.at[4], close_sems.at[0, 2], close_sems.at[1, 2], mate_place)
    to_mate.start()
    mate_a = remote(
        a_ref, pair_a.at[pl.ds(part * tiles, tiles)], pair_sems.at[0, 0], pair_sems.at[1, 0], mate_place
    )
    mate_a.start()

    own_a.wait()
    early_copy = remote(
        pair_a.at[pl.ds(part * tiles, early)], landed.at[pl.ds(part * near_slots, early)],
        early_sems.at[0], early_sems.at[1], (near, group),
    )
    early_copy.start()
    mate_r = remote(r_ref, pair_r.at[pl.ds(part * row_count * r_slots, row_count * r_slots)], pair_sems.at[0, 1], pair_sems.at[1, 1], mate_place)
    mate_r.start()

    lanes = lax.broadcasted_iota(jnp.int32, (1, width), 1)
    real = lanes < op_slots * span
    lane_slot = lanes // span
    lane_fine = jnp.where(real, lax.rem(lanes, span), -(1 << 24))
    lane_core = lax.rem(lanes, span) // local_rows
    lane_local = lax.rem(lanes, local_rows)
    lane_tile = lane_core * tiles + lane_local * op_slots + lane_slot
    late = jnp.where(lane_local > 0, 1, 0)

    def pair_columns(which_row):
        start = (which_row * groups + first_group) * local_rows
        block = start // 128
        values = columns_ref[:, pl.ds(pl.multiple_of(block * 128, 128), 128)]
        if width > 128:
            values = jnp.concatenate([values] * (width // 128), axis=1)
        offset = start - block * 128
        total = jnp.zeros((1, width), jnp.int32)
        for t in range(op_slots):
            moved = pltpu.roll(values[t : t + 1, :], lax.rem(t * span - offset + 128 * width, width), 1)
            total = jnp.where(lane_slot == t, moved, total)
        return jnp.where(real, total, -2)

    def pair_fine(which_row):
        return lane_fine + (which_row * groups + first_group) * local_rows

    def named_by(meta_low, meta_high, fine):
        named = fine == meta_low[:, 0:1]
        for j in range(1, r_slots):
            named = named | (fine == meta_low[:, j : j + 1])
        for j in range(r_slots):
            named = named | (fine == meta_high[:, j : j + 1])
        return named

    def need_of(meta_low, meta_high, columns, fine):
        named = named_by(meta_low, meta_high, fine)
        wanted = columns == meta_low[:, r_slots : r_slots + 1]
        for s in range(1, cap):
            wanted = wanted | (columns == meta_low[:, r_slots + s : r_slots + s + 1])
        return jnp.max((named & wanted).astype(jnp.int32), axis=0, keepdims=True)

    def before(need):
        total = need
        step = 1
        while step < width:
            total = total + jnp.where(lanes >= step, pltpu.roll(total, step, 1), 0)
            step *= 2
        return total - need

    def landing(places, count, base, slots):
        fits = (places >= 0) & (places < 2 * count)
        at = lax.rem(places, 2) * slots + early + places // 2
        at = jnp.where(late > 0, jnp.where(fits, at, -1), lane_core * slots + lane_slot)
        return jnp.where(real & (at >= 0), REMOTE + base + at, -1)

    own_columns = pair_columns(row)
    own_fine = pair_fine(row)

    @pl.when(has_far)
    def _():
        wait_bytes(close.at[pl.ds(2, 2)], close_sems.at[1, 1])

    @pl.when(jnp.logical_not(has_far))
    def _():
        close[2] = jnp.full(close.shape[1:], -9, jnp.int32)
        close[3] = jnp.full(close.shape[1:], -9, jnp.int32)

    need_far = need_of(close[2], close[3], own_columns, own_fine) * late
    far_before = before(need_far)
    far_total = jnp.sum(need_far, axis=1, keepdims=True)
    wait_bytes(close.at[pl.ds(0, 2)], close_sems.at[1, 0])
    need_near = need_of(close[0], close[1], own_columns, own_fine) * late
    need_only = need_near * (1 - need_far)
    near_total = far_total + jnp.sum(need_only, axis=1, keepdims=True)
    places = jnp.where(
        need_far > 0, far_before, jnp.where(need_only > 0, before(need_only) + far_total, -1)
    )
    pick_rows = -(-list_slots // 8) * 8
    slot_down = lax.broadcasted_iota(jnp.int32, (pick_rows, width), 0)
    chosen = jnp.broadcast_to(places, (pick_rows, width)) == 2 * slot_down + part
    picked = jnp.sum(
        jnp.where(chosen, jnp.broadcast_to(lane_tile, (pick_rows, width)), 0), axis=1, keepdims=True
    )
    across = lax.broadcasted_iota(jnp.int32, (pick_rows, width), 1)
    pick_row = jnp.sum(
        jnp.where(slot_down == across, jnp.broadcast_to(picked, (pick_rows, width)), 0),
        axis=0, keepdims=True,
    )
    tables[0:8, :] = jnp.broadcast_to(pick_row, (8, width))
    pick_copy = pltpu.make_async_copy(tables.at[pl.ds(0, 8)], picks, table_sems.at[0])
    pick_copy.start()
    placing[0] = jnp.broadcast_to(landing(places, list_slots, 0, near_slots), placing.shape[1:])
    place_copy = remote(placing.at[0], placing.at[1], place_sems.at[0], place_sems.at[1], (near, group))
    place_copy.start()
    near_columns = pair_columns(near)
    near_fine = pair_fine(near)
    far_row = jnp.clip(far, 0, rows - 1)
    far_columns = pair_columns(far_row)
    far_fine = jnp.where(has_far, pair_fine(far_row), -(1 << 24))
    to_mate.wait_recv()
    mine, other = meta[...], close[4]
    my_low = jnp.where(part == 0, mine, other)
    my_high = jnp.where(part == 0, other, mine)
    near_named = named_by(my_low, my_high, near_fine)
    far_named = named_by(my_low, my_high, far_fine)
    crowded = jnp.zeros((1, 1), jnp.int32)
    for s in range(cap):
        column = my_low[:, r_slots + s : r_slots + s + 1]
        hits = (near_named & (near_columns == column)).astype(jnp.int32)
        hits = hits + (far_named & (far_columns == column)).astype(jnp.int32)
        held = jnp.sum(hits, axis=1, keepdims=True)
        crowded = jnp.maximum(crowded, jnp.max(held, axis=0, keepdims=True))
    over = jnp.maximum(near_total - 2 * list_slots, far_total - 2 * pass_slots)
    over = jnp.maximum(over, crowded - JOBS)
    over = (over > 0).astype(jnp.int32)
    if groups > 2:
        told[group] = jnp.broadcast_to(over, told.shape[1:])

        def tell(ahead):
            return remote(
                told.at[group], told.at[group], told_sems.at[0], told_sems.at[1],
                (row, lax.rem(group + ahead, groups)),
            )

        for ahead in range(1, groups):
            tell(ahead).start()
        wait_bytes(told.at[pl.ds(0, groups - 1)], told_sems.at[1])
        over = told[0]
        for other_group in range(1, groups):
            over = over + told[other_group]

    tile = pair_a.shape[1]
    total_count = jnp.sum(own_counts, axis=0, keepdims=True)

    def scan_copy(k, side):
        other = row + (1 << k) if side == 0 else row - (1 << k)
        return remote(
            scan_out.at[k], scan_in.at[k, side], scan_sems.at[0, k, side], scan_sems.at[1, k, side],
            (other, group),
        )

    scan_shape = scan_out.shape[1:]
    scan_lane = lax.broadcasted_iota(jnp.int32, scan_shape, 1)
    above_there = [row + (1 << k) < rows for k in range(rounds)]
    below_there = [row - (1 << k) >= 0 for k in range(rounds)]

    def scan_send(k, state):
        scan_out[k] = state

        @pl.when(above_there[k])
        def _():
            scan_copy(k, 0).start()

        @pl.when(below_there[k])
        def _():
            scan_copy(k, 1).start()

    def scan_take(k, state):
        @pl.when(below_there[k])
        def _():
            scan_copy(k, 0).wait_recv()

        @pl.when(above_there[k])
        def _():
            scan_copy(k, 1).wait_recv()

        below = jnp.where((scan_lane < 2) & below_there[k], scan_in[k, 0], 0)
        beyond = jnp.where((scan_lane == 2) & above_there[k], scan_in[k, 1], 0)
        return state + below + beyond

    state = jnp.where(
        scan_lane == 0, jnp.broadcast_to(total_count, scan_shape),
        jnp.where(scan_lane < 3, over, 0),
    )
    scan_send(0, state)
    scans = 0

    def scan_step():
        nonlocal state, scans
        state = scan_take(scans, state)
        scans += 1
        if scans < rounds:
            scan_send(scans, state)

    mate_a.wait_recv()
    pick_copy.wait()

    def near_view(index):
        return landed.at[pl.ds(part * near_slots + early + index * chunk, chunk)]

    def near_copy(index):
        return remote(
            packed.at[pl.ds(index * chunk, chunk)], near_view(index),
            near_send.at[0], near_sems.at[index], (near, group),
        )

    def pack(index):
        for extra in range(chunk):
            packed[index * chunk + extra] = pair_a[picks[0, index * chunk + extra]]

    pack(0)
    for index in range(near_chunks):
        if index + 1 < near_chunks:
            pack(index + 1)
        near_copy(index).start()

    def mate_copy(view, sems):
        return remote(view, view, sems.at[0], sems.at[1], mate_place)

    early_view = landed.at[pl.ds(part * near_slots, early)]
    early_far_view = landed.at[pl.ds(far_base + part * far_slots, early)]

    def far_view(index):
        return landed.at[pl.ds(far_base + part * far_slots + early + index * chunk, chunk)]

    early_far = remote(early_view, early_far_view, far_send.at[0], far_sems.at[far_chunks], (onward, group))

    def far_copy(index):
        return remote(
            near_view(index), far_view(index), far_send.at[0], far_sems.at[index], (onward, group)
        )

    def take_far(index):
        @pl.when(has_far)
        def _():
            if index < 0:
                early_far.wait_recv()
                mate_copy(early_far_view, far_pair_sems).start()
            else:
                far_copy(index).wait_recv()
                mate_copy(far_view(index), far_pair_sems).start()

    early_copy.wait_recv()

    @pl.when(has_onward)
    def _():
        early_far.start()

    mate_copy(early_view, near_pair_sems).start()
    if scans < rounds:
        scan_step()
    far_need = need_of(my_low, my_high, far_columns, far_fine) * late
    far_places = jnp.where(far_need > 0, before(far_need), -1)
    far_at = landing(far_places, pass_slots, far_base, far_slots)
    place_copy.wait_recv()
    near_at = placing[1][0:1, :]

    above = (row_count, width)
    table_lanes = lax.broadcasted_iota(jnp.int32, above, 1)
    own_at, near_at, far_at = [jnp.broadcast_to(x, above) for x in (lane_tile, near_at, far_at)]
    slot_own, slot_near, slot_far = [], [], []
    for index in range(half_cap):
        even = (2 * (index // own_cap)) * own_cap + index % own_cap
        low = my_low[:, r_slots + even : r_slots + even + 1]
        high = my_low[:, r_slots + even + own_cap : r_slots + even + own_cap + 1]
        column = jnp.where(part == 0, low, high)
        slot_own.append(jnp.where(own_columns == column, own_at, -1))
        slot_near.append(jnp.where(near_columns == column, near_at, -1))
        slot_far.append(jnp.where(far_columns == column, far_at, -1))
    code = jnp.full(above, -1, jnp.int32)
    for j in range(both):
        block = my_low if j < r_slots else my_high
        named = block[:, j % r_slots : j % r_slots + 1]
        in_own = own_fine == named
        in_near = near_fine == named
        in_far = far_fine == named
        for index in range(half_cap):
            found = jnp.where(in_own, slot_own[index], -1)
            found = jnp.where(in_near, slot_near[index], found)
            found = jnp.where(in_far, slot_far[index], found)
            best = jnp.max(found, axis=1, keepdims=True)
            code = jnp.where(table_lanes == index * both + j, best, code)
    tables[0:row_count, :] = jnp.where((code >= 0) & (code < REMOTE), code, zero_own)
    away = code >= REMOTE
    rank = away.astype(jnp.int32)
    table_j = lax.rem(table_lanes, both)
    step = 1
    while step < both:
        rank = rank + jnp.where(table_j >= step, pltpu.roll(rank, step, 1), 0)
        step *= 2
    job = jnp.where(away, (code - REMOTE) * both + table_j, -1)
    rank = jnp.where(away, rank - 1 + (table_lanes // both) * JOBS, -1)
    short = jnp.full(above, -1, jnp.int32)
    for at in range(half_cap * JOBS):
        best = jnp.max(jnp.where(rank == at, job, -1), axis=1, keepdims=True)
        short = jnp.where(table_lanes == at, best, short)
    job_j = lax.rem(jnp.maximum(short, 0), both)
    job_c = lax.broadcasted_iota(jnp.int32, above, 0)
    job_r = (job_j // r_slots) * (row_count * r_slots) + job_c * r_slots + lax.rem(job_j, r_slots)
    tables[row_count : 2 * row_count, :] = jnp.where(short >= 0, short // both, zero_near)
    tables[2 * row_count : 3 * row_count, :] = job_r
    code_copy = pltpu.make_async_copy(tables, codes, table_sems.at[1])
    code_copy.start()

    code_copy.wait()
    own_r.wait()
    mate_r.wait_recv()
    if scans < rounds:
        scan_step()

    def own_stage(c, carry):
        for index in range(0, half_cap, 2):
            total = None
            for j in range(0, both, 2):
                left = jnp.concatenate(
                    [pair_r[x // r_slots * row_count * r_slots + c * r_slots + x % r_slots] for x in (j, j + 1)], axis=1
                )
                right = jnp.concatenate(
                    [
                        jnp.concatenate(
                            [pair_a[codes[c, slot * both + x]] for slot in (index, index + 1)], axis=1
                        )
                        for x in (j, j + 1)
                    ],
                    axis=0,
                )
                term = jnp.dot(left, right, preferred_element_type=jnp.float32)
                total = term if total is None else total + term
            sums[c * half_cap + index] = total[:, :tile]
            sums[c * half_cap + index + 1] = total[:, tile:]
        return carry

    lag = 3
    for index in range(near_chunks):
        near_copy(index).wait_recv()
        if index < far_chunks:
            @pl.when(has_onward)
            def _():
                far_copy(index).start()
        mate_copy(near_view(index), near_pair_sems).start()
        if -1 <= index - lag < far_chunks:
            take_far(index - lag)
        lax.fori_loop(
            index * row_count // near_chunks, (index + 1) * row_count // near_chunks, own_stage, 0
        )
        if index % 3 == 1 and scans < rounds:
            scan_step()
    for index in range(max(near_chunks - lag, -1), far_chunks):
        take_far(index)
    while scans < rounds:
        scan_step()

    flags = jnp.where((scan_lane == 1) | (scan_lane == 2), state, 0)
    flags = jnp.max(jnp.max(flags, axis=1, keepdims=True), axis=0, keepdims=True)
    flag_ref[...] = (flags > 0).astype(jnp.int32)
    reached = jnp.where(scan_lane == 0, state, 0)
    reached = jnp.max(jnp.max(reached, axis=1, keepdims=True), axis=0, keepdims=True)
    earlier = lax.broadcasted_iota(jnp.int32, small, 0) < lax.broadcasted_iota(jnp.int32, small, 1)
    counts = jnp.broadcast_to(own_counts, small)
    inner_sum = jnp.sum(jnp.where(earlier, counts, 0), axis=0, keepdims=True)
    offsets_ref[...] = inner_sum + (reached - total_count)

    wait_bytes(landed.at[pl.ds(0, near_slots)], near_pair_sems.at[1])

    @pl.when(has_far)
    def _():
        wait_bytes(landed.at[pl.ds(0, far_slots)], far_pair_sems.at[1])

    ahead_of = [lax.rem(index // own_cap + pairs - group // 2, pairs) for index in range(half_cap)]

    def near_stage(c, carry):
        for index in range(half_cap):
            jobs = range(index * JOBS, (index + 1) * JOBS)
            left = jnp.concatenate([pair_r[codes[2 * row_count + c, x]] for x in jobs], axis=1)
            right = jnp.concatenate([landed[codes[row_count + c, x]] for x in jobs], axis=0)
            total = sums[c * half_cap + index] + jnp.dot(
                left, right, preferred_element_type=jnp.float32
            )
            place = ahead_of[index] * row_count * own_cap + c * own_cap + index % own_cap
            out_ref[place] = total.astype(out_ref.dtype)
        return carry

    lax.fori_loop(0, row_count, near_stage, 0, unroll=4)

    wait_bytes(close.at[pl.ds(0, 2)], close_sems.at[0, 0])
    to_mate.wait_send()
    mate_a.wait_send()
    mate_r.wait_send()
    early_copy.wait_send()
    place_copy.wait_send()
    wait_bytes(packed, near_send.at[0])
    if groups > 2:
        wait_bytes(told.at[pl.ds(0, groups - 1)], told_sems.at[0])
    wait_bytes(landed.at[pl.ds(0, near_slots)], near_pair_sems.at[0])

    @pl.when(has_onward)
    def _():
        wait_bytes(landed.at[pl.ds(0, far_slots)], far_send.at[0])

    @pl.when(has_far)
    def _():
        wait_bytes(close.at[pl.ds(2, 2)], close_sems.at[0, 1])
        wait_bytes(landed.at[pl.ds(0, far_slots)], far_pair_sems.at[0])

    for k in range(rounds):
        @pl.when(above_there[k])
        def _():
            scan_copy(k, 0).wait_send()

        @pl.when(below_there[k])
        def _():
            scan_copy(k, 1).wait_send()


def pair_sum_kernel(pairs, own, part_ref, landed, send_sems, recv_sems):
    row = lax.axis_index("rows")
    group = lax.axis_index("inner")
    core = lax.rem(group, 2)
    barrier = pltpu.get_barrier_semaphore()

    def place(ahead):
        return (row, 2 * lax.rem(group // 2 + ahead, pairs) + core)

    for ahead in range(1, pairs):
        pl.semaphore_signal(barrier, inc=1, device_id=place(ahead), device_id_type=MESH)
    pl.semaphore_wait(barrier, pairs - 1)
    copies = []
    for ahead in range(1, pairs):
        copy = pltpu.make_async_remote_copy(
            src_ref=part_ref.at[pl.ds(ahead * own, own)],
            dst_ref=landed.at[ahead - 1],
            send_sem=send_sems.at[ahead - 1],
            recv_sem=recv_sems.at[ahead - 1],
            device_id=place(ahead),
            device_id_type=MESH,
        )
        copy.start()
        copies.append(copy)
    for copy in copies:
        copy.wait()


def fused_body(rows, groups, r_tiles, r_cols, a_tiles, a_cols, c_cols, c_counts):
    local_rows, op_slots, tile, _ = a_tiles.shape
    row_count, r_slots = r_tiles.shape[:2]
    cap = c_cols.shape[1]
    tiles = local_rows * op_slots
    pairs = groups // 2
    own_cap = cap // groups
    half_cap = cap // 2
    width = -(-2 * tiles // 128) * 128
    list_slots = min(LIST_SLOTS, -(-tiles // CHUNK) * CHUNK)
    pass_slots = min(PASS_SLOTS, list_slots)
    dims = (rows, groups, local_rows, op_slots, r_slots, cap, width, list_slots, pass_slots, CHUNK)
    near_chunks = list_slots // CHUNK
    far_chunks = pass_slots // CHUNK
    near_slots = op_slots + list_slots
    far_slots = op_slots + pass_slots
    rounds = (rows - 1).bit_length()
    dtype = a_tiles.dtype
    out_dtype = jnp.bfloat16 if pairs == 1 else jnp.float32
    own = row_count * own_cap
    vmem = pl.BlockSpec(memory_space=pltpu.VMEM)
    anywhere = pl.BlockSpec(memory_space=pl.ANY)
    dma = pltpu.SemaphoreType.DMA
    block = (row_count, 128)
    part, offsets, flag = pl.pallas_call(
        functools.partial(fused_kernel, dims),
        out_shape=(
            jax.ShapeDtypeStruct((pairs * own, tile, tile), out_dtype),
            jax.ShapeDtypeStruct((1, row_count), jnp.int32),
            jax.ShapeDtypeStruct((1, 1), jnp.int32),
        ),
        in_specs=[anywhere] * 6,
        out_specs=(vmem, vmem, vmem),
        scratch_shapes=[
            pltpu.VMEM(r_cols.shape, jnp.int32),
            pltpu.VMEM(c_cols.shape, jnp.int32),
            pltpu.VMEM((1, row_count), jnp.int32),
            pltpu.VMEM((op_slots, a_cols.shape[0]), jnp.int32),
            pltpu.VMEM(block, jnp.int32),
            pltpu.VMEM((5,) + block, jnp.int32),
            pltpu.VMEM((2, 8, width), jnp.int32),
            pltpu.VMEM((2 * tiles + 1, tile, tile), dtype),
            pltpu.VMEM((2 * row_count * r_slots, tile, tile), dtype),
            pltpu.VMEM((list_slots, tile, tile), dtype),
            pltpu.VMEM((2 * (near_slots + far_slots) + 1, tile, tile), dtype),
            pltpu.VMEM((row_count * half_cap, tile, tile), jnp.float32),
            pltpu.VMEM((3 * row_count, width), jnp.int32),
            pltpu.SMEM((3 * row_count, width), jnp.int32),
            pltpu.SMEM((8, width), jnp.int32),
            pltpu.VMEM((groups, 8, 128), jnp.int32),
            pltpu.VMEM((rounds, 8, 128), jnp.int32),
            pltpu.VMEM((rounds, 2, 8, 128), jnp.int32),
            dma((6,)),
            dma((2, 3)),
            dma((2, 2)),
            dma((2,)),
            dma((2,)),
            dma((near_chunks,)),
            dma((1,)),
            dma((2,)),
            dma((far_chunks + 1,)),
            dma((1,)),
            dma((2,)),
            dma((2,)),
            dma((2,)),
            dma((2, rounds, 2)),
        ],
        compiler_params=pltpu.CompilerParams(collective_id=40, has_side_effects=True),
        name="fused",
    )(
        r_cols,
        c_cols,
        c_counts[None, :],
        a_cols.T,
        a_tiles.reshape(tiles, tile, tile),
        r_tiles.reshape(row_count * r_slots, tile, tile),
    )
    if pairs == 1:
        c_tiles = part
    else:
        landed = pl.pallas_call(
            functools.partial(pair_sum_kernel, pairs, own),
            out_shape=jax.ShapeDtypeStruct((pairs - 1, own, tile, tile), jnp.float32),
            in_specs=[anywhere],
            out_specs=anywhere,
            scratch_shapes=[dma((pairs - 1,)), dma((pairs - 1,))],
            compiler_params=pltpu.CompilerParams(collective_id=41, has_side_effects=True),
            name="pair_sums",
        )(part)
        c_tiles = part[:own]
        for ahead in range(pairs - 1):
            c_tiles = c_tiles + landed[ahead]
        c_tiles = c_tiles.astype(jnp.bfloat16)
    return c_tiles.reshape(row_count, own_cap, tile, tile), offsets[0], flag[0, 0]


def body(rows, groups, *args):
    if rows % 2 or groups % 2:
        return plain_body(rows, groups, *args)
    c_tiles, offsets, flag = fused_body(rows, groups, *args)

    def again(c_tiles, offsets, *args):
        return plain_body(rows, groups, *args)

    def keep(c_tiles, offsets, *args):
        return c_tiles, offsets

    return lax.cond(flag > 0, again, keep, c_tiles, offsets, *args)


def solution(mesh):
    rows = mesh.shape["rows"]
    groups = mesh.shape["inner"]
    return jax.shard_map(
        functools.partial(body, rows, groups),
        mesh=mesh,
        in_specs=(
            P("rows", "inner", None, None),
            P("rows", "inner"),
            P(("rows", "inner"), None, None, None),
            P(),
            P("rows", None),
            P("rows"),
        ),
        out_specs=(P("rows", "inner", None, None), P("rows")),
        check_vma=False,
    )
```

```python
import functools

import jax
import jax.numpy as jnp
from jax import lax
from jax.experimental import pallas as pl
from jax.experimental.pallas import tpu as pltpu
from jax.sharding import PartitionSpec as P

MESH = pl.DeviceIdType.MESH
BATCH = 4


def plan_kernel(
    dims, r_cols_ref, c_cols_ref, counts_ref, columns_ref, code_ref, plan_ref,
    meta_ref, gathered, needs, send_sem, recv_sem,
):
    rows, groups, local_rows, op_slots, r_slots, cap, half = dims
    width = 2 * half
    count = rows * groups
    tiles = local_rows * op_slots
    row = lax.axis_index("rows")
    group = lax.axis_index("inner")
    me = row * groups + group

    barrier = pltpu.get_barrier_semaphore()

    def place(step):
        other = lax.rem(me + step, count)
        return (other // groups, lax.rem(other, groups))

    def greet(step, carry):
        pl.semaphore_signal(barrier, inc=1, device_id=place(step), device_id_type=MESH)
        return carry

    lax.fori_loop(1, count, greet, 0)
    row_count = r_cols_ref.shape[0]
    live = r_slots + cap
    lanes = lax.broadcasted_iota(jnp.int32, (row_count, width), 1)
    above = lax.broadcasted_iota(jnp.int32, (row_count, width), 0)
    small = (row_count, row_count)
    diagonal = lax.broadcasted_iota(jnp.int32, small, 0) == lax.broadcasted_iota(jnp.int32, small, 1)
    spread_counts = jnp.broadcast_to(counts_ref[...], small)
    own_counts = jnp.sum(jnp.where(diagonal, spread_counts, 0), axis=1, keepdims=True)
    meta_ref[...] = jnp.full(meta_ref.shape, -9, jnp.int32)
    meta_ref[:, 0:r_slots] = r_cols_ref[...]
    meta_ref[:, r_slots:live] = c_cols_ref[...]
    meta_ref[:, live : live + 1] = own_counts
    gathered[me] = meta_ref[...]
    pl.semaphore_wait(barrier, count - 1)

    def post(step, carry):
        pltpu.make_async_remote_copy(
            src_ref=meta_ref,
            dst_ref=gathered.at[me],
            send_sem=send_sem,
            recv_sem=recv_sem,
            device_id=place(step),
            device_id_type=MESH,
        ).start()
        return carry

    lax.fori_loop(1, count, post, 0)
    everyone = gathered.at[pl.ds(0, count - 1)]
    pltpu.make_async_copy(everyone, everyone, send_sem).wait()
    pltpu.make_async_copy(everyone, everyone, recv_sem).wait()

    def matches(block, columns, fine_rows):
        named = fine_rows == block[:, 0:1]
        for j in range(1, r_slots):
            named = named | (fine_rows == block[:, j : j + 1])
        slot = jnp.full((row_count, width), -1, jnp.int32)
        for s in range(cap):
            slot = jnp.where(columns == block[:, r_slots + s : r_slots + s + 1], s, slot)
        return jnp.where(named, slot, -1)

    shift = jnp.where(lanes < half, -groups, groups) * local_rows
    tile = jnp.where(lanes < half, lanes, lanes - half)
    lane_rows = jnp.where(tile < tiles, shift + tile // op_slots, -(1 << 24))
    low_lanes = lanes[0:1] < half

    def near_matches(device):
        before = columns_ref[pl.ds(jnp.maximum(device - groups, 0), 1), :]
        after = columns_ref[pl.ds(jnp.minimum(device + groups, count - 1), 1), :]
        columns = jnp.where(low_lanes, before, after)
        return matches(gathered[device], columns, lane_rows + device * local_rows)

    def wanted(found):
        return jnp.max((found >= 0).astype(jnp.int32), axis=0, keepdims=True)

    def gather_needs(device, carry):
        needs[pl.ds(device, 1), :] = wanted(near_matches(device))
        return carry

    lax.fori_loop(0, count, gather_needs, 0, unroll=4)
    every = needs[...]
    low_side = lax.broadcasted_iota(jnp.int32, every.shape, 1) < half
    low = jnp.sum(jnp.where(low_side, every, 0), axis=1, keepdims=True)
    high = jnp.sum(jnp.where(low_side, 0, every), axis=1, keepdims=True)
    most = jnp.max(jnp.maximum(low, high), axis=0, keepdims=True)

    down = lax.broadcasted_iota(jnp.int32, (width, width), 0)
    across = lax.broadcasted_iota(jnp.int32, (width, width), 1)
    same = (down < half) == (across < half)

    def ranks(need):
        spread = jnp.broadcast_to(need, (width, width))
        column = jnp.sum(jnp.where(down == across, spread, 0), axis=1, keepdims=True)
        before = jnp.sum(jnp.where((across < down) & same, spread, 0), axis=1, keepdims=True)
        along = jnp.sum(
            jnp.where((down < across) & same, jnp.broadcast_to(column, (width, width)), 0),
            axis=0,
            keepdims=True,
        )
        return column, before, along

    def send_list(device, high):
        column, before, _ = ranks(needs[pl.ds(device, 1), :])
        first = half if high else 0
        mine = (down >= half) if high else (down < half)
        chosen = mine & (column > 0) & (before == across)
        return jnp.sum(jnp.where(chosen, down - first, 0), axis=0, keepdims=True)

    left = jnp.maximum(row - 1, 0) * groups + group
    right = jnp.minimum(row + 1, rows - 1) * groups + group
    plan_ref[0:1, :] = send_list(left, True)
    plan_ref[1:2, :] = send_list(right, False)

    found = near_matches(me)
    _, _, along = ranks(wanted(found))
    slot_at = along + jnp.where(lanes[0:1] < half, tiles, 2 * tiles)
    code_ref[:, 0:width] = jnp.where(found >= 0, found + cap * slot_at, -1)
    fine = me * local_rows + jnp.where(lanes < tiles, lanes // op_slots, 0)
    fine = jnp.where(lanes < tiles, fine, -5)
    found = matches(gathered[me], columns_ref[pl.ds(me, 1), :], fine)
    code_ref[:, width:] = jnp.where(found >= 0, found + cap * lanes, -1)

    def earlier(index, total):
        block = gathered[index * groups]
        return total + jnp.sum(block[:, live : live + 1], axis=0, keepdims=True)

    first = lax.fori_loop(0, row, earlier, jnp.zeros((1, 1), jnp.int32))
    counts = jnp.broadcast_to(own_counts, (row_count, width))
    inner_sum = jnp.sum(jnp.where(above < lanes, counts, 0), axis=0, keepdims=True)
    plan_ref[2:3, :] = inner_sum + first
    level = jnp.zeros((1, 1), jnp.int32)
    for size in sizes_for(tiles)[:-1]:
        level = level + (most > size).astype(jnp.int32)
    plan_ref[3:4, :] = jnp.broadcast_to(level, (1, width))


def halo_kernel(rows, size, plan_ref, a_ref, out_ref, packed, send_sems, recv_sems):
    row = lax.axis_index("rows")
    group = lax.axis_index("inner")
    barrier = pltpu.get_barrier_semaphore()
    has_left = row > 0
    has_right = row < rows - 1

    @pl.when(has_left)
    def _():
        pl.semaphore_signal(barrier, inc=1, device_id=(row - 1, group), device_id_type=MESH)

    @pl.when(has_right)
    def _():
        pl.semaphore_signal(barrier, inc=1, device_id=(row + 1, group), device_id_type=MESH)

    def pack(index, carry):
        packed[0, index] = a_ref[plan_ref[0, index]]
        packed[1, index] = a_ref[plan_ref[1, index]]
        return carry

    lax.fori_loop(0, size, pack, 0, unroll=2)

    pl.semaphore_wait(barrier, has_left.astype(jnp.int32) + has_right.astype(jnp.int32))

    def copy(side, other):
        return pltpu.make_async_remote_copy(
            src_ref=packed.at[side],
            dst_ref=out_ref.at[1 - side, pl.ds(0, size)],
            send_sem=send_sems.at[side],
            recv_sem=recv_sems.at[1 - side],
            device_id=(other, group),
            device_id_type=MESH,
        )

    @pl.when(has_left)
    def _():
        copy(0, row - 1).start()

    @pl.when(has_right)
    def _():
        copy(1, row + 1).start()

    @pl.when(has_left)
    def _():
        copy(0, row - 1).wait_send()
        copy(1, row - 1).wait_recv()

    @pl.when(has_right)
    def _():
        copy(1, row + 1).wait_send()
        copy(0, row + 1).wait_recv()


def product_kernel(dims, code_ref, cols_ref, r_ref, a_ref, halo_ref, out_ref, tiles_ref, jobs, sems):
    rows, groups, local_rows, op_slots, r_slots, cap, half = dims
    width = 2 * half
    tiles = local_rows * op_slots
    row_count = cols_ref.shape[0]
    own_cap = cap // groups
    row = lax.axis_index("rows")
    group = lax.axis_index("inner")
    own = pltpu.make_async_copy(a_ref, tiles_ref.at[pl.ds(0, tiles)], sems.at[0])
    near = pltpu.make_async_copy(halo_ref, tiles_ref.at[pl.ds(tiles, 2 * tiles)], sems.at[1])
    own.start()
    near.start()
    last = groups * row_count * own_cap
    scale = 1 << (3 * tiles * cap - 1).bit_length()

    def clear(index, carry):
        out_ref[index] = jnp.zeros(out_ref.shape[1:], jnp.float32)
        return carry

    lax.fori_loop(0, last, clear, 0, unroll=4)

    def list_row(c, found):
        def list_slot(j, found):
            fine = cols_ref[c, j]
            side = fine // (local_rows * groups) - row
            base = jnp.where(side == 0, width, jnp.where(side < 0, 0, half))
            base = base + lax.rem(fine, local_rows) * op_slots
            for t in range(op_slots):
                code = code_ref[c, base + t]
                jobs[found] = (c * r_slots + j) * scale + code
                found = found + (code >= 0).astype(jnp.int32)
            return found

        return lax.fori_loop(0, r_slots, list_slot, found)

    found = lax.fori_loop(0, row_count, list_row, jnp.int32(0))
    for extra in range(BATCH):
        jobs[found + extra] = -1
    own.wait()
    near.wait()

    def batch(step, carry):
        results = []
        targets = []
        for extra in range(BATCH):
            job = jobs[step * BATCH + extra]
            valid = job >= 0
            job = jnp.maximum(job, 0)
            pair = job // scale
            code = lax.rem(job, scale)
            slot = lax.rem(code, cap)
            ahead = lax.rem(slot // own_cap + groups - group, groups)
            target = (ahead * row_count + pair // r_slots) * own_cap + lax.rem(slot, own_cap)
            targets.append(jnp.where(valid, target, last))
            results.append(
                jnp.dot(
                    r_ref[pair],
                    tiles_ref[code // cap],
                    preferred_element_type=jnp.float32,
                )
            )
        for extra in range(BATCH):
            target = targets[extra]
            out_ref[target] = out_ref[target] + results[extra]
        return carry

    lax.fori_loop(0, (found + BATCH - 1) // BATCH, batch, 0)


def sum_kernel(groups, own, part_ref, landed, send_sems, recv_sems):
    row = lax.axis_index("rows")
    group = lax.axis_index("inner")
    barrier = pltpu.get_barrier_semaphore()
    for ahead in range(1, groups):
        pl.semaphore_signal(
            barrier, inc=1, device_id=(row, lax.rem(group + ahead, groups)), device_id_type=MESH
        )
    pl.semaphore_wait(barrier, groups - 1)
    copies = []
    for ahead in range(1, groups):
        copy = pltpu.make_async_remote_copy(
            src_ref=part_ref.at[pl.ds(ahead * own, own)],
            dst_ref=landed.at[ahead - 1],
            send_sem=send_sems.at[ahead - 1],
            recv_sem=recv_sems.at[ahead - 1],
            device_id=(row, lax.rem(group + ahead, groups)),
            device_id_type=MESH,
        )
        copy.start()
        copies.append(copy)
    for copy in copies:
        copy.wait()


def sizes_for(tiles):
    steps = [16, 18, 20, 21, 22, 23, 24, 25, 26, 27, 28, 29, 30, 32, 36, 42]
    return [size for size in steps if size < tiles] + [tiles]


def plain_body(rows, groups, r_tiles, r_cols, a_tiles, a_cols, c_cols, c_counts):
    local_rows, op_slots, tile, _ = a_tiles.shape
    row_count, r_slots = r_tiles.shape[:2]
    cap = c_cols.shape[1]
    tiles = local_rows * op_slots
    half = -(-tiles // 64) * 64
    width = 2 * half
    count = rows * groups
    own_cap = cap // groups
    dims = (rows, groups, local_rows, op_slots, r_slots, cap, half)
    vmem = pl.BlockSpec(memory_space=pltpu.VMEM)
    smem = pl.BlockSpec(memory_space=pltpu.SMEM)
    anywhere = pl.BlockSpec(memory_space=pl.ANY)

    flat = a_cols.reshape(count, tiles)
    flat = jnp.pad(flat, ((0, 0), (0, half - tiles)), constant_values=-2)
    columns = jnp.concatenate([flat, flat], axis=1)

    code, plan = pl.pallas_call(
        functools.partial(plan_kernel, dims),
        out_shape=(
            jax.ShapeDtypeStruct((row_count, 2 * width), jnp.int32),
            jax.ShapeDtypeStruct((8, width), jnp.int32),
        ),
        in_specs=[vmem] * 4,
        out_specs=(vmem, vmem),
        scratch_shapes=[
            pltpu.VMEM((row_count, width), jnp.int32),
            pltpu.VMEM((count, row_count, width), jnp.int32),
            pltpu.VMEM((count, width), jnp.int32),
            pltpu.SemaphoreType.DMA,
            pltpu.SemaphoreType.DMA,
        ],
        compiler_params=pltpu.CompilerParams(collective_id=0, has_side_effects=True),
        name="plan",
    )(r_cols, c_cols, c_counts[None, :], columns)

    flat_a = a_tiles.reshape(tiles, tile, tile)
    sizes = sizes_for(tiles)

    def exchange(number, size, plan, flat_a):
        return pl.pallas_call(
            functools.partial(halo_kernel, rows, size),
            out_shape=jax.ShapeDtypeStruct((2, tiles, tile, tile), a_tiles.dtype),
            in_specs=[smem, vmem],
            out_specs=anywhere,
            scratch_shapes=[
                pltpu.VMEM((2, size, tile, tile), a_tiles.dtype),
                pltpu.SemaphoreType.DMA((2,)),
                pltpu.SemaphoreType.DMA((2,)),
            ],
            compiler_params=pltpu.CompilerParams(collective_id=number + 2, has_side_effects=True),
            name=f"halo{size}",
        )(plan, flat_a)

    halo = lax.switch(
        plan[3, 0],
        [functools.partial(exchange, number, size) for number, size in enumerate(sizes)],
        plan,
        flat_a,
    )

    slots = row_count * r_slots * op_slots + BATCH
    partial_value = pl.pallas_call(
        functools.partial(product_kernel, dims),
        out_shape=jax.ShapeDtypeStruct((row_count * cap + 1, tile, tile), jnp.float32),
        in_specs=[smem, smem, vmem, anywhere, anywhere],
        out_specs=vmem,
        scratch_shapes=[
            pltpu.VMEM((3 * tiles, tile, tile), a_tiles.dtype),
            pltpu.SMEM((slots,), jnp.int32),
            pltpu.SemaphoreType.DMA((2,)),
        ],
        name="products",
    )(
        code,
        r_cols,
        r_tiles.reshape(row_count * r_slots, tile, tile),
        flat_a,
        halo.reshape(2 * tiles, tile, tile),
    )

    own_count = row_count * own_cap
    landed = pl.pallas_call(
        functools.partial(sum_kernel, groups, own_count),
        out_shape=jax.ShapeDtypeStruct((groups - 1, own_count, tile, tile), jnp.float32),
        in_specs=[anywhere],
        out_specs=anywhere,
        scratch_shapes=[
            pltpu.SemaphoreType.DMA((groups - 1,)),
            pltpu.SemaphoreType.DMA((groups - 1,)),
        ],
        compiler_params=pltpu.CompilerParams(collective_id=1, has_side_effects=True),
        name="sums",
    )(partial_value)
    c_tiles = partial_value[:own_count]
    for ahead in range(groups - 1):
        c_tiles = c_tiles + landed[ahead]
    c_tiles = c_tiles.astype(jnp.bfloat16)
    return (c_tiles.reshape(row_count, own_cap, tile, tile), plan[2, :row_count])

PASS_SLOTS = 15
CHUNK = 3
LAST_CHUNKS = (3, 3, 3, 2)
JOBS = 4
REMOTE = 1 << 14


def fused_kernel(
    dims, r_cols_hbm, c_cols_hbm, counts_hbm, columns_hbm, a_ref, r_ref,
    out_ref, offsets_ref, flag_hbm,
    flag_ref, r_cols_ref, c_cols_ref, counts_ref, columns_ref,
    meta, close, placing, pair_a, pair_r, packed, landed, sums, tables, codes, picks,
    told, scan_out, scan_in,
    local_sems, close_sems, pair_sems, place_sems, early_sems, near_sems, near_send,
    near_pair_sems, far_sems, far_send, far_pair_sems, table_sems, told_sems, scan_sems,
):
    (rows, groups, local_rows, op_slots, r_slots, cap, width, list_slots, pass_slots, chunks) = dims
    pairs = groups // 2
    tiles = local_rows * op_slots
    span = 2 * local_rows
    own_cap = cap // groups
    half_cap = cap // 2
    both = 2 * r_slots
    row_count = r_cols_ref.shape[0]
    live = r_slots + cap
    early = op_slots
    near_slots = early + list_slots
    far_slots = early + pass_slots
    near_chunks = len(chunks)
    far_chunks = sum(start < pass_slots for start, _ in chunks)
    far_base = 2 * near_slots
    zero_near = 2 * (near_slots + far_slots)
    zero_own = 2 * tiles
    rounds = (rows - 1).bit_length()

    row = lax.axis_index("rows")
    group = lax.axis_index("inner")
    part = lax.rem(group, 2)
    first_group = group - part
    mate = first_group + 1 - part
    odd = lax.rem(row, 2)
    near = row + 1 - 2 * odd
    far = row - 1 + 2 * odd
    has_far = (far >= 0) & (far < rows)
    onward = near + 1 - 2 * odd
    has_onward = (onward >= 0) & (onward < rows)
    mate_place = (row, mate)

    barrier = pltpu.get_barrier_semaphore()

    def greet(place):
        pl.semaphore_signal(barrier, inc=1, device_id=place, device_id_type=MESH)

    for core in range(2):
        greet((near, first_group + core))

    @pl.when(has_far)
    def _():
        for core in range(2):
            greet((far, first_group + core))

    for ahead in range(1, groups):
        greet((row, lax.rem(group + ahead, groups)))

    small_copies = [
        pltpu.make_async_copy(src, dst, local_sems.at[2 + index])
        for index, (src, dst) in enumerate(
            [
                (r_cols_hbm, r_cols_ref),
                (c_cols_hbm, c_cols_ref),
                (counts_hbm, counts_ref),
                (columns_hbm, columns_ref),
            ]
        )
    ]
    for copy in small_copies:
        copy.start()
    own_a = pltpu.make_async_copy(
        a_ref, pair_a.at[pl.ds(part * tiles, tiles)], local_sems.at[0]
    )
    own_r = pltpu.make_async_copy(r_ref, pair_r.at[pl.ds(part * row_count * r_slots, row_count * r_slots)], local_sems.at[1])
    own_a.start()
    own_r.start()

    def remote(src, dst, send_sem, recv_sem, place):
        return pltpu.make_async_remote_copy(
            src_ref=src, dst_ref=dst, send_sem=send_sem, recv_sem=recv_sem,
            device_id=place, device_id_type=MESH,
        )

    def wait_bytes(view, sem):
        pltpu.make_async_copy(view, view, sem).wait()

    small = (row_count, row_count)
    diagonal = lax.broadcasted_iota(jnp.int32, small, 0) == lax.broadcasted_iota(jnp.int32, small, 1)
    meta[...] = jnp.full(meta.shape, -9, jnp.int32)
    pair_a[zero_own] = jnp.zeros(pair_a.shape[1:], pair_a.dtype)
    landed[zero_near] = jnp.zeros(landed.shape[1:], landed.dtype)
    for copy in small_copies:
        copy.wait()
    spread_counts = jnp.broadcast_to(counts_ref[...], small)
    own_counts = jnp.sum(jnp.where(diagonal, spread_counts, 0), axis=1, keepdims=True)
    meta[:, 0:r_slots] = r_cols_ref[...]
    meta[:, r_slots:live] = c_cols_ref[...]
    pl.semaphore_wait(barrier, groups + 1 + 2 * has_far.astype(jnp.int32))

    def start_close(target, first, which):
        for core in range(2):
            remote(
                meta, close.at[first + part], close_sems.at[0, which], close_sems.at[1, which],
                (target, first_group + core),
            ).start()

    @pl.when(has_far)
    def _():
        start_close(far, 2, 1)

    start_close(near, 0, 0)
    to_mate = remote(meta, close.at[4], close_sems.at[0, 2], close_sems.at[1, 2], mate_place)
    to_mate.start()
    mate_a = remote(
        a_ref, pair_a.at[pl.ds(part * tiles, tiles)], pair_sems.at[0, 0], pair_sems.at[1, 0], mate_place
    )
    mate_a.start()

    own_a.wait()
    early_copy = remote(
        pair_a.at[pl.ds(part * tiles, early)], landed.at[pl.ds(part * near_slots, early)],
        early_sems.at[0], early_sems.at[1], (near, group),
    )
    early_copy.start()
    mate_r = remote(r_ref, pair_r.at[pl.ds(part * row_count * r_slots, row_count * r_slots)], pair_sems.at[0, 1], pair_sems.at[1, 1], mate_place)
    mate_r.start()

    lanes = lax.broadcasted_iota(jnp.int32, (1, width), 1)
    real = lanes < op_slots * span
    lane_slot = lanes // span
    lane_fine = jnp.where(real, lax.rem(lanes, span), -(1 << 24))
    lane_core = lax.rem(lanes, span) // local_rows
    lane_local = lax.rem(lanes, local_rows)
    lane_tile = lane_core * tiles + lane_local * op_slots + lane_slot
    late = jnp.where(lane_local > 0, 1, 0)

    def pair_columns(which_row):
        start = (which_row * groups + first_group) * local_rows
        block = start // 128
        values = columns_ref[:, pl.ds(pl.multiple_of(block * 128, 128), 128)]
        if width > 128:
            values = jnp.concatenate([values] * (width // 128), axis=1)
        offset = start - block * 128
        total = jnp.zeros((1, width), jnp.int32)
        for t in range(op_slots):
            moved = pltpu.roll(values[t : t + 1, :], lax.rem(t * span - offset + 128 * width, width), 1)
            total = jnp.where(lane_slot == t, moved, total)
        return jnp.where(real, total, -2)

    def pair_fine(which_row):
        return lane_fine + (which_row * groups + first_group) * local_rows

    def named_by(meta_low, meta_high, fine):
        named = fine == meta_low[:, 0:1]
        for j in range(1, r_slots):
            named = named | (fine == meta_low[:, j : j + 1])
        for j in range(r_slots):
            named = named | (fine == meta_high[:, j : j + 1])
        return named

    def need_of(meta_low, meta_high, columns, fine):
        named = named_by(meta_low, meta_high, fine)
        wanted = columns == meta_low[:, r_slots : r_slots + 1]
        for s in range(1, cap):
            wanted = wanted | (columns == meta_low[:, r_slots + s : r_slots + s + 1])
        return jnp.max((named & wanted).astype(jnp.int32), axis=0, keepdims=True)

    def before(need):
        total = need
        step = 1
        while step < width:
            total = total + jnp.where(lanes >= step, pltpu.roll(total, step, 1), 0)
            step *= 2
        return total - need

    def landing(places, count, base, slots):
        fits = (places >= 0) & (places < 2 * count)
        at = lax.rem(places, 2) * slots + early + places // 2
        at = jnp.where(late > 0, jnp.where(fits, at, -1), lane_core * slots + lane_slot)
        return jnp.where(real & (at >= 0), REMOTE + base + at, -1)

    own_columns = pair_columns(row)
    own_fine = pair_fine(row)

    @pl.when(has_far)
    def _():
        wait_bytes(close.at[pl.ds(2, 2)], close_sems.at[1, 1])

    @pl.when(jnp.logical_not(has_far))
    def _():
        close[2] = jnp.full(close.shape[1:], -9, jnp.int32)
        close[3] = jnp.full(close.shape[1:], -9, jnp.int32)

    need_far = need_of(close[2], close[3], own_columns, own_fine) * late
    far_before = before(need_far)
    far_total = jnp.sum(need_far, axis=1, keepdims=True)
    wait_bytes(close.at[pl.ds(0, 2)], close_sems.at[1, 0])
    need_near = need_of(close[0], close[1], own_columns, own_fine) * late
    need_only = need_near * (1 - need_far)
    near_total = far_total + jnp.sum(need_only, axis=1, keepdims=True)
    places = jnp.where(
        need_far > 0, far_before, jnp.where(need_only > 0, before(need_only) + far_total, -1)
    )
    pick_rows = -(-list_slots // 8) * 8
    slot_down = lax.broadcasted_iota(jnp.int32, (pick_rows, width), 0)
    chosen = jnp.broadcast_to(places, (pick_rows, width)) == 2 * slot_down + part
    picked = jnp.sum(
        jnp.where(chosen, jnp.broadcast_to(lane_tile, (pick_rows, width)), 0), axis=1, keepdims=True
    )
    across = lax.broadcasted_iota(jnp.int32, (pick_rows, width), 1)
    pick_row = jnp.sum(
        jnp.where(slot_down == across, jnp.broadcast_to(picked, (pick_rows, width)), 0),
        axis=0, keepdims=True,
    )
    tables[0:8, :] = jnp.broadcast_to(pick_row, (8, width))
    pick_copy = pltpu.make_async_copy(tables.at[pl.ds(0, 8)], picks, table_sems.at[0])
    pick_copy.start()
    placing[0] = jnp.broadcast_to(landing(places, list_slots, 0, near_slots), placing.shape[1:])
    place_copy = remote(placing.at[0], placing.at[1], place_sems.at[0], place_sems.at[1], (near, group))
    place_copy.start()
    near_columns = pair_columns(near)
    near_fine = pair_fine(near)
    far_row = jnp.clip(far, 0, rows - 1)
    far_columns = pair_columns(far_row)
    far_fine = jnp.where(has_far, pair_fine(far_row), -(1 << 24))
    to_mate.wait_recv()
    mine, other = meta[...], close[4]
    my_low = jnp.where(part == 0, mine, other)
    my_high = jnp.where(part == 0, other, mine)
    near_named = named_by(my_low, my_high, near_fine)
    far_named = named_by(my_low, my_high, far_fine)
    crowded = jnp.zeros((1, 1), jnp.int32)
    for s in range(cap):
        column = my_low[:, r_slots + s : r_slots + s + 1]
        hits = (near_named & (near_columns == column)).astype(jnp.int32)
        hits = hits + (far_named & (far_columns == column)).astype(jnp.int32)
        held = jnp.sum(hits, axis=1, keepdims=True)
        crowded = jnp.maximum(crowded, jnp.max(held, axis=0, keepdims=True))
    over = jnp.maximum(near_total - 2 * list_slots, far_total - 2 * pass_slots)
    over = jnp.maximum(over, crowded - JOBS)
    over = (over > 0).astype(jnp.int32)
    if groups > 2:
        told[group] = jnp.broadcast_to(over, told.shape[1:])

        def tell(ahead):
            return remote(
                told.at[group], told.at[group], told_sems.at[0], told_sems.at[1],
                (row, lax.rem(group + ahead, groups)),
            )

        for ahead in range(1, groups):
            tell(ahead).start()
        wait_bytes(told.at[pl.ds(0, groups - 1)], told_sems.at[1])
        over = told[0]
        for other_group in range(1, groups):
            over = over + told[other_group]

    tile = pair_a.shape[1]
    total_count = jnp.sum(own_counts, axis=0, keepdims=True)

    def scan_copy(k, side):
        other = row + (1 << k) if side == 0 else row - (1 << k)
        return remote(
            scan_out.at[k], scan_in.at[k, side], scan_sems.at[0, k, side], scan_sems.at[1, k, side],
            (other, group),
        )

    scan_shape = scan_out.shape[1:]
    scan_lane = lax.broadcasted_iota(jnp.int32, scan_shape, 1)
    above_there = [row + (1 << k) < rows for k in range(rounds)]
    below_there = [row - (1 << k) >= 0 for k in range(rounds)]

    def scan_send(k, state):
        scan_out[k] = state

        @pl.when(above_there[k])
        def _():
            scan_copy(k, 0).start()

        @pl.when(below_there[k])
        def _():
            scan_copy(k, 1).start()

    def scan_take(k, state):
        @pl.when(below_there[k])
        def _():
            scan_copy(k, 0).wait_recv()

        @pl.when(above_there[k])
        def _():
            scan_copy(k, 1).wait_recv()

        below = jnp.where((scan_lane < 2) & below_there[k], scan_in[k, 0], 0)
        beyond = jnp.where((scan_lane == 2) & above_there[k], scan_in[k, 1], 0)
        return state + below + beyond

    state = jnp.where(
        scan_lane == 0, jnp.broadcast_to(total_count, scan_shape),
        jnp.where(scan_lane < 3, over, 0),
    )
    scan_send(0, state)
    scans = 0

    def scan_step():
        nonlocal state, scans
        state = scan_take(scans, state)
        scans += 1
        if scans < rounds:
            scan_send(scans, state)

    mate_a.wait_recv()
    pick_copy.wait()

    def near_view(index):
        start, size = chunks[index]
        return landed.at[pl.ds(part * near_slots + early + start, size)]

    def near_copy(index):
        return remote(
            packed.at[pl.ds(*chunks[index])], near_view(index),
            near_send.at[0], near_sems.at[index], (near, group),
        )

    def pack(index):
        start, size = chunks[index]
        for slot in range(start, start + size):
            packed[slot] = pair_a[picks[0, slot]]

    pack(0)
    for index in range(near_chunks):
        if index + 1 < near_chunks:
            pack(index + 1)
        near_copy(index).start()

    def mate_copy(view, sems):
        return remote(view, view, sems.at[0], sems.at[1], mate_place)

    early_view = landed.at[pl.ds(part * near_slots, early)]
    early_far_view = landed.at[pl.ds(far_base + part * far_slots, early)]

    def far_view(index):
        start, size = chunks[index]
        return landed.at[pl.ds(far_base + part * far_slots + early + start, size)]

    early_far = remote(early_view, early_far_view, far_send.at[0], far_sems.at[far_chunks], (onward, group))

    def far_copy(index):
        return remote(
            near_view(index), far_view(index), far_send.at[0], far_sems.at[index], (onward, group)
        )

    def take_far(index):
        @pl.when(has_far)
        def _():
            if index < 0:
                early_far.wait_recv()
                mate_copy(early_far_view, far_pair_sems).start()
            else:
                far_copy(index).wait_recv()
                mate_copy(far_view(index), far_pair_sems).start()

    early_copy.wait_recv()

    @pl.when(has_onward)
    def _():
        early_far.start()

    mate_copy(early_view, near_pair_sems).start()
    if scans < rounds:
        scan_step()
    far_need = need_of(my_low, my_high, far_columns, far_fine) * late
    far_places = jnp.where(far_need > 0, before(far_need), -1)
    far_at = landing(far_places, pass_slots, far_base, far_slots)
    place_copy.wait_recv()
    near_at = placing[1][0:1, :]

    above = (row_count, width)
    table_lanes = lax.broadcasted_iota(jnp.int32, above, 1)
    own_at, near_at, far_at = [jnp.broadcast_to(x, above) for x in (lane_tile, near_at, far_at)]
    slot_own, slot_near, slot_far = [], [], []
    for index in range(half_cap):
        even = (2 * (index // own_cap)) * own_cap + index % own_cap
        low = my_low[:, r_slots + even : r_slots + even + 1]
        high = my_low[:, r_slots + even + own_cap : r_slots + even + own_cap + 1]
        column = jnp.where(part == 0, low, high)
        slot_own.append(jnp.where(own_columns == column, own_at, -1))
        slot_near.append(jnp.where(near_columns == column, near_at, -1))
        slot_far.append(jnp.where(far_columns == column, far_at, -1))
    code = jnp.full(above, -1, jnp.int32)
    for j in range(both):
        block = my_low if j < r_slots else my_high
        named = block[:, j % r_slots : j % r_slots + 1]
        in_own = own_fine == named
        in_near = near_fine == named
        in_far = far_fine == named
        for index in range(half_cap):
            found = jnp.where(in_own, slot_own[index], -1)
            found = jnp.where(in_near, slot_near[index], found)
            found = jnp.where(in_far, slot_far[index], found)
            best = jnp.max(found, axis=1, keepdims=True)
            code = jnp.where(table_lanes == index * both + j, best, code)
    tables[0:row_count, :] = jnp.where((code >= 0) & (code < REMOTE), code, zero_own)
    away = code >= REMOTE
    rank = away.astype(jnp.int32)
    table_j = lax.rem(table_lanes, both)
    step = 1
    while step < both:
        rank = rank + jnp.where(table_j >= step, pltpu.roll(rank, step, 1), 0)
        step *= 2
    job = jnp.where(away, (code - REMOTE) * both + table_j, -1)
    rank = jnp.where(away, rank - 1 + (table_lanes // both) * JOBS, -1)
    short = jnp.full(above, -1, jnp.int32)
    for at in range(half_cap * JOBS):
        best = jnp.max(jnp.where(rank == at, job, -1), axis=1, keepdims=True)
        short = jnp.where(table_lanes == at, best, short)
    job_j = lax.rem(jnp.maximum(short, 0), both)
    job_c = lax.broadcasted_iota(jnp.int32, above, 0)
    job_r = (job_j // r_slots) * (row_count * r_slots) + job_c * r_slots + lax.rem(job_j, r_slots)
    tables[row_count : 2 * row_count, :] = jnp.where(short >= 0, short // both, zero_near)
    tables[2 * row_count : 3 * row_count, :] = job_r
    code_copy = pltpu.make_async_copy(tables, codes, table_sems.at[1])
    code_copy.start()

    code_copy.wait()
    own_r.wait()
    mate_r.wait_recv()
    if scans < rounds:
        scan_step()

    def own_stage(c, carry):
        for index in range(0, half_cap, 2):
            total = None
            for j in range(0, both, 2):
                left = jnp.concatenate(
                    [pair_r[x // r_slots * row_count * r_slots + c * r_slots + x % r_slots] for x in (j, j + 1)], axis=1
                )
                right = jnp.concatenate(
                    [
                        jnp.concatenate(
                            [pair_a[codes[c, slot * both + x]] for slot in (index, index + 1)], axis=1
                        )
                        for x in (j, j + 1)
                    ],
                    axis=0,
                )
                term = jnp.dot(left, right, preferred_element_type=jnp.float32)
                total = term if total is None else total + term
            sums[c * half_cap + index] = total[:, :tile]
            sums[c * half_cap + index + 1] = total[:, tile:]
        return carry

    lag = 3
    for index in range(near_chunks):
        near_copy(index).wait_recv()
        if index < far_chunks:
            @pl.when(has_onward)
            def _():
                far_copy(index).start()
        mate_copy(near_view(index), near_pair_sems).start()
        if -1 <= index - lag < far_chunks:
            take_far(index - lag)
        lax.fori_loop(
            index * row_count // near_chunks, (index + 1) * row_count // near_chunks, own_stage, 0
        )
        if index % 3 == 1 and scans < rounds:
            scan_step()
    for index in range(max(near_chunks - lag, -1), far_chunks):
        take_far(index)
    while scans < rounds:
        scan_step()

    flags = jnp.where((scan_lane == 1) | (scan_lane == 2), state, 0)
    flags = jnp.max(jnp.max(flags, axis=1, keepdims=True), axis=0, keepdims=True)
    flag_ref[...] = jnp.broadcast_to((flags > 0).astype(jnp.int32), flag_ref.shape)
    flag_copy = pltpu.make_async_copy(flag_ref, flag_hbm, table_sems.at[0])
    flag_copy.start()
    reached = jnp.where(scan_lane == 0, state, 0)
    reached = jnp.max(jnp.max(reached, axis=1, keepdims=True), axis=0, keepdims=True)
    earlier = lax.broadcasted_iota(jnp.int32, small, 0) < lax.broadcasted_iota(jnp.int32, small, 1)
    counts = jnp.broadcast_to(own_counts, small)
    inner_sum = jnp.sum(jnp.where(earlier, counts, 0), axis=0, keepdims=True)
    offsets_ref[...] = inner_sum + (reached - total_count)

    wait_bytes(landed.at[pl.ds(0, near_slots)], near_pair_sems.at[1])

    @pl.when(has_far)
    def _():
        wait_bytes(landed.at[pl.ds(0, far_slots)], far_pair_sems.at[1])

    ahead_of = [lax.rem(index // own_cap + pairs - group // 2, pairs) for index in range(half_cap)]

    def near_stage(c, carry):
        for index in range(half_cap):
            jobs = range(index * JOBS, (index + 1) * JOBS)
            left = jnp.concatenate([pair_r[codes[2 * row_count + c, x]] for x in jobs], axis=1)
            right = jnp.concatenate([landed[codes[row_count + c, x]] for x in jobs], axis=0)
            total = sums[c * half_cap + index] + jnp.dot(
                left, right, preferred_element_type=jnp.float32
            )
            place = ahead_of[index] * row_count * own_cap + c * own_cap + index % own_cap
            out_ref[place] = total.astype(out_ref.dtype)
        return carry

    lax.fori_loop(0, row_count, near_stage, 0, unroll=4)

    flag_copy.wait()
    wait_bytes(close.at[pl.ds(0, 2)], close_sems.at[0, 0])
    to_mate.wait_send()
    mate_a.wait_send()
    mate_r.wait_send()
    early_copy.wait_send()
    place_copy.wait_send()
    wait_bytes(packed, near_send.at[0])
    if groups > 2:
        wait_bytes(told.at[pl.ds(0, groups - 1)], told_sems.at[0])
    wait_bytes(landed.at[pl.ds(0, near_slots)], near_pair_sems.at[0])

    @pl.when(has_onward)
    def _():
        wait_bytes(landed.at[pl.ds(0, far_slots)], far_send.at[0])

    @pl.when(has_far)
    def _():
        wait_bytes(close.at[pl.ds(2, 2)], close_sems.at[0, 1])
        wait_bytes(landed.at[pl.ds(0, far_slots)], far_pair_sems.at[0])

    for k in range(rounds):
        @pl.when(above_there[k])
        def _():
            scan_copy(k, 0).wait_send()

        @pl.when(below_there[k])
        def _():
            scan_copy(k, 1).wait_send()


def put_kernel(tiles_ref, offsets_ref, tiles_out, offsets_out, sems):
    copies = [
        pltpu.make_async_copy(tiles_ref, tiles_out, sems.at[0]),
        pltpu.make_async_copy(offsets_ref, offsets_out, sems.at[1]),
    ]
    for copy in copies:
        copy.start()
    for copy in copies:
        copy.wait()


def pair_sum_kernel(pairs, own, part_ref, landed, send_sems, recv_sems):
    row = lax.axis_index("rows")
    group = lax.axis_index("inner")
    core = lax.rem(group, 2)
    barrier = pltpu.get_barrier_semaphore()

    def place(ahead):
        return (row, 2 * lax.rem(group // 2 + ahead, pairs) + core)

    for ahead in range(1, pairs):
        pl.semaphore_signal(barrier, inc=1, device_id=place(ahead), device_id_type=MESH)
    pl.semaphore_wait(barrier, pairs - 1)
    copies = []
    for ahead in range(1, pairs):
        copy = pltpu.make_async_remote_copy(
            src_ref=part_ref.at[pl.ds(ahead * own, own)],
            dst_ref=landed.at[ahead - 1],
            send_sem=send_sems.at[ahead - 1],
            recv_sem=recv_sems.at[ahead - 1],
            device_id=place(ahead),
            device_id_type=MESH,
        )
        copy.start()
        copies.append(copy)
    for copy in copies:
        copy.wait()


def fused_body(rows, groups, r_tiles, r_cols, a_tiles, a_cols, c_cols, c_counts):
    local_rows, op_slots, tile, _ = a_tiles.shape
    row_count, r_slots = r_tiles.shape[:2]
    cap = c_cols.shape[1]
    tiles = local_rows * op_slots
    pairs = groups // 2
    own_cap = cap // groups
    half_cap = cap // 2
    width = -(-2 * tiles // 128) * 128
    chunks = []
    for size in [CHUNK] * (PASS_SLOTS // CHUNK) + list(LAST_CHUNKS):
        chunks.append((sum(before for _, before in chunks), size))
    list_slots = sum(size for _, size in chunks)
    pass_slots = PASS_SLOTS
    dims = (
        rows, groups, local_rows, op_slots, r_slots, cap, width, list_slots, pass_slots, tuple(chunks)
    )
    near_chunks = len(chunks)
    far_chunks = PASS_SLOTS // CHUNK
    near_slots = op_slots + list_slots
    far_slots = op_slots + pass_slots
    rounds = (rows - 1).bit_length()
    dtype = a_tiles.dtype
    out_dtype = jnp.bfloat16 if pairs == 1 else jnp.float32
    own = row_count * own_cap
    vmem = pl.BlockSpec(memory_space=pltpu.VMEM)
    anywhere = pl.BlockSpec(memory_space=pl.ANY)
    dma = pltpu.SemaphoreType.DMA
    block = (row_count, 128)
    part, offsets, flag = pl.pallas_call(
        functools.partial(fused_kernel, dims),
        out_shape=(
            jax.ShapeDtypeStruct((pairs * own, tile, tile), out_dtype),
            jax.ShapeDtypeStruct((1, row_count), jnp.int32),
            jax.ShapeDtypeStruct((1, 128), jnp.int32),
        ),
        in_specs=[anywhere] * 6,
        out_specs=(vmem, vmem, anywhere),
        scratch_shapes=[
            pltpu.VMEM((1, 128), jnp.int32),
            pltpu.VMEM(r_cols.shape, jnp.int32),
            pltpu.VMEM(c_cols.shape, jnp.int32),
            pltpu.VMEM((1, row_count), jnp.int32),
            pltpu.VMEM((op_slots, a_cols.shape[0]), jnp.int32),
            pltpu.VMEM(block, jnp.int32),
            pltpu.VMEM((5,) + block, jnp.int32),
            pltpu.VMEM((2, 8, width), jnp.int32),
            pltpu.VMEM((2 * tiles + 1, tile, tile), dtype),
            pltpu.VMEM((2 * row_count * r_slots, tile, tile), dtype),
            pltpu.VMEM((list_slots, tile, tile), dtype),
            pltpu.VMEM((2 * (near_slots + far_slots) + 1, tile, tile), dtype),
            pltpu.VMEM((row_count * half_cap, tile, tile), jnp.float32),
            pltpu.VMEM((3 * row_count, width), jnp.int32),
            pltpu.SMEM((3 * row_count, width), jnp.int32),
            pltpu.SMEM((8, width), jnp.int32),
            pltpu.VMEM((groups, 8, 128), jnp.int32),
            pltpu.VMEM((rounds, 8, 128), jnp.int32),
            pltpu.VMEM((rounds, 2, 8, 128), jnp.int32),
            dma((6,)),
            dma((2, 3)),
            dma((2, 2)),
            dma((2,)),
            dma((2,)),
            dma((near_chunks,)),
            dma((1,)),
            dma((2,)),
            dma((far_chunks + 1,)),
            dma((1,)),
            dma((2,)),
            dma((2,)),
            dma((2,)),
            dma((2, rounds, 2)),
        ],
        compiler_params=pltpu.CompilerParams(collective_id=40, has_side_effects=True),
        name="fused",
    )(
        r_cols,
        c_cols,
        c_counts[None, :],
        a_cols.T,
        a_tiles.reshape(tiles, tile, tile),
        r_tiles.reshape(row_count * r_slots, tile, tile),
    )
    if pairs == 1:
        c_tiles = part
    else:
        landed = pl.pallas_call(
            functools.partial(pair_sum_kernel, pairs, own),
            out_shape=jax.ShapeDtypeStruct((pairs - 1, own, tile, tile), jnp.float32),
            in_specs=[anywhere],
            out_specs=anywhere,
            scratch_shapes=[dma((pairs - 1,)), dma((pairs - 1,))],
            compiler_params=pltpu.CompilerParams(collective_id=41, has_side_effects=True),
            name="pair_sums",
        )(part)
        c_tiles = part[:own]
        for ahead in range(pairs - 1):
            c_tiles = c_tiles + landed[ahead]
        c_tiles = c_tiles.astype(jnp.bfloat16)
    return c_tiles.reshape(row_count, own_cap, tile, tile), offsets[0], flag[0, 0]


def body(rows, groups, *args):
    if rows % 2 or groups % 2:
        return plain_body(rows, groups, *args)
    c_tiles, offsets, flag = fused_body(rows, groups, *args)

    def again(c_tiles, offsets, *args):
        return plain_body(rows, groups, *args)

    def keep(c_tiles, offsets, *args):
        return c_tiles, offsets

    c_tiles, offsets = lax.cond(flag > 0, again, keep, c_tiles, offsets, *args)
    vmem = pl.BlockSpec(memory_space=pltpu.VMEM)
    anywhere = pl.BlockSpec(memory_space=pl.ANY)
    c_tiles, offsets = pl.pallas_call(
        put_kernel,
        out_shape=(
            jax.ShapeDtypeStruct(c_tiles.shape, c_tiles.dtype),
            jax.ShapeDtypeStruct((1,) + offsets.shape, offsets.dtype),
        ),
        in_specs=[vmem, vmem],
        out_specs=(anywhere, anywhere),
        scratch_shapes=[pltpu.SemaphoreType.DMA((2,))],
        name="put",
    )(c_tiles, offsets[None, :])
    return c_tiles, offsets[0]


def solution(mesh):
    rows = mesh.shape["rows"]
    groups = mesh.shape["inner"]
    return jax.shard_map(
        functools.partial(body, rows, groups),
        mesh=mesh,
        in_specs=(
            P("rows", "inner", None, None),
            P("rows", "inner"),
            P(("rows", "inner"), None, None, None),
            P(),
            P("rows", None),
            P("rows"),
        ),
        out_specs=(P("rows", "inner", None, None), P("rows")),
        check_vma=False,
    )
```

```python
import functools

import jax
import jax.numpy as jnp
from jax import lax
from jax.experimental import pallas as pl
from jax.experimental.pallas import tpu as pltpu
from jax.sharding import PartitionSpec as P

MESH = pl.DeviceIdType.MESH
BATCH = 4


def plan_kernel(
    dims, r_cols_ref, c_cols_ref, counts_ref, columns_ref, code_ref, plan_ref,
    meta_ref, gathered, needs, send_sem, recv_sem,
):
    rows, groups, local_rows, op_slots, r_slots, cap, half = dims
    width = 2 * half
    count = rows * groups
    tiles = local_rows * op_slots
    row = lax.axis_index("rows")
    group = lax.axis_index("inner")
    me = row * groups + group

    barrier = pltpu.get_barrier_semaphore()

    def place(step):
        other = lax.rem(me + step, count)
        return (other // groups, lax.rem(other, groups))

    def greet(step, carry):
        pl.semaphore_signal(barrier, inc=1, device_id=place(step), device_id_type=MESH)
        return carry

    lax.fori_loop(1, count, greet, 0)
    row_count = r_cols_ref.shape[0]
    live = r_slots + cap
    lanes = lax.broadcasted_iota(jnp.int32, (row_count, width), 1)
    above = lax.broadcasted_iota(jnp.int32, (row_count, width), 0)
    small = (row_count, row_count)
    diagonal = lax.broadcasted_iota(jnp.int32, small, 0) == lax.broadcasted_iota(jnp.int32, small, 1)
    spread_counts = jnp.broadcast_to(counts_ref[...], small)
    own_counts = jnp.sum(jnp.where(diagonal, spread_counts, 0), axis=1, keepdims=True)
    meta_ref[...] = jnp.full(meta_ref.shape, -9, jnp.int32)
    meta_ref[:, 0:r_slots] = r_cols_ref[...]
    meta_ref[:, r_slots:live] = c_cols_ref[...]
    meta_ref[:, live : live + 1] = own_counts
    gathered[me] = meta_ref[...]
    pl.semaphore_wait(barrier, count - 1)

    def post(step, carry):
        pltpu.make_async_remote_copy(
            src_ref=meta_ref,
            dst_ref=gathered.at[me],
            send_sem=send_sem,
            recv_sem=recv_sem,
            device_id=place(step),
            device_id_type=MESH,
        ).start()
        return carry

    lax.fori_loop(1, count, post, 0)
    everyone = gathered.at[pl.ds(0, count - 1)]
    pltpu.make_async_copy(everyone, everyone, send_sem).wait()
    pltpu.make_async_copy(everyone, everyone, recv_sem).wait()

    def matches(block, columns, fine_rows):
        named = fine_rows == block[:, 0:1]
        for j in range(1, r_slots):
            named = named | (fine_rows == block[:, j : j + 1])
        slot = jnp.full((row_count, width), -1, jnp.int32)
        for s in range(cap):
            slot = jnp.where(columns == block[:, r_slots + s : r_slots + s + 1], s, slot)
        return jnp.where(named, slot, -1)

    shift = jnp.where(lanes < half, -groups, groups) * local_rows
    tile = jnp.where(lanes < half, lanes, lanes - half)
    lane_rows = jnp.where(tile < tiles, shift + tile // op_slots, -(1 << 24))
    low_lanes = lanes[0:1] < half

    def near_matches(device):
        before = columns_ref[pl.ds(jnp.maximum(device - groups, 0), 1), :]
        after = columns_ref[pl.ds(jnp.minimum(device + groups, count - 1), 1), :]
        columns = jnp.where(low_lanes, before, after)
        return matches(gathered[device], columns, lane_rows + device * local_rows)

    def wanted(found):
        return jnp.max((found >= 0).astype(jnp.int32), axis=0, keepdims=True)

    def gather_needs(device, carry):
        needs[pl.ds(device, 1), :] = wanted(near_matches(device))
        return carry

    lax.fori_loop(0, count, gather_needs, 0, unroll=4)
    every = needs[...]
    low_side = lax.broadcasted_iota(jnp.int32, every.shape, 1) < half
    low = jnp.sum(jnp.where(low_side, every, 0), axis=1, keepdims=True)
    high = jnp.sum(jnp.where(low_side, 0, every), axis=1, keepdims=True)
    most = jnp.max(jnp.maximum(low, high), axis=0, keepdims=True)

    down = lax.broadcasted_iota(jnp.int32, (width, width), 0)
    across = lax.broadcasted_iota(jnp.int32, (width, width), 1)
    same = (down < half) == (across < half)

    def ranks(need):
        spread = jnp.broadcast_to(need, (width, width))
        column = jnp.sum(jnp.where(down == across, spread, 0), axis=1, keepdims=True)
        before = jnp.sum(jnp.where((across < down) & same, spread, 0), axis=1, keepdims=True)
        along = jnp.sum(
            jnp.where((down < across) & same, jnp.broadcast_to(column, (width, width)), 0),
            axis=0,
            keepdims=True,
        )
        return column, before, along

    def send_list(device, high):
        column, before, _ = ranks(needs[pl.ds(device, 1), :])
        first = half if high else 0
        mine = (down >= half) if high else (down < half)
        chosen = mine & (column > 0) & (before == across)
        return jnp.sum(jnp.where(chosen, down - first, 0), axis=0, keepdims=True)

    left = jnp.maximum(row - 1, 0) * groups + group
    right = jnp.minimum(row + 1, rows - 1) * groups + group
    plan_ref[0:1, :] = send_list(left, True)
    plan_ref[1:2, :] = send_list(right, False)

    found = near_matches(me)
    _, _, along = ranks(wanted(found))
    slot_at = along + jnp.where(lanes[0:1] < half, tiles, 2 * tiles)
    code_ref[:, 0:width] = jnp.where(found >= 0, found + cap * slot_at, -1)
    fine = me * local_rows + jnp.where(lanes < tiles, lanes // op_slots, 0)
    fine = jnp.where(lanes < tiles, fine, -5)
    found = matches(gathered[me], columns_ref[pl.ds(me, 1), :], fine)
    code_ref[:, width:] = jnp.where(found >= 0, found + cap * lanes, -1)

    def earlier(index, total):
        block = gathered[index * groups]
        return total + jnp.sum(block[:, live : live + 1], axis=0, keepdims=True)

    first = lax.fori_loop(0, row, earlier, jnp.zeros((1, 1), jnp.int32))
    counts = jnp.broadcast_to(own_counts, (row_count, width))
    inner_sum = jnp.sum(jnp.where(above < lanes, counts, 0), axis=0, keepdims=True)
    plan_ref[2:3, :] = inner_sum + first
    level = jnp.zeros((1, 1), jnp.int32)
    for size in sizes_for(tiles)[:-1]:
        level = level + (most > size).astype(jnp.int32)
    plan_ref[3:4, :] = jnp.broadcast_to(level, (1, width))


def halo_kernel(rows, size, plan_ref, a_ref, out_ref, packed, send_sems, recv_sems):
    row = lax.axis_index("rows")
    group = lax.axis_index("inner")
    barrier = pltpu.get_barrier_semaphore()
    has_left = row > 0
    has_right = row < rows - 1

    @pl.when(has_left)
    def _():
        pl.semaphore_signal(barrier, inc=1, device_id=(row - 1, group), device_id_type=MESH)

    @pl.when(has_right)
    def _():
        pl.semaphore_signal(barrier, inc=1, device_id=(row + 1, group), device_id_type=MESH)

    def pack(index, carry):
        packed[0, index] = a_ref[plan_ref[0, index]]
        packed[1, index] = a_ref[plan_ref[1, index]]
        return carry

    lax.fori_loop(0, size, pack, 0, unroll=2)

    pl.semaphore_wait(barrier, has_left.astype(jnp.int32) + has_right.astype(jnp.int32))

    def copy(side, other):
        return pltpu.make_async_remote_copy(
            src_ref=packed.at[side],
            dst_ref=out_ref.at[1 - side, pl.ds(0, size)],
            send_sem=send_sems.at[side],
            recv_sem=recv_sems.at[1 - side],
            device_id=(other, group),
            device_id_type=MESH,
        )

    @pl.when(has_left)
    def _():
        copy(0, row - 1).start()

    @pl.when(has_right)
    def _():
        copy(1, row + 1).start()

    @pl.when(has_left)
    def _():
        copy(0, row - 1).wait_send()
        copy(1, row - 1).wait_recv()

    @pl.when(has_right)
    def _():
        copy(1, row + 1).wait_send()
        copy(0, row + 1).wait_recv()


def product_kernel(dims, code_ref, cols_ref, r_ref, a_ref, halo_ref, out_ref, tiles_ref, jobs, sems):
    rows, groups, local_rows, op_slots, r_slots, cap, half = dims
    width = 2 * half
    tiles = local_rows * op_slots
    row_count = cols_ref.shape[0]
    own_cap = cap // groups
    row = lax.axis_index("rows")
    group = lax.axis_index("inner")
    own = pltpu.make_async_copy(a_ref, tiles_ref.at[pl.ds(0, tiles)], sems.at[0])
    near = pltpu.make_async_copy(halo_ref, tiles_ref.at[pl.ds(tiles, 2 * tiles)], sems.at[1])
    own.start()
    near.start()
    last = groups * row_count * own_cap
    scale = 1 << (3 * tiles * cap - 1).bit_length()

    def clear(index, carry):
        out_ref[index] = jnp.zeros(out_ref.shape[1:], jnp.float32)
        return carry

    lax.fori_loop(0, last, clear, 0, unroll=4)

    def list_row(c, found):
        def list_slot(j, found):
            fine = cols_ref[c, j]
            side = fine // (local_rows * groups) - row
            base = jnp.where(side == 0, width, jnp.where(side < 0, 0, half))
            base = base + lax.rem(fine, local_rows) * op_slots
            for t in range(op_slots):
                code = code_ref[c, base + t]
                jobs[found] = (c * r_slots + j) * scale + code
                found = found + (code >= 0).astype(jnp.int32)
            return found

        return lax.fori_loop(0, r_slots, list_slot, found)

    found = lax.fori_loop(0, row_count, list_row, jnp.int32(0))
    for extra in range(BATCH):
        jobs[found + extra] = -1
    own.wait()
    near.wait()

    def batch(step, carry):
        results = []
        targets = []
        for extra in range(BATCH):
            job = jobs[step * BATCH + extra]
            valid = job >= 0
            job = jnp.maximum(job, 0)
            pair = job // scale
            code = lax.rem(job, scale)
            slot = lax.rem(code, cap)
            ahead = lax.rem(slot // own_cap + groups - group, groups)
            target = (ahead * row_count + pair // r_slots) * own_cap + lax.rem(slot, own_cap)
            targets.append(jnp.where(valid, target, last))
            results.append(
                jnp.dot(
                    r_ref[pair],
                    tiles_ref[code // cap],
                    preferred_element_type=jnp.float32,
                )
            )
        for extra in range(BATCH):
            target = targets[extra]
            out_ref[target] = out_ref[target] + results[extra]
        return carry

    lax.fori_loop(0, (found + BATCH - 1) // BATCH, batch, 0)


def sum_kernel(groups, own, part_ref, landed, send_sems, recv_sems):
    row = lax.axis_index("rows")
    group = lax.axis_index("inner")
    barrier = pltpu.get_barrier_semaphore()
    for ahead in range(1, groups):
        pl.semaphore_signal(
            barrier, inc=1, device_id=(row, lax.rem(group + ahead, groups)), device_id_type=MESH
        )
    pl.semaphore_wait(barrier, groups - 1)
    copies = []
    for ahead in range(1, groups):
        copy = pltpu.make_async_remote_copy(
            src_ref=part_ref.at[pl.ds(ahead * own, own)],
            dst_ref=landed.at[ahead - 1],
            send_sem=send_sems.at[ahead - 1],
            recv_sem=recv_sems.at[ahead - 1],
            device_id=(row, lax.rem(group + ahead, groups)),
            device_id_type=MESH,
        )
        copy.start()
        copies.append(copy)
    for copy in copies:
        copy.wait()


def sizes_for(tiles):
    steps = [16, 18, 20, 21, 22, 23, 24, 25, 26, 27, 28, 29, 30, 32, 36, 42]
    return [size for size in steps if size < tiles] + [tiles]


def plain_body(rows, groups, r_tiles, r_cols, a_tiles, a_cols, c_cols, c_counts):
    local_rows, op_slots, tile, _ = a_tiles.shape
    row_count, r_slots = r_tiles.shape[:2]
    cap = c_cols.shape[1]
    tiles = local_rows * op_slots
    half = -(-tiles // 64) * 64
    width = 2 * half
    count = rows * groups
    own_cap = cap // groups
    dims = (rows, groups, local_rows, op_slots, r_slots, cap, half)
    vmem = pl.BlockSpec(memory_space=pltpu.VMEM)
    smem = pl.BlockSpec(memory_space=pltpu.SMEM)
    anywhere = pl.BlockSpec(memory_space=pl.ANY)

    flat = a_cols.reshape(count, tiles)
    flat = jnp.pad(flat, ((0, 0), (0, half - tiles)), constant_values=-2)
    columns = jnp.concatenate([flat, flat], axis=1)

    code, plan = pl.pallas_call(
        functools.partial(plan_kernel, dims),
        out_shape=(
            jax.ShapeDtypeStruct((row_count, 2 * width), jnp.int32),
            jax.ShapeDtypeStruct((8, width), jnp.int32),
        ),
        in_specs=[vmem] * 4,
        out_specs=(vmem, vmem),
        scratch_shapes=[
            pltpu.VMEM((row_count, width), jnp.int32),
            pltpu.VMEM((count, row_count, width), jnp.int32),
            pltpu.VMEM((count, width), jnp.int32),
            pltpu.SemaphoreType.DMA,
            pltpu.SemaphoreType.DMA,
        ],
        compiler_params=pltpu.CompilerParams(collective_id=0, has_side_effects=True),
        name="plan",
    )(r_cols, c_cols, c_counts[None, :], columns)

    flat_a = a_tiles.reshape(tiles, tile, tile)
    sizes = sizes_for(tiles)

    def exchange(number, size, plan, flat_a):
        return pl.pallas_call(
            functools.partial(halo_kernel, rows, size),
            out_shape=jax.ShapeDtypeStruct((2, tiles, tile, tile), a_tiles.dtype),
            in_specs=[smem, vmem],
            out_specs=anywhere,
            scratch_shapes=[
                pltpu.VMEM((2, size, tile, tile), a_tiles.dtype),
                pltpu.SemaphoreType.DMA((2,)),
                pltpu.SemaphoreType.DMA((2,)),
            ],
            compiler_params=pltpu.CompilerParams(collective_id=number + 2, has_side_effects=True),
            name=f"halo{size}",
        )(plan, flat_a)

    halo = lax.switch(
        plan[3, 0],
        [functools.partial(exchange, number, size) for number, size in enumerate(sizes)],
        plan,
        flat_a,
    )

    slots = row_count * r_slots * op_slots + BATCH
    partial_value = pl.pallas_call(
        functools.partial(product_kernel, dims),
        out_shape=jax.ShapeDtypeStruct((row_count * cap + 1, tile, tile), jnp.float32),
        in_specs=[smem, smem, vmem, anywhere, anywhere],
        out_specs=vmem,
        scratch_shapes=[
            pltpu.VMEM((3 * tiles, tile, tile), a_tiles.dtype),
            pltpu.SMEM((slots,), jnp.int32),
            pltpu.SemaphoreType.DMA((2,)),
        ],
        name="products",
    )(
        code,
        r_cols,
        r_tiles.reshape(row_count * r_slots, tile, tile),
        flat_a,
        halo.reshape(2 * tiles, tile, tile),
    )

    own_count = row_count * own_cap
    landed = pl.pallas_call(
        functools.partial(sum_kernel, groups, own_count),
        out_shape=jax.ShapeDtypeStruct((groups - 1, own_count, tile, tile), jnp.float32),
        in_specs=[anywhere],
        out_specs=anywhere,
        scratch_shapes=[
            pltpu.SemaphoreType.DMA((groups - 1,)),
            pltpu.SemaphoreType.DMA((groups - 1,)),
        ],
        compiler_params=pltpu.CompilerParams(collective_id=1, has_side_effects=True),
        name="sums",
    )(partial_value)
    c_tiles = partial_value[:own_count]
    for ahead in range(groups - 1):
        c_tiles = c_tiles + landed[ahead]
    c_tiles = c_tiles.astype(jnp.bfloat16)
    return (c_tiles.reshape(row_count, own_cap, tile, tile), plan[2, :row_count])

EARLY = 7
PASS_SLOTS = 15
CHUNK = 3
LAST_CHUNKS = (3, 3, 3, 2)
JOBS = 4
REMOTE = 1 << 14


def fused_kernel(
    dims, r_cols_hbm, c_cols_hbm, counts_hbm, columns_hbm, a_ref, r_ref,
    out_ref, offsets_ref, flag_hbm,
    flag_ref, r_cols_ref, c_cols_ref, counts_ref, columns_ref,
    meta, close, placing, pair_a, pair_r, packed, landed, sums, tables, codes, picks,
    told, scan_out, scan_in,
    local_sems, close_sems, pair_sems, place_sems, early_sems, near_sems, near_send,
    near_pair_sems, far_sems, far_send, far_pair_sems, table_sems, told_sems, scan_sems,
):
    (rows, groups, local_rows, op_slots, r_slots, cap, width, list_slots, pass_slots, chunks) = dims
    pairs = groups // 2
    tiles = local_rows * op_slots
    span = 2 * local_rows
    own_cap = cap // groups
    half_cap = cap // 2
    both = 2 * r_slots
    row_count = r_cols_ref.shape[0]
    live = r_slots + cap
    early = min(EARLY, op_slots)
    near_slots = early + list_slots
    far_slots = early + pass_slots
    near_chunks = len(chunks)
    far_chunks = sum(start < pass_slots for start, _ in chunks)
    last_slots = chunks[-1][1]
    far_base = 2 * near_slots
    zero_near = 2 * (near_slots + far_slots)
    zero_own = 2 * tiles
    rounds = (rows - 1).bit_length()

    row = lax.axis_index("rows")
    group = lax.axis_index("inner")
    part = lax.rem(group, 2)
    first_group = group - part
    mate = first_group + 1 - part
    odd = lax.rem(row, 2)
    near = row + 1 - 2 * odd
    far = row - 1 + 2 * odd
    has_far = (far >= 0) & (far < rows)
    onward = near + 1 - 2 * odd
    has_onward = (onward >= 0) & (onward < rows)
    mate_place = (row, mate)

    barrier = pltpu.get_barrier_semaphore()

    def greet(place):
        pl.semaphore_signal(barrier, inc=1, device_id=place, device_id_type=MESH)

    for core in range(2):
        greet((near, first_group + core))

    @pl.when(has_far)
    def _():
        for core in range(2):
            greet((far, first_group + core))

    for ahead in range(1, groups):
        greet((row, lax.rem(group + ahead, groups)))

    small_copies = [
        pltpu.make_async_copy(src, dst, local_sems.at[2 + index])
        for index, (src, dst) in enumerate(
            [
                (r_cols_hbm, r_cols_ref),
                (c_cols_hbm, c_cols_ref),
                (counts_hbm, counts_ref),
                (columns_hbm, columns_ref),
            ]
        )
    ]
    for copy in small_copies:
        copy.start()
    own_a = pltpu.make_async_copy(
        a_ref, pair_a.at[pl.ds(part * tiles, tiles)], local_sems.at[0]
    )
    own_r = pltpu.make_async_copy(r_ref, pair_r.at[pl.ds(part * row_count * r_slots, row_count * r_slots)], local_sems.at[1])
    own_a.start()
    own_r.start()

    def remote(src, dst, send_sem, recv_sem, place):
        return pltpu.make_async_remote_copy(
            src_ref=src, dst_ref=dst, send_sem=send_sem, recv_sem=recv_sem,
            device_id=place, device_id_type=MESH,
        )

    def wait_bytes(view, sem):
        pltpu.make_async_copy(view, view, sem).wait()

    small = (row_count, row_count)
    diagonal = lax.broadcasted_iota(jnp.int32, small, 0) == lax.broadcasted_iota(jnp.int32, small, 1)
    meta[...] = jnp.full(meta.shape, -9, jnp.int32)
    pair_a[zero_own] = jnp.zeros(pair_a.shape[1:], pair_a.dtype)
    landed[zero_near] = jnp.zeros(landed.shape[1:], landed.dtype)
    for copy in small_copies:
        copy.wait()
    spread_counts = jnp.broadcast_to(counts_ref[...], small)
    own_counts = jnp.sum(jnp.where(diagonal, spread_counts, 0), axis=1, keepdims=True)
    meta[:, 0:r_slots] = r_cols_ref[...]
    meta[:, r_slots:live] = c_cols_ref[...]
    pl.semaphore_wait(barrier, groups + 1 + 2 * has_far.astype(jnp.int32))

    def start_close(target, first, which):
        for core in range(2):
            remote(
                meta, close.at[first + part], close_sems.at[0, which], close_sems.at[1, which],
                (target, first_group + core),
            ).start()

    @pl.when(has_far)
    def _():
        start_close(far, 2, 1)

    start_close(near, 0, 0)
    to_mate = remote(meta, close.at[4], close_sems.at[0, 2], close_sems.at[1, 2], mate_place)
    to_mate.start()
    mate_a = remote(
        a_ref, pair_a.at[pl.ds(part * tiles, tiles)], pair_sems.at[0, 0], pair_sems.at[1, 0], mate_place
    )
    mate_a.start()

    own_a.wait()
    early_copy = remote(
        pair_a.at[pl.ds(part * tiles, early)], landed.at[pl.ds(part * near_slots, early)],
        early_sems.at[0], early_sems.at[1], (near, group),
    )
    early_copy.start()
    mate_r = remote(r_ref, pair_r.at[pl.ds(part * row_count * r_slots, row_count * r_slots)], pair_sems.at[0, 1], pair_sems.at[1, 1], mate_place)
    mate_r.start()

    lanes = lax.broadcasted_iota(jnp.int32, (1, width), 1)
    real = lanes < op_slots * span
    lane_slot = lanes // span
    lane_fine = jnp.where(real, lax.rem(lanes, span), -(1 << 24))
    lane_core = lax.rem(lanes, span) // local_rows
    lane_local = lax.rem(lanes, local_rows)
    lane_tile = lane_core * tiles + lane_local * op_slots + lane_slot
    late = jnp.where((lane_local > 0) | (lane_slot >= early), 1, 0)

    def pair_columns(which_row):
        start = (which_row * groups + first_group) * local_rows
        block = start // 128
        values = columns_ref[:, pl.ds(pl.multiple_of(block * 128, 128), 128)]
        if width > 128:
            values = jnp.concatenate([values] * (width // 128), axis=1)
        offset = start - block * 128
        total = jnp.zeros((1, width), jnp.int32)
        for t in range(op_slots):
            moved = pltpu.roll(values[t : t + 1, :], lax.rem(t * span - offset + 128 * width, width), 1)
            total = jnp.where(lane_slot == t, moved, total)
        return jnp.where(real, total, -2)

    def pair_fine(which_row):
        return lane_fine + (which_row * groups + first_group) * local_rows

    def named_by(meta_low, meta_high, fine):
        named = fine == meta_low[:, 0:1]
        for j in range(1, r_slots):
            named = named | (fine == meta_low[:, j : j + 1])
        for j in range(r_slots):
            named = named | (fine == meta_high[:, j : j + 1])
        return named

    def need_by_core(meta_low, meta_high, columns, fine):
        named = named_by(meta_low, meta_high, fine)
        needs = []
        for core in range(2):
            wanted = jnp.zeros(named.shape, jnp.bool_)
            for s in range(cap):
                if s // own_cap % 2 == core:
                    wanted = wanted | (columns == meta_low[:, r_slots + s : r_slots + s + 1])
            needs.append(jnp.max((named & wanted).astype(jnp.int32), axis=0, keepdims=True))
        return needs

    def need_of(meta_low, meta_high, columns, fine):
        low, high = need_by_core(meta_low, meta_high, columns, fine)
        return jnp.maximum(low, high)

    def before(need):
        total = need
        step = 1
        while step < width:
            total = total + jnp.where(lanes >= step, pltpu.roll(total, step, 1), 0)
            step *= 2
        return total - need

    def landing(places, count, base, slots):
        fits = (places >= 0) & (places < 2 * count)
        at = lax.rem(places, 2) * slots + early + places // 2
        at = jnp.where(late > 0, jnp.where(fits, at, -1), lane_core * slots + lane_slot)
        return jnp.where(real & (at >= 0), REMOTE + base + at, -1)

    own_columns = pair_columns(row)
    own_fine = pair_fine(row)

    near_columns = pair_columns(near)
    near_fine = pair_fine(near)
    far_row = jnp.clip(far, 0, rows - 1)
    far_columns = pair_columns(far_row)
    far_fine = jnp.where(has_far, pair_fine(far_row), -(1 << 24))
    to_mate.wait_recv()
    mine, other = meta[...], close[4]
    my_low = jnp.where(part == 0, mine, other)
    my_high = jnp.where(part == 0, other, mine)
    near_named = named_by(my_low, my_high, near_fine)
    far_named = named_by(my_low, my_high, far_fine)
    crowded = jnp.zeros((1, 1), jnp.int32)
    for s in range(cap):
        column = my_low[:, r_slots + s : r_slots + s + 1]
        hits = (near_named & (near_columns == column)).astype(jnp.int32)
        hits = hits + (far_named & (far_columns == column)).astype(jnp.int32)
        held = jnp.sum(hits, axis=1, keepdims=True)
        crowded = jnp.maximum(crowded, jnp.max(held, axis=0, keepdims=True))

    wait_bytes(close.at[pl.ds(0, 2)], close_sems.at[1, 0])
    near_low, near_high = [
        need * late for need in need_by_core(close[0], close[1], own_columns, own_fine)
    ]

    @pl.when(has_far)
    def _():
        wait_bytes(close.at[pl.ds(2, 2)], close_sems.at[1, 1])

    @pl.when(jnp.logical_not(has_far))
    def _():
        close[2] = jnp.full(close.shape[1:], -9, jnp.int32)
        close[3] = jnp.full(close.shape[1:], -9, jnp.int32)

    need_far = need_of(close[2], close[3], own_columns, own_fine) * late
    need_only = jnp.maximum(near_low, near_high) * (1 - need_far)
    lone_low = need_only * (1 - near_high)
    lone_high = need_only * (1 - near_low)
    counts_before = before(jnp.concatenate([need_far, lone_low, lone_high], axis=0))
    far_before, low_before, high_before = [counts_before[x : x + 1] for x in range(3)]
    far_total = jnp.sum(need_far, axis=1, keepdims=True)
    last_low = (lone_low > 0) & (low_before < last_slots)
    last_high = (lone_high > 0) & (high_before < last_slots)
    need_rest = jnp.where(last_low | last_high, 0, need_only)
    near_total = far_total + jnp.sum(need_rest, axis=1, keepdims=True)
    places = jnp.where(
        need_far > 0, far_before, jnp.where(need_rest > 0, before(need_rest) + far_total, -1)
    )
    last_first = list_slots - last_slots
    places = jnp.where(places < 2 * last_first, places, -1)
    places = jnp.where(last_low, 2 * (last_first + low_before), places)
    places = jnp.where(last_high, 2 * (last_first + high_before) + 1, places)
    pick_rows = -(-list_slots // 8) * 8
    slot_down = lax.broadcasted_iota(jnp.int32, (pick_rows, width), 0)
    chosen = jnp.broadcast_to(places, (pick_rows, width)) == 2 * slot_down + part
    picked = jnp.sum(
        jnp.where(chosen, jnp.broadcast_to(lane_tile, (pick_rows, width)), 0), axis=1, keepdims=True
    )
    across = lax.broadcasted_iota(jnp.int32, (pick_rows, width), 1)
    pick_row = jnp.sum(
        jnp.where(slot_down == across, jnp.broadcast_to(picked, (pick_rows, width)), 0),
        axis=0, keepdims=True,
    )
    tables[0:8, :] = jnp.broadcast_to(pick_row, (8, width))
    pick_copy = pltpu.make_async_copy(tables.at[pl.ds(0, 8)], picks, table_sems.at[0])
    pick_copy.start()
    placing[0] = jnp.broadcast_to(landing(places, list_slots, 0, near_slots), placing.shape[1:])
    place_copy = remote(placing.at[0], placing.at[1], place_sems.at[0], place_sems.at[1], (near, group))
    place_copy.start()
    over = jnp.maximum(near_total - 2 * (list_slots - last_slots), far_total - 2 * pass_slots)
    over = jnp.maximum(over, crowded - JOBS)
    over = (over > 0).astype(jnp.int32)
    if groups > 2:
        told[group] = jnp.broadcast_to(over, told.shape[1:])

        def tell(ahead):
            return remote(
                told.at[group], told.at[group], told_sems.at[0], told_sems.at[1],
                (row, lax.rem(group + ahead, groups)),
            )

        for ahead in range(1, groups):
            tell(ahead).start()
        wait_bytes(told.at[pl.ds(0, groups - 1)], told_sems.at[1])
        over = told[0]
        for other_group in range(1, groups):
            over = over + told[other_group]

    tile = pair_a.shape[1]
    total_count = jnp.sum(own_counts, axis=0, keepdims=True)

    def scan_copy(k, side):
        other = row + (1 << k) if side == 0 else row - (1 << k)
        return remote(
            scan_out.at[k], scan_in.at[k, side], scan_sems.at[0, k, side], scan_sems.at[1, k, side],
            (other, group),
        )

    scan_shape = scan_out.shape[1:]
    scan_lane = lax.broadcasted_iota(jnp.int32, scan_shape, 1)
    above_there = [row + (1 << k) < rows for k in range(rounds)]
    below_there = [row - (1 << k) >= 0 for k in range(rounds)]

    def scan_send(k, state):
        scan_out[k] = state

        @pl.when(above_there[k])
        def _():
            scan_copy(k, 0).start()

        @pl.when(below_there[k])
        def _():
            scan_copy(k, 1).start()

    def scan_take(k, state):
        @pl.when(below_there[k])
        def _():
            scan_copy(k, 0).wait_recv()

        @pl.when(above_there[k])
        def _():
            scan_copy(k, 1).wait_recv()

        below = jnp.where((scan_lane < 2) & below_there[k], scan_in[k, 0], 0)
        beyond = jnp.where((scan_lane == 2) & above_there[k], scan_in[k, 1], 0)
        return state + below + beyond

    state = jnp.where(
        scan_lane == 0, jnp.broadcast_to(total_count, scan_shape),
        jnp.where(scan_lane < 3, over, 0),
    )
    scan_send(0, state)
    scans = 0

    def scan_step():
        nonlocal state, scans
        state = scan_take(scans, state)
        scans += 1
        if scans < rounds:
            scan_send(scans, state)

    mate_a.wait_recv()
    pick_copy.wait()

    def near_view(index):
        start, size = chunks[index]
        return landed.at[pl.ds(part * near_slots + early + start, size)]

    def near_copy(index):
        return remote(
            packed.at[pl.ds(*chunks[index])], near_view(index),
            near_send.at[0], near_sems.at[index], (near, group),
        )

    def pack(index):
        start, size = chunks[index]
        for slot in range(start, start + size):
            packed[slot] = pair_a[picks[0, slot]]

    pack(0)
    for index in range(near_chunks):
        if index + 1 < near_chunks:
            pack(index + 1)
        near_copy(index).start()

    def mate_copy(view, sems):
        return remote(view, view, sems.at[0], sems.at[1], mate_place)

    early_view = landed.at[pl.ds(part * near_slots, early)]
    early_far_view = landed.at[pl.ds(far_base + part * far_slots, early)]

    def far_view(index):
        start, size = chunks[index]
        return landed.at[pl.ds(far_base + part * far_slots + early + start, size)]

    early_far = remote(early_view, early_far_view, far_send.at[0], far_sems.at[far_chunks], (onward, group))

    def far_copy(index):
        return remote(
            near_view(index), far_view(index), far_send.at[0], far_sems.at[index], (onward, group)
        )

    def take_far(index):
        @pl.when(has_far)
        def _():
            if index < 0:
                early_far.wait_recv()
                mate_copy(early_far_view, far_pair_sems).start()
            else:
                far_copy(index).wait_recv()
                mate_copy(far_view(index), far_pair_sems).start()

    early_copy.wait_recv()

    @pl.when(has_onward)
    def _():
        early_far.start()

    mate_copy(early_view, near_pair_sems).start()
    if scans < rounds:
        scan_step()
    far_need = need_of(my_low, my_high, far_columns, far_fine) * late
    far_places = jnp.where(far_need > 0, before(far_need), -1)
    far_at = landing(far_places, pass_slots, far_base, far_slots)
    place_copy.wait_recv()
    near_at = placing[1][0:1, :]

    above = (row_count, width)
    table_lanes = lax.broadcasted_iota(jnp.int32, above, 1)
    own_at, near_at, far_at = [jnp.broadcast_to(x, above) for x in (lane_tile, near_at, far_at)]
    slot_own, slot_near, slot_far = [], [], []
    for index in range(half_cap):
        even = (2 * (index // own_cap)) * own_cap + index % own_cap
        low = my_low[:, r_slots + even : r_slots + even + 1]
        high = my_low[:, r_slots + even + own_cap : r_slots + even + own_cap + 1]
        column = jnp.where(part == 0, low, high)
        slot_own.append(jnp.where(own_columns == column, own_at, -1))
        slot_near.append(jnp.where(near_columns == column, near_at, -1))
        slot_far.append(jnp.where(far_columns == column, far_at, -1))
    code = jnp.full(above, -1, jnp.int32)
    for j in range(both):
        block = my_low if j < r_slots else my_high
        named = block[:, j % r_slots : j % r_slots + 1]
        in_own = own_fine == named
        in_near = near_fine == named
        in_far = far_fine == named
        for index in range(half_cap):
            found = jnp.where(in_own, slot_own[index], -1)
            found = jnp.where(in_near, slot_near[index], found)
            found = jnp.where(in_far, slot_far[index], found)
            best = jnp.max(found, axis=1, keepdims=True)
            code = jnp.where(table_lanes == index * both + j, best, code)
    tables[0:row_count, :] = jnp.where((code >= 0) & (code < REMOTE), code, zero_own)
    away = code >= REMOTE
    rank = away.astype(jnp.int32)
    table_j = lax.rem(table_lanes, both)
    step = 1
    while step < both:
        rank = rank + jnp.where(table_j >= step, pltpu.roll(rank, step, 1), 0)
        step *= 2
    job = jnp.where(away, (code - REMOTE) * both + table_j, -1)
    rank = jnp.where(away, rank - 1 + (table_lanes // both) * JOBS, -1)
    short = jnp.full(above, -1, jnp.int32)
    for at in range(half_cap * JOBS):
        best = jnp.max(jnp.where(rank == at, job, -1), axis=1, keepdims=True)
        short = jnp.where(table_lanes == at, best, short)
    job_j = lax.rem(jnp.maximum(short, 0), both)
    job_c = lax.broadcasted_iota(jnp.int32, above, 0)
    job_r = (job_j // r_slots) * (row_count * r_slots) + job_c * r_slots + lax.rem(job_j, r_slots)
    tables[row_count : 2 * row_count, :] = jnp.where(short >= 0, short // both, zero_near)
    tables[2 * row_count : 3 * row_count, :] = job_r
    code_copy = pltpu.make_async_copy(tables, codes, table_sems.at[1])
    code_copy.start()

    code_copy.wait()
    own_r.wait()
    mate_r.wait_recv()
    if scans < rounds:
        scan_step()

    def own_stage(c, carry):
        for index in range(0, half_cap, 2):
            total = None
            for j in range(0, both, 2):
                left = jnp.concatenate(
                    [pair_r[x // r_slots * row_count * r_slots + c * r_slots + x % r_slots] for x in (j, j + 1)], axis=1
                )
                right = jnp.concatenate(
                    [
                        jnp.concatenate(
                            [pair_a[codes[c, slot * both + x]] for slot in (index, index + 1)], axis=1
                        )
                        for x in (j, j + 1)
                    ],
                    axis=0,
                )
                term = jnp.dot(left, right, preferred_element_type=jnp.float32)
                total = term if total is None else total + term
            sums[c * half_cap + index] = total[:, :tile]
            sums[c * half_cap + index + 1] = total[:, tile:]
        return carry

    lag = 3
    for index in range(near_chunks):
        near_copy(index).wait_recv()
        if index < far_chunks:
            @pl.when(has_onward)
            def _():
                far_copy(index).start()
        if index + 1 < near_chunks:
            mate_copy(near_view(index), near_pair_sems).start()
        if -1 <= index - lag < far_chunks:
            take_far(index - lag)
        lax.fori_loop(
            index * row_count // near_chunks, (index + 1) * row_count // near_chunks, own_stage, 0
        )
        if index % 3 == 1 and scans < rounds:
            scan_step()
    for index in range(max(near_chunks - lag, -1), far_chunks):
        take_far(index)
    while scans < rounds:
        scan_step()

    flags = jnp.where((scan_lane == 1) | (scan_lane == 2), state, 0)
    flags = jnp.max(jnp.max(flags, axis=1, keepdims=True), axis=0, keepdims=True)
    flag_ref[...] = jnp.broadcast_to((flags > 0).astype(jnp.int32), flag_ref.shape)
    flag_copy = pltpu.make_async_copy(flag_ref, flag_hbm, table_sems.at[0])
    flag_copy.start()
    reached = jnp.where(scan_lane == 0, state, 0)
    reached = jnp.max(jnp.max(reached, axis=1, keepdims=True), axis=0, keepdims=True)
    earlier = lax.broadcasted_iota(jnp.int32, small, 0) < lax.broadcasted_iota(jnp.int32, small, 1)
    counts = jnp.broadcast_to(own_counts, small)
    inner_sum = jnp.sum(jnp.where(earlier, counts, 0), axis=0, keepdims=True)
    offsets_ref[...] = inner_sum + (reached - total_count)

    wait_bytes(landed.at[pl.ds(0, near_slots - last_slots)], near_pair_sems.at[1])

    @pl.when(has_far)
    def _():
        wait_bytes(landed.at[pl.ds(0, far_slots)], far_pair_sems.at[1])

    ahead_of = [lax.rem(index // own_cap + pairs - group // 2, pairs) for index in range(half_cap)]

    def near_stage(c, carry):
        for index in range(half_cap):
            jobs = range(index * JOBS, (index + 1) * JOBS)
            left = jnp.concatenate([pair_r[codes[2 * row_count + c, x]] for x in jobs], axis=1)
            right = jnp.concatenate([landed[codes[row_count + c, x]] for x in jobs], axis=0)
            total = sums[c * half_cap + index] + jnp.dot(
                left, right, preferred_element_type=jnp.float32
            )
            place = ahead_of[index] * row_count * own_cap + c * own_cap + index % own_cap
            out_ref[place] = total.astype(out_ref.dtype)
        return carry

    lax.fori_loop(0, row_count, near_stage, 0, unroll=4)

    flag_copy.wait()
    wait_bytes(close.at[pl.ds(0, 2)], close_sems.at[0, 0])
    to_mate.wait_send()
    mate_a.wait_send()
    mate_r.wait_send()
    early_copy.wait_send()
    place_copy.wait_send()
    wait_bytes(packed, near_send.at[0])
    if groups > 2:
        wait_bytes(told.at[pl.ds(0, groups - 1)], told_sems.at[0])
    wait_bytes(landed.at[pl.ds(0, near_slots - last_slots)], near_pair_sems.at[0])

    @pl.when(has_onward)
    def _():
        wait_bytes(landed.at[pl.ds(0, far_slots)], far_send.at[0])

    @pl.when(has_far)
    def _():
        wait_bytes(close.at[pl.ds(2, 2)], close_sems.at[0, 1])
        wait_bytes(landed.at[pl.ds(0, far_slots)], far_pair_sems.at[0])

    for k in range(rounds):
        @pl.when(above_there[k])
        def _():
            scan_copy(k, 0).wait_send()

        @pl.when(below_there[k])
        def _():
            scan_copy(k, 1).wait_send()


def put_kernel(tiles_ref, offsets_ref, tiles_out, offsets_out, sems):
    copies = [
        pltpu.make_async_copy(tiles_ref, tiles_out, sems.at[0]),
        pltpu.make_async_copy(offsets_ref, offsets_out, sems.at[1]),
    ]
    for copy in copies:
        copy.start()
    for copy in copies:
        copy.wait()


def pair_sum_kernel(pairs, own, part_ref, landed, send_sems, recv_sems):
    row = lax.axis_index("rows")
    group = lax.axis_index("inner")
    core = lax.rem(group, 2)
    barrier = pltpu.get_barrier_semaphore()

    def place(ahead):
        return (row, 2 * lax.rem(group // 2 + ahead, pairs) + core)

    for ahead in range(1, pairs):
        pl.semaphore_signal(barrier, inc=1, device_id=place(ahead), device_id_type=MESH)
    pl.semaphore_wait(barrier, pairs - 1)
    copies = []
    for ahead in range(1, pairs):
        copy = pltpu.make_async_remote_copy(
            src_ref=part_ref.at[pl.ds(ahead * own, own)],
            dst_ref=landed.at[ahead - 1],
            send_sem=send_sems.at[ahead - 1],
            recv_sem=recv_sems.at[ahead - 1],
            device_id=place(ahead),
            device_id_type=MESH,
        )
        copy.start()
        copies.append(copy)
    for copy in copies:
        copy.wait()


def fused_body(rows, groups, r_tiles, r_cols, a_tiles, a_cols, c_cols, c_counts):
    local_rows, op_slots, tile, _ = a_tiles.shape
    row_count, r_slots = r_tiles.shape[:2]
    cap = c_cols.shape[1]
    tiles = local_rows * op_slots
    pairs = groups // 2
    own_cap = cap // groups
    half_cap = cap // 2
    width = -(-2 * tiles // 128) * 128
    chunks = []
    for size in [CHUNK] * (PASS_SLOTS // CHUNK) + list(LAST_CHUNKS):
        chunks.append((sum(before for _, before in chunks), size))
    list_slots = sum(size for _, size in chunks)
    pass_slots = PASS_SLOTS
    dims = (
        rows, groups, local_rows, op_slots, r_slots, cap, width, list_slots, pass_slots, tuple(chunks)
    )
    near_chunks = len(chunks)
    far_chunks = PASS_SLOTS // CHUNK
    early = min(EARLY, op_slots)
    near_slots = early + list_slots
    far_slots = early + pass_slots
    rounds = (rows - 1).bit_length()
    dtype = a_tiles.dtype
    out_dtype = jnp.bfloat16 if pairs == 1 else jnp.float32
    own = row_count * own_cap
    vmem = pl.BlockSpec(memory_space=pltpu.VMEM)
    anywhere = pl.BlockSpec(memory_space=pl.ANY)
    dma = pltpu.SemaphoreType.DMA
    block = (row_count, 128)
    part, offsets, flag = pl.pallas_call(
        functools.partial(fused_kernel, dims),
        out_shape=(
            jax.ShapeDtypeStruct((pairs * own, tile, tile), out_dtype),
            jax.ShapeDtypeStruct((1, row_count), jnp.int32),
            jax.ShapeDtypeStruct((1, 128), jnp.int32),
        ),
        in_specs=[anywhere] * 6,
        out_specs=(vmem, vmem, anywhere),
        scratch_shapes=[
            pltpu.VMEM((1, 128), jnp.int32),
            pltpu.VMEM(r_cols.shape, jnp.int32),
            pltpu.VMEM(c_cols.shape, jnp.int32),
            pltpu.VMEM((1, row_count), jnp.int32),
            pltpu.VMEM((op_slots, a_cols.shape[0]), jnp.int32),
            pltpu.VMEM(block, jnp.int32),
            pltpu.VMEM((5,) + block, jnp.int32),
            pltpu.VMEM((2, 8, width), jnp.int32),
            pltpu.VMEM((2 * tiles + 1, tile, tile), dtype),
            pltpu.VMEM((2 * row_count * r_slots, tile, tile), dtype),
            pltpu.VMEM((list_slots, tile, tile), dtype),
            pltpu.VMEM((2 * (near_slots + far_slots) + 1, tile, tile), dtype),
            pltpu.VMEM((row_count * half_cap, tile, tile), jnp.float32),
            pltpu.VMEM((3 * row_count, width), jnp.int32),
            pltpu.SMEM((3 * row_count, width), jnp.int32),
            pltpu.SMEM((8, width), jnp.int32),
            pltpu.VMEM((groups, 8, 128), jnp.int32),
            pltpu.VMEM((rounds, 8, 128), jnp.int32),
            pltpu.VMEM((rounds, 2, 8, 128), jnp.int32),
            dma((6,)),
            dma((2, 3)),
            dma((2, 2)),
            dma((2,)),
            dma((2,)),
            dma((near_chunks,)),
            dma((1,)),
            dma((2,)),
            dma((far_chunks + 1,)),
            dma((1,)),
            dma((2,)),
            dma((2,)),
            dma((2,)),
            dma((2, rounds, 2)),
        ],
        compiler_params=pltpu.CompilerParams(collective_id=40, has_side_effects=True),
        name="fused",
    )(
        r_cols,
        c_cols,
        c_counts[None, :],
        a_cols.T,
        a_tiles.reshape(tiles, tile, tile),
        r_tiles.reshape(row_count * r_slots, tile, tile),
    )
    if pairs == 1:
        c_tiles = part
    else:
        landed = pl.pallas_call(
            functools.partial(pair_sum_kernel, pairs, own),
            out_shape=jax.ShapeDtypeStruct((pairs - 1, own, tile, tile), jnp.float32),
            in_specs=[anywhere],
            out_specs=anywhere,
            scratch_shapes=[dma((pairs - 1,)), dma((pairs - 1,))],
            compiler_params=pltpu.CompilerParams(collective_id=41, has_side_effects=True),
            name="pair_sums",
        )(part)
        c_tiles = part[:own]
        for ahead in range(pairs - 1):
            c_tiles = c_tiles + landed[ahead]
        c_tiles = c_tiles.astype(jnp.bfloat16)
    return c_tiles.reshape(row_count, own_cap, tile, tile), offsets[0], flag[0, 0]


def body(rows, groups, *args):
    if rows % 2 or groups % 2:
        return plain_body(rows, groups, *args)
    c_tiles, offsets, flag = fused_body(rows, groups, *args)

    def again(c_tiles, offsets, *args):
        return plain_body(rows, groups, *args)

    def keep(c_tiles, offsets, *args):
        return c_tiles, offsets

    c_tiles, offsets = lax.cond(flag > 0, again, keep, c_tiles, offsets, *args)
    vmem = pl.BlockSpec(memory_space=pltpu.VMEM)
    anywhere = pl.BlockSpec(memory_space=pl.ANY)
    c_tiles, offsets = pl.pallas_call(
        put_kernel,
        out_shape=(
            jax.ShapeDtypeStruct(c_tiles.shape, c_tiles.dtype),
            jax.ShapeDtypeStruct((1,) + offsets.shape, offsets.dtype),
        ),
        in_specs=[vmem, vmem],
        out_specs=(anywhere, anywhere),
        scratch_shapes=[pltpu.SemaphoreType.DMA((2,))],
        name="put",
    )(c_tiles, offsets[None, :])
    return c_tiles, offsets[0]


def solution(mesh):
    rows = mesh.shape["rows"]
    groups = mesh.shape["inner"]
    return jax.shard_map(
        functools.partial(body, rows, groups),
        mesh=mesh,
        in_specs=(
            P("rows", "inner", None, None),
            P("rows", "inner"),
            P(("rows", "inner"), None, None, None),
            P(),
            P("rows", None),
            P("rows"),
        ),
        out_specs=(P("rows", "inner", None, None), P("rows")),
        check_vma=False,
    )
```

```python
import functools

import jax
import jax.numpy as jnp
from jax import lax
from jax.experimental import pallas as pl
from jax.experimental.pallas import tpu as pltpu
from jax.sharding import PartitionSpec as P

MESH = pl.DeviceIdType.MESH
BATCH = 4


def plan_kernel(
    dims, r_cols_ref, c_cols_ref, counts_ref, columns_ref, code_ref, plan_ref,
    meta_ref, gathered, needs, send_sem, recv_sem,
):
    rows, groups, local_rows, op_slots, r_slots, cap, half = dims
    width = 2 * half
    count = rows * groups
    tiles = local_rows * op_slots
    row = lax.axis_index("rows")
    group = lax.axis_index("inner")
    me = row * groups + group

    barrier = pltpu.get_barrier_semaphore()

    def place(step):
        other = lax.rem(me + step, count)
        return (other // groups, lax.rem(other, groups))

    def greet(step, carry):
        pl.semaphore_signal(barrier, inc=1, device_id=place(step), device_id_type=MESH)
        return carry

    lax.fori_loop(1, count, greet, 0)
    row_count = r_cols_ref.shape[0]
    live = r_slots + cap
    lanes = lax.broadcasted_iota(jnp.int32, (row_count, width), 1)
    above = lax.broadcasted_iota(jnp.int32, (row_count, width), 0)
    small = (row_count, row_count)
    diagonal = lax.broadcasted_iota(jnp.int32, small, 0) == lax.broadcasted_iota(jnp.int32, small, 1)
    spread_counts = jnp.broadcast_to(counts_ref[...], small)
    own_counts = jnp.sum(jnp.where(diagonal, spread_counts, 0), axis=1, keepdims=True)
    meta_ref[...] = jnp.full(meta_ref.shape, -9, jnp.int32)
    meta_ref[:, 0:r_slots] = r_cols_ref[...]
    meta_ref[:, r_slots:live] = c_cols_ref[...]
    meta_ref[:, live : live + 1] = own_counts
    gathered[me] = meta_ref[...]
    pl.semaphore_wait(barrier, count - 1)

    def post(step, carry):
        pltpu.make_async_remote_copy(
            src_ref=meta_ref,
            dst_ref=gathered.at[me],
            send_sem=send_sem,
            recv_sem=recv_sem,
            device_id=place(step),
            device_id_type=MESH,
        ).start()
        return carry

    lax.fori_loop(1, count, post, 0)
    everyone = gathered.at[pl.ds(0, count - 1)]
    pltpu.make_async_copy(everyone, everyone, send_sem).wait()
    pltpu.make_async_copy(everyone, everyone, recv_sem).wait()

    def matches(block, columns, fine_rows):
        named = fine_rows == block[:, 0:1]
        for j in range(1, r_slots):
            named = named | (fine_rows == block[:, j : j + 1])
        slot = jnp.full((row_count, width), -1, jnp.int32)
        for s in range(cap):
            slot = jnp.where(columns == block[:, r_slots + s : r_slots + s + 1], s, slot)
        return jnp.where(named, slot, -1)

    shift = jnp.where(lanes < half, -groups, groups) * local_rows
    tile = jnp.where(lanes < half, lanes, lanes - half)
    lane_rows = jnp.where(tile < tiles, shift + tile // op_slots, -(1 << 24))
    low_lanes = lanes[0:1] < half

    def near_matches(device):
        before = columns_ref[pl.ds(jnp.maximum(device - groups, 0), 1), :]
        after = columns_ref[pl.ds(jnp.minimum(device + groups, count - 1), 1), :]
        columns = jnp.where(low_lanes, before, after)
        return matches(gathered[device], columns, lane_rows + device * local_rows)

    def wanted(found):
        return jnp.max((found >= 0).astype(jnp.int32), axis=0, keepdims=True)

    def gather_needs(device, carry):
        needs[pl.ds(device, 1), :] = wanted(near_matches(device))
        return carry

    lax.fori_loop(0, count, gather_needs, 0, unroll=4)
    every = needs[...]
    low_side = lax.broadcasted_iota(jnp.int32, every.shape, 1) < half
    low = jnp.sum(jnp.where(low_side, every, 0), axis=1, keepdims=True)
    high = jnp.sum(jnp.where(low_side, 0, every), axis=1, keepdims=True)
    most = jnp.max(jnp.maximum(low, high), axis=0, keepdims=True)

    down = lax.broadcasted_iota(jnp.int32, (width, width), 0)
    across = lax.broadcasted_iota(jnp.int32, (width, width), 1)
    same = (down < half) == (across < half)

    def ranks(need):
        spread = jnp.broadcast_to(need, (width, width))
        column = jnp.sum(jnp.where(down == across, spread, 0), axis=1, keepdims=True)
        before = jnp.sum(jnp.where((across < down) & same, spread, 0), axis=1, keepdims=True)
        along = jnp.sum(
            jnp.where((down < across) & same, jnp.broadcast_to(column, (width, width)), 0),
            axis=0,
            keepdims=True,
        )
        return column, before, along

    def send_list(device, high):
        column, before, _ = ranks(needs[pl.ds(device, 1), :])
        first = half if high else 0
        mine = (down >= half) if high else (down < half)
        chosen = mine & (column > 0) & (before == across)
        return jnp.sum(jnp.where(chosen, down - first, 0), axis=0, keepdims=True)

    left = jnp.maximum(row - 1, 0) * groups + group
    right = jnp.minimum(row + 1, rows - 1) * groups + group
    plan_ref[0:1, :] = send_list(left, True)
    plan_ref[1:2, :] = send_list(right, False)

    found = near_matches(me)
    _, _, along = ranks(wanted(found))
    slot_at = along + jnp.where(lanes[0:1] < half, tiles, 2 * tiles)
    code_ref[:, 0:width] = jnp.where(found >= 0, found + cap * slot_at, -1)
    fine = me * local_rows + jnp.where(lanes < tiles, lanes // op_slots, 0)
    fine = jnp.where(lanes < tiles, fine, -5)
    found = matches(gathered[me], columns_ref[pl.ds(me, 1), :], fine)
    code_ref[:, width:] = jnp.where(found >= 0, found + cap * lanes, -1)

    def earlier(index, total):
        block = gathered[index * groups]
        return total + jnp.sum(block[:, live : live + 1], axis=0, keepdims=True)

    first = lax.fori_loop(0, row, earlier, jnp.zeros((1, 1), jnp.int32))
    counts = jnp.broadcast_to(own_counts, (row_count, width))
    inner_sum = jnp.sum(jnp.where(above < lanes, counts, 0), axis=0, keepdims=True)
    plan_ref[2:3, :] = inner_sum + first
    level = jnp.zeros((1, 1), jnp.int32)
    for size in sizes_for(tiles)[:-1]:
        level = level + (most > size).astype(jnp.int32)
    plan_ref[3:4, :] = jnp.broadcast_to(level, (1, width))


def halo_kernel(rows, size, plan_ref, a_ref, out_ref, packed, send_sems, recv_sems):
    row = lax.axis_index("rows")
    group = lax.axis_index("inner")
    barrier = pltpu.get_barrier_semaphore()
    has_left = row > 0
    has_right = row < rows - 1

    @pl.when(has_left)
    def _():
        pl.semaphore_signal(barrier, inc=1, device_id=(row - 1, group), device_id_type=MESH)

    @pl.when(has_right)
    def _():
        pl.semaphore_signal(barrier, inc=1, device_id=(row + 1, group), device_id_type=MESH)

    def pack(index, carry):
        packed[0, index] = a_ref[plan_ref[0, index]]
        packed[1, index] = a_ref[plan_ref[1, index]]
        return carry

    lax.fori_loop(0, size, pack, 0, unroll=2)

    pl.semaphore_wait(barrier, has_left.astype(jnp.int32) + has_right.astype(jnp.int32))

    def copy(side, other):
        return pltpu.make_async_remote_copy(
            src_ref=packed.at[side],
            dst_ref=out_ref.at[1 - side, pl.ds(0, size)],
            send_sem=send_sems.at[side],
            recv_sem=recv_sems.at[1 - side],
            device_id=(other, group),
            device_id_type=MESH,
        )

    @pl.when(has_left)
    def _():
        copy(0, row - 1).start()

    @pl.when(has_right)
    def _():
        copy(1, row + 1).start()

    @pl.when(has_left)
    def _():
        copy(0, row - 1).wait_send()
        copy(1, row - 1).wait_recv()

    @pl.when(has_right)
    def _():
        copy(1, row + 1).wait_send()
        copy(0, row + 1).wait_recv()


def product_kernel(dims, code_ref, cols_ref, r_ref, a_ref, halo_ref, out_ref, tiles_ref, jobs, sems):
    rows, groups, local_rows, op_slots, r_slots, cap, half = dims
    width = 2 * half
    tiles = local_rows * op_slots
    row_count = cols_ref.shape[0]
    own_cap = cap // groups
    row = lax.axis_index("rows")
    group = lax.axis_index("inner")
    own = pltpu.make_async_copy(a_ref, tiles_ref.at[pl.ds(0, tiles)], sems.at[0])
    near = pltpu.make_async_copy(halo_ref, tiles_ref.at[pl.ds(tiles, 2 * tiles)], sems.at[1])
    own.start()
    near.start()
    last = groups * row_count * own_cap
    scale = 1 << (3 * tiles * cap - 1).bit_length()

    def clear(index, carry):
        out_ref[index] = jnp.zeros(out_ref.shape[1:], jnp.float32)
        return carry

    lax.fori_loop(0, last, clear, 0, unroll=4)

    def list_row(c, found):
        def list_slot(j, found):
            fine = cols_ref[c, j]
            side = fine // (local_rows * groups) - row
            base = jnp.where(side == 0, width, jnp.where(side < 0, 0, half))
            base = base + lax.rem(fine, local_rows) * op_slots
            for t in range(op_slots):
                code = code_ref[c, base + t]
                jobs[found] = (c * r_slots + j) * scale + code
                found = found + (code >= 0).astype(jnp.int32)
            return found

        return lax.fori_loop(0, r_slots, list_slot, found)

    found = lax.fori_loop(0, row_count, list_row, jnp.int32(0))
    for extra in range(BATCH):
        jobs[found + extra] = -1
    own.wait()
    near.wait()

    def batch(step, carry):
        results = []
        targets = []
        for extra in range(BATCH):
            job = jobs[step * BATCH + extra]
            valid = job >= 0
            job = jnp.maximum(job, 0)
            pair = job // scale
            code = lax.rem(job, scale)
            slot = lax.rem(code, cap)
            ahead = lax.rem(slot // own_cap + groups - group, groups)
            target = (ahead * row_count + pair // r_slots) * own_cap + lax.rem(slot, own_cap)
            targets.append(jnp.where(valid, target, last))
            results.append(
                jnp.dot(
                    r_ref[pair],
                    tiles_ref[code // cap],
                    preferred_element_type=jnp.float32,
                )
            )
        for extra in range(BATCH):
            target = targets[extra]
            out_ref[target] = out_ref[target] + results[extra]
        return carry

    lax.fori_loop(0, (found + BATCH - 1) // BATCH, batch, 0)


def sum_kernel(groups, own, part_ref, landed, send_sems, recv_sems):
    row = lax.axis_index("rows")
    group = lax.axis_index("inner")
    barrier = pltpu.get_barrier_semaphore()
    for ahead in range(1, groups):
        pl.semaphore_signal(
            barrier, inc=1, device_id=(row, lax.rem(group + ahead, groups)), device_id_type=MESH
        )
    pl.semaphore_wait(barrier, groups - 1)
    copies = []
    for ahead in range(1, groups):
        copy = pltpu.make_async_remote_copy(
            src_ref=part_ref.at[pl.ds(ahead * own, own)],
            dst_ref=landed.at[ahead - 1],
            send_sem=send_sems.at[ahead - 1],
            recv_sem=recv_sems.at[ahead - 1],
            device_id=(row, lax.rem(group + ahead, groups)),
            device_id_type=MESH,
        )
        copy.start()
        copies.append(copy)
    for copy in copies:
        copy.wait()


def sizes_for(tiles):
    steps = [16, 18, 20, 21, 22, 23, 24, 25, 26, 27, 28, 29, 30, 32, 36, 42]
    return [size for size in steps if size < tiles] + [tiles]


def plain_body(rows, groups, r_tiles, r_cols, a_tiles, a_cols, c_cols, c_counts):
    local_rows, op_slots, tile, _ = a_tiles.shape
    row_count, r_slots = r_tiles.shape[:2]
    cap = c_cols.shape[1]
    tiles = local_rows * op_slots
    half = -(-tiles // 64) * 64
    width = 2 * half
    count = rows * groups
    own_cap = cap // groups
    dims = (rows, groups, local_rows, op_slots, r_slots, cap, half)
    vmem = pl.BlockSpec(memory_space=pltpu.VMEM)
    smem = pl.BlockSpec(memory_space=pltpu.SMEM)
    anywhere = pl.BlockSpec(memory_space=pl.ANY)

    flat = a_cols.reshape(count, tiles)
    flat = jnp.pad(flat, ((0, 0), (0, half - tiles)), constant_values=-2)
    columns = jnp.concatenate([flat, flat], axis=1)

    code, plan = pl.pallas_call(
        functools.partial(plan_kernel, dims),
        out_shape=(
            jax.ShapeDtypeStruct((row_count, 2 * width), jnp.int32),
            jax.ShapeDtypeStruct((8, width), jnp.int32),
        ),
        in_specs=[vmem] * 4,
        out_specs=(vmem, vmem),
        scratch_shapes=[
            pltpu.VMEM((row_count, width), jnp.int32),
            pltpu.VMEM((count, row_count, width), jnp.int32),
            pltpu.VMEM((count, width), jnp.int32),
            pltpu.SemaphoreType.DMA,
            pltpu.SemaphoreType.DMA,
        ],
        compiler_params=pltpu.CompilerParams(collective_id=0, has_side_effects=True),
        name="plan",
    )(r_cols, c_cols, c_counts[None, :], columns)

    flat_a = a_tiles.reshape(tiles, tile, tile)
    sizes = sizes_for(tiles)

    def exchange(number, size, plan, flat_a):
        return pl.pallas_call(
            functools.partial(halo_kernel, rows, size),
            out_shape=jax.ShapeDtypeStruct((2, tiles, tile, tile), a_tiles.dtype),
            in_specs=[smem, vmem],
            out_specs=anywhere,
            scratch_shapes=[
                pltpu.VMEM((2, size, tile, tile), a_tiles.dtype),
                pltpu.SemaphoreType.DMA((2,)),
                pltpu.SemaphoreType.DMA((2,)),
            ],
            compiler_params=pltpu.CompilerParams(collective_id=number + 2, has_side_effects=True),
            name=f"halo{size}",
        )(plan, flat_a)

    halo = lax.switch(
        plan[3, 0],
        [functools.partial(exchange, number, size) for number, size in enumerate(sizes)],
        plan,
        flat_a,
    )

    slots = row_count * r_slots * op_slots + BATCH
    partial_value = pl.pallas_call(
        functools.partial(product_kernel, dims),
        out_shape=jax.ShapeDtypeStruct((row_count * cap + 1, tile, tile), jnp.float32),
        in_specs=[smem, smem, vmem, anywhere, anywhere],
        out_specs=vmem,
        scratch_shapes=[
            pltpu.VMEM((3 * tiles, tile, tile), a_tiles.dtype),
            pltpu.SMEM((slots,), jnp.int32),
            pltpu.SemaphoreType.DMA((2,)),
        ],
        name="products",
    )(
        code,
        r_cols,
        r_tiles.reshape(row_count * r_slots, tile, tile),
        flat_a,
        halo.reshape(2 * tiles, tile, tile),
    )

    own_count = row_count * own_cap
    landed = pl.pallas_call(
        functools.partial(sum_kernel, groups, own_count),
        out_shape=jax.ShapeDtypeStruct((groups - 1, own_count, tile, tile), jnp.float32),
        in_specs=[anywhere],
        out_specs=anywhere,
        scratch_shapes=[
            pltpu.SemaphoreType.DMA((groups - 1,)),
            pltpu.SemaphoreType.DMA((groups - 1,)),
        ],
        compiler_params=pltpu.CompilerParams(collective_id=1, has_side_effects=True),
        name="sums",
    )(partial_value)
    c_tiles = partial_value[:own_count]
    for ahead in range(groups - 1):
        c_tiles = c_tiles + landed[ahead]
    c_tiles = c_tiles.astype(jnp.bfloat16)
    return (c_tiles.reshape(row_count, own_cap, tile, tile), plan[2, :row_count])

EARLY = 7
PASS_SLOTS = 15
CHUNK = 3
LAST_CHUNKS = (3, 3, 3, 2)
JOBS = 4
REMOTE = 1 << 14


def fused_kernel(
    dims, r_cols_hbm, c_cols_hbm, counts_hbm, columns_hbm, a_ref, r_ref,
    out_ref, offsets_ref, flag_hbm,
    flag_ref, r_cols_ref, c_cols_ref, counts_ref, columns_ref,
    meta, close, placing, pair_a, pair_r, packed, landed, sums, tables, codes, picks,
    told, scan_out, scan_in,
    local_sems, close_sems, pair_sems, place_sems, early_sems, near_sems, near_send,
    near_pair_sems, far_sems, far_send, far_pair_sems, table_sems, told_sems, scan_sems,
):
    (rows, groups, local_rows, op_slots, r_slots, cap, width, list_slots, pass_slots, chunks) = dims
    pairs = groups // 2
    tiles = local_rows * op_slots
    span = 2 * local_rows
    own_cap = cap // groups
    half_cap = cap // 2
    both = 2 * r_slots
    row_count = r_cols_ref.shape[0]
    live = r_slots + cap
    early = min(EARLY, op_slots)
    near_slots = early + list_slots
    far_slots = early + pass_slots
    near_chunks = len(chunks)
    far_chunks = sum(start < pass_slots for start, _ in chunks)
    last_slots = chunks[-1][1]
    far_base = 2 * near_slots
    zero_near = 2 * (near_slots + far_slots)
    zero_own = 2 * tiles
    rounds = (rows - 1).bit_length()

    row = lax.axis_index("rows")
    group = lax.axis_index("inner")
    part = lax.rem(group, 2)
    first_group = group - part
    mate = first_group + 1 - part
    odd = lax.rem(row, 2)
    near = row + 1 - 2 * odd
    far = row - 1 + 2 * odd
    has_far = (far >= 0) & (far < rows)
    onward = near + 1 - 2 * odd
    has_onward = (onward >= 0) & (onward < rows)
    mate_place = (row, mate)

    barrier = pltpu.get_barrier_semaphore()

    def greet(place):
        pl.semaphore_signal(barrier, inc=1, device_id=place, device_id_type=MESH)

    for core in range(2):
        greet((near, first_group + core))

    @pl.when(has_far)
    def _():
        for core in range(2):
            greet((far, first_group + core))

    for ahead in range(1, groups):
        greet((row, lax.rem(group + ahead, groups)))

    small_copies = [
        pltpu.make_async_copy(src, dst, local_sems.at[2 + index])
        for index, (src, dst) in enumerate(
            [
                (r_cols_hbm, r_cols_ref),
                (c_cols_hbm, c_cols_ref),
                (counts_hbm, counts_ref),
                (columns_hbm, columns_ref),
            ]
        )
    ]
    for copy in small_copies:
        copy.start()
    own_a = pltpu.make_async_copy(
        a_ref, pair_a.at[pl.ds(part * tiles, tiles)], local_sems.at[0]
    )
    own_r = pltpu.make_async_copy(r_ref, pair_r.at[pl.ds(part * row_count * r_slots, row_count * r_slots)], local_sems.at[1])
    own_a.start()
    own_r.start()

    def remote(src, dst, send_sem, recv_sem, place):
        return pltpu.make_async_remote_copy(
            src_ref=src, dst_ref=dst, send_sem=send_sem, recv_sem=recv_sem,
            device_id=place, device_id_type=MESH,
        )

    def wait_bytes(view, sem):
        pltpu.make_async_copy(view, view, sem).wait()

    small = (row_count, row_count)
    diagonal = lax.broadcasted_iota(jnp.int32, small, 0) == lax.broadcasted_iota(jnp.int32, small, 1)
    meta[...] = jnp.full(meta.shape, -9, jnp.int32)
    pair_a[zero_own] = jnp.zeros(pair_a.shape[1:], pair_a.dtype)
    landed[zero_near] = jnp.zeros(landed.shape[1:], landed.dtype)
    for copy in small_copies:
        copy.wait()
    spread_counts = jnp.broadcast_to(counts_ref[...], small)
    own_counts = jnp.sum(jnp.where(diagonal, spread_counts, 0), axis=1, keepdims=True)
    meta[:, 0:r_slots] = r_cols_ref[...]
    meta[:, r_slots:live] = c_cols_ref[...]
    pl.semaphore_wait(barrier, groups + 1 + 2 * has_far.astype(jnp.int32))

    def start_close(target, first, which):
        for core in range(2):
            remote(
                meta, close.at[first + part], close_sems.at[0, which], close_sems.at[1, which],
                (target, first_group + core),
            ).start()

    @pl.when(has_far)
    def _():
        start_close(far, 2, 1)

    start_close(near, 0, 0)
    to_mate = remote(meta, close.at[4], close_sems.at[0, 2], close_sems.at[1, 2], mate_place)
    to_mate.start()
    mate_a = remote(
        a_ref, pair_a.at[pl.ds(part * tiles, tiles)], pair_sems.at[0, 0], pair_sems.at[1, 0], mate_place
    )
    mate_a.start()

    own_a.wait()
    early_copy = remote(
        pair_a.at[pl.ds(part * tiles, early)], landed.at[pl.ds(part * near_slots, early)],
        early_sems.at[0], early_sems.at[1], (near, group),
    )
    early_copy.start()
    mate_r = remote(r_ref, pair_r.at[pl.ds(part * row_count * r_slots, row_count * r_slots)], pair_sems.at[0, 1], pair_sems.at[1, 1], mate_place)
    mate_r.start()

    lanes = lax.broadcasted_iota(jnp.int32, (1, width), 1)
    real = lanes < op_slots * span
    lane_slot = lanes // span
    lane_fine = jnp.where(real, lax.rem(lanes, span), -(1 << 24))
    lane_core = lax.rem(lanes, span) // local_rows
    lane_local = lax.rem(lanes, local_rows)
    lane_tile = lane_core * tiles + lane_local * op_slots + lane_slot
    late = jnp.where((lane_local > 0) | (lane_slot >= early), 1, 0)

    def pair_columns(which_row):
        start = (which_row * groups + first_group) * local_rows
        block = start // 128
        values = columns_ref[:, pl.ds(pl.multiple_of(block * 128, 128), 128)]
        if width > 128:
            values = jnp.concatenate([values] * (width // 128), axis=1)
        offset = start - block * 128
        total = jnp.zeros((1, width), jnp.int32)
        for t in range(op_slots):
            moved = pltpu.roll(values[t : t + 1, :], lax.rem(t * span - offset + 128 * width, width), 1)
            total = jnp.where(lane_slot == t, moved, total)
        return jnp.where(real, total, -2)

    def pair_fine(which_row):
        return lane_fine + (which_row * groups + first_group) * local_rows

    def named_by(meta_low, meta_high, fine):
        named = fine == meta_low[:, 0:1]
        for j in range(1, r_slots):
            named = named | (fine == meta_low[:, j : j + 1])
        for j in range(r_slots):
            named = named | (fine == meta_high[:, j : j + 1])
        return named

    def need_by_core(meta_low, meta_high, columns, fine):
        named = named_by(meta_low, meta_high, fine)
        needs = []
        for core in range(2):
            wanted = jnp.zeros(named.shape, jnp.bool_)
            for s in range(cap):
                if s // own_cap % 2 == core:
                    wanted = wanted | (columns == meta_low[:, r_slots + s : r_slots + s + 1])
            needs.append(jnp.max((named & wanted).astype(jnp.int32), axis=0, keepdims=True))
        return needs

    def need_of(meta_low, meta_high, columns, fine):
        low, high = need_by_core(meta_low, meta_high, columns, fine)
        return jnp.maximum(low, high)

    def before(need):
        total = need
        step = 1
        while step < width:
            total = total + jnp.where(lanes >= step, pltpu.roll(total, step, 1), 0)
            step *= 2
        return total - need

    def landing(places, count, base, slots):
        fits = (places >= 0) & (places < 2 * count)
        at = lax.rem(places, 2) * slots + early + places // 2
        at = jnp.where(late > 0, jnp.where(fits, at, -1), lane_core * slots + lane_slot)
        return jnp.where(real & (at >= 0), REMOTE + base + at, -1)

    own_columns = pair_columns(row)
    own_fine = pair_fine(row)

    near_columns = pair_columns(near)
    near_fine = pair_fine(near)
    far_row = jnp.clip(far, 0, rows - 1)
    far_columns = pair_columns(far_row)
    far_fine = jnp.where(has_far, pair_fine(far_row), -(1 << 24))
    to_mate.wait_recv()
    mine, other = meta[...], close[4]
    my_low = jnp.where(part == 0, mine, other)
    my_high = jnp.where(part == 0, other, mine)
    near_named = named_by(my_low, my_high, near_fine)
    far_named = named_by(my_low, my_high, far_fine)
    crowded = jnp.zeros((1, 1), jnp.int32)
    for s in range(cap):
        column = my_low[:, r_slots + s : r_slots + s + 1]
        hits = (near_named & (near_columns == column)).astype(jnp.int32)
        hits = hits + (far_named & (far_columns == column)).astype(jnp.int32)
        held = jnp.sum(hits, axis=1, keepdims=True)
        crowded = jnp.maximum(crowded, jnp.max(held, axis=0, keepdims=True))

    wait_bytes(close.at[pl.ds(0, 2)], close_sems.at[1, 0])
    near_low, near_high = [
        need * late for need in need_by_core(close[0], close[1], own_columns, own_fine)
    ]

    @pl.when(has_far)
    def _():
        wait_bytes(close.at[pl.ds(2, 2)], close_sems.at[1, 1])

    @pl.when(jnp.logical_not(has_far))
    def _():
        close[2] = jnp.full(close.shape[1:], -9, jnp.int32)
        close[3] = jnp.full(close.shape[1:], -9, jnp.int32)

    need_far = need_of(close[2], close[3], own_columns, own_fine) * late
    need_only = jnp.maximum(near_low, near_high) * (1 - need_far)
    lone_low = need_only * (1 - near_high)
    lone_high = need_only * (1 - near_low)
    lists = jnp.concatenate([need_far, need_only, lone_low, lone_high], axis=0)
    ahead_in = before(lists)
    totals = jnp.sum(lists, axis=1, keepdims=True)
    far_before, only_before, low_before, high_before = [ahead_in[x : x + 1] for x in range(4)]
    far_total, only_total, low_total, high_total = [totals[x : x + 1] for x in range(4)]
    last_low = (lone_low > 0) & (low_before < last_slots)
    last_high = (lone_high > 0) & (high_before < last_slots)
    need_rest = jnp.where(last_low | last_high, 0, need_only)
    near_total = far_total + only_total
    near_total = near_total - jnp.minimum(low_total, last_slots) - jnp.minimum(high_total, last_slots)
    rest_before = only_before - jnp.minimum(low_before, last_slots)
    rest_before = rest_before - jnp.minimum(high_before, last_slots)
    places = jnp.where(
        need_far > 0, far_before, jnp.where(need_rest > 0, rest_before + far_total, -1)
    )
    last_first = list_slots - last_slots
    places = jnp.where(places < 2 * last_first, places, -1)
    places = jnp.where(last_low, 2 * (last_first + low_before), places)
    places = jnp.where(last_high, 2 * (last_first + high_before) + 1, places)
    pick_rows = -(-list_slots // 8) * 8
    slot_down = lax.broadcasted_iota(jnp.int32, (pick_rows, width), 0)
    chosen = jnp.broadcast_to(places, (pick_rows, width)) == 2 * slot_down + part
    picked = jnp.sum(
        jnp.where(chosen, jnp.broadcast_to(lane_tile, (pick_rows, width)), 0), axis=1, keepdims=True
    )
    across = lax.broadcasted_iota(jnp.int32, (pick_rows, width), 1)
    pick_row = jnp.sum(
        jnp.where(slot_down == across, jnp.broadcast_to(picked, (pick_rows, width)), 0),
        axis=0, keepdims=True,
    )
    tables[0:8, :] = jnp.broadcast_to(pick_row, (8, width))
    pick_copy = pltpu.make_async_copy(tables.at[pl.ds(0, 8)], picks, table_sems.at[0])
    pick_copy.start()
    placing[0] = jnp.broadcast_to(landing(places, list_slots, 0, near_slots), placing.shape[1:])
    place_copy = remote(placing.at[0], placing.at[1], place_sems.at[0], place_sems.at[1], (near, group))
    place_copy.start()
    over = jnp.maximum(near_total - 2 * (list_slots - last_slots), far_total - 2 * pass_slots)
    over = jnp.maximum(over, crowded - JOBS)
    over = (over > 0).astype(jnp.int32)
    if groups > 2:
        told[group] = jnp.broadcast_to(over, told.shape[1:])

        def tell(ahead):
            return remote(
                told.at[group], told.at[group], told_sems.at[0], told_sems.at[1],
                (row, lax.rem(group + ahead, groups)),
            )

        for ahead in range(1, groups):
            tell(ahead).start()
        wait_bytes(told.at[pl.ds(0, groups - 1)], told_sems.at[1])
        over = told[0]
        for other_group in range(1, groups):
            over = over + told[other_group]

    tile = pair_a.shape[1]
    total_count = jnp.sum(own_counts, axis=0, keepdims=True)

    def scan_copy(k, side):
        other = row + (1 << k) if side == 0 else row - (1 << k)
        return remote(
            scan_out.at[k], scan_in.at[k, side], scan_sems.at[0, k, side], scan_sems.at[1, k, side],
            (other, group),
        )

    scan_shape = scan_out.shape[1:]
    scan_lane = lax.broadcasted_iota(jnp.int32, scan_shape, 1)
    above_there = [row + (1 << k) < rows for k in range(rounds)]
    below_there = [row - (1 << k) >= 0 for k in range(rounds)]

    def scan_send(k, state):
        scan_out[k] = state

        @pl.when(above_there[k])
        def _():
            scan_copy(k, 0).start()

        @pl.when(below_there[k])
        def _():
            scan_copy(k, 1).start()

    def scan_take(k, state):
        @pl.when(below_there[k])
        def _():
            scan_copy(k, 0).wait_recv()

        @pl.when(above_there[k])
        def _():
            scan_copy(k, 1).wait_recv()

        below = jnp.where((scan_lane < 2) & below_there[k], scan_in[k, 0], 0)
        beyond = jnp.where((scan_lane == 2) & above_there[k], scan_in[k, 1], 0)
        return state + below + beyond

    state = jnp.where(
        scan_lane == 0, jnp.broadcast_to(total_count, scan_shape),
        jnp.where(scan_lane < 3, over, 0),
    )
    scan_send(0, state)
    scans = 0

    def scan_step():
        nonlocal state, scans
        state = scan_take(scans, state)
        scans += 1
        if scans < rounds:
            scan_send(scans, state)

    mate_a.wait_recv()
    pick_copy.wait()

    def near_view(index):
        start, size = chunks[index]
        return landed.at[pl.ds(part * near_slots + early + start, size)]

    def near_copy(index):
        return remote(
            packed.at[pl.ds(*chunks[index])], near_view(index),
            near_send.at[0], near_sems.at[index], (near, group),
        )

    def pack(index):
        start, size = chunks[index]
        for slot in range(start, start + size):
            packed[slot] = pair_a[picks[0, slot]]

    pack(0)
    for index in range(near_chunks):
        if index + 1 < near_chunks:
            pack(index + 1)
        near_copy(index).start()

    def mate_copy(view, sems):
        return remote(view, view, sems.at[0], sems.at[1], mate_place)

    early_view = landed.at[pl.ds(part * near_slots, early)]
    early_far_view = landed.at[pl.ds(far_base + part * far_slots, early)]

    def far_view(index):
        start, size = chunks[index]
        return landed.at[pl.ds(far_base + part * far_slots + early + start, size)]

    early_far = remote(early_view, early_far_view, far_send.at[0], far_sems.at[far_chunks], (onward, group))

    def far_copy(index):
        return remote(
            near_view(index), far_view(index), far_send.at[0], far_sems.at[index], (onward, group)
        )

    def take_far(index):
        @pl.when(has_far)
        def _():
            if index < 0:
                early_far.wait_recv()
                mate_copy(early_far_view, far_pair_sems).start()
            else:
                far_copy(index).wait_recv()
                mate_copy(far_view(index), far_pair_sems).start()

    early_copy.wait_recv()

    @pl.when(has_onward)
    def _():
        early_far.start()

    mate_copy(early_view, near_pair_sems).start()
    if scans < rounds:
        scan_step()
    far_need = need_of(my_low, my_high, far_columns, far_fine) * late
    far_places = jnp.where(far_need > 0, before(far_need), -1)
    far_at = landing(far_places, pass_slots, far_base, far_slots)
    place_copy.wait_recv()
    near_at = placing[1][0:1, :]

    above = (row_count, width)
    table_lanes = lax.broadcasted_iota(jnp.int32, above, 1)
    own_at, near_at, far_at = [jnp.broadcast_to(x, above) for x in (lane_tile, near_at, far_at)]
    slot_own, slot_near, slot_far = [], [], []
    for index in range(half_cap):
        even = (2 * (index // own_cap)) * own_cap + index % own_cap
        low = my_low[:, r_slots + even : r_slots + even + 1]
        high = my_low[:, r_slots + even + own_cap : r_slots + even + own_cap + 1]
        column = jnp.where(part == 0, low, high)
        slot_own.append(jnp.where(own_columns == column, own_at, -1))
        slot_near.append(jnp.where(near_columns == column, near_at, -1))
        slot_far.append(jnp.where(far_columns == column, far_at, -1))
    code = jnp.full(above, -1, jnp.int32)
    for j in range(both):
        block = my_low if j < r_slots else my_high
        named = block[:, j % r_slots : j % r_slots + 1]
        in_own = own_fine == named
        in_near = near_fine == named
        in_far = far_fine == named
        for index in range(half_cap):
            found = jnp.where(in_own, slot_own[index], -1)
            found = jnp.where(in_near, slot_near[index], found)
            found = jnp.where(in_far, slot_far[index], found)
            best = jnp.max(found, axis=1, keepdims=True)
            code = jnp.where(table_lanes == index * both + j, best, code)
    tables[0:row_count, :] = jnp.where((code >= 0) & (code < REMOTE), code, zero_own)
    away = code >= REMOTE
    rank = away.astype(jnp.int32)
    table_j = lax.rem(table_lanes, both)
    step = 1
    while step < both:
        rank = rank + jnp.where(table_j >= step, pltpu.roll(rank, step, 1), 0)
        step *= 2
    job = jnp.where(away, (code - REMOTE) * both + table_j, -1)
    rank = jnp.where(away, rank - 1 + (table_lanes // both) * JOBS, -1)
    short = jnp.full(above, -1, jnp.int32)
    for at in range(half_cap * JOBS):
        best = jnp.max(jnp.where(rank == at, job, -1), axis=1, keepdims=True)
        short = jnp.where(table_lanes == at, best, short)
    job_j = lax.rem(jnp.maximum(short, 0), both)
    job_c = lax.broadcasted_iota(jnp.int32, above, 0)
    job_r = (job_j // r_slots) * (row_count * r_slots) + job_c * r_slots + lax.rem(job_j, r_slots)
    tables[row_count : 2 * row_count, :] = jnp.where(short >= 0, short // both, zero_near)
    tables[2 * row_count : 3 * row_count, :] = job_r
    code_copy = pltpu.make_async_copy(tables, codes, table_sems.at[1])
    code_copy.start()

    code_copy.wait()
    own_r.wait()
    mate_r.wait_recv()
    if scans < rounds:
        scan_step()

    def own_stage(c, carry):
        for index in range(0, half_cap, 2):
            total = None
            for j in range(0, both, 2):
                left = jnp.concatenate(
                    [pair_r[x // r_slots * row_count * r_slots + c * r_slots + x % r_slots] for x in (j, j + 1)], axis=1
                )
                right = jnp.concatenate(
                    [
                        jnp.concatenate(
                            [pair_a[codes[c, slot * both + x]] for slot in (index, index + 1)], axis=1
                        )
                        for x in (j, j + 1)
                    ],
                    axis=0,
                )
                term = jnp.dot(left, right, preferred_element_type=jnp.float32)
                total = term if total is None else total + term
            sums[c * half_cap + index] = total[:, :tile]
            sums[c * half_cap + index + 1] = total[:, tile:]
        return carry

    def share(index):
        return min(index * row_count // (near_chunks - 1), row_count)

    lag = 3
    for index in range(near_chunks - 1):
        near_copy(index).wait_recv()
        if index < far_chunks:
            @pl.when(has_onward)
            def _():
                far_copy(index).start()
        mate_copy(near_view(index), near_pair_sems).start()
        if -1 <= index - lag < far_chunks:
            take_far(index - lag)
        lax.fori_loop(
            share(index), share(index + 1), own_stage, 0
        )
        if index % 3 == 1 and scans < rounds:
            scan_step()
    for index in range(max(near_chunks - 1 - lag, -1), far_chunks):
        take_far(index)
    while scans < rounds:
        scan_step()

    flags = jnp.where((scan_lane == 1) | (scan_lane == 2), state, 0)
    flags = jnp.max(jnp.max(flags, axis=1, keepdims=True), axis=0, keepdims=True)
    flag_ref[...] = jnp.broadcast_to((flags > 0).astype(jnp.int32), flag_ref.shape)
    flag_copy = pltpu.make_async_copy(flag_ref, flag_hbm, table_sems.at[0])
    flag_copy.start()
    reached = jnp.where(scan_lane == 0, state, 0)
    reached = jnp.max(jnp.max(reached, axis=1, keepdims=True), axis=0, keepdims=True)
    earlier = lax.broadcasted_iota(jnp.int32, small, 0) < lax.broadcasted_iota(jnp.int32, small, 1)
    counts = jnp.broadcast_to(own_counts, small)
    inner_sum = jnp.sum(jnp.where(earlier, counts, 0), axis=0, keepdims=True)
    offsets_ref[...] = inner_sum + (reached - total_count)

    near_copy(near_chunks - 1).wait_recv()
    wait_bytes(landed.at[pl.ds(0, near_slots - last_slots)], near_pair_sems.at[1])

    @pl.when(has_far)
    def _():
        wait_bytes(landed.at[pl.ds(0, far_slots)], far_pair_sems.at[1])

    ahead_of = [lax.rem(index // own_cap + pairs - group // 2, pairs) for index in range(half_cap)]

    def near_stage(c, carry):
        for index in range(half_cap):
            jobs = range(index * JOBS, (index + 1) * JOBS)
            left = jnp.concatenate([pair_r[codes[2 * row_count + c, x]] for x in jobs], axis=1)
            right = jnp.concatenate([landed[codes[row_count + c, x]] for x in jobs], axis=0)
            total = sums[c * half_cap + index] + jnp.dot(
                left, right, preferred_element_type=jnp.float32
            )
            place = ahead_of[index] * row_count * own_cap + c * own_cap + index % own_cap
            out_ref[place] = total.astype(out_ref.dtype)
        return carry

    lax.fori_loop(0, row_count, near_stage, 0, unroll=8)

    flag_copy.wait()
    wait_bytes(close.at[pl.ds(0, 2)], close_sems.at[0, 0])
    to_mate.wait_send()
    mate_a.wait_send()
    mate_r.wait_send()
    early_copy.wait_send()
    place_copy.wait_send()
    wait_bytes(packed, near_send.at[0])
    if groups > 2:
        wait_bytes(told.at[pl.ds(0, groups - 1)], told_sems.at[0])
    wait_bytes(landed.at[pl.ds(0, near_slots - last_slots)], near_pair_sems.at[0])

    @pl.when(has_onward)
    def _():
        wait_bytes(landed.at[pl.ds(0, far_slots)], far_send.at[0])

    @pl.when(has_far)
    def _():
        wait_bytes(close.at[pl.ds(2, 2)], close_sems.at[0, 1])
        wait_bytes(landed.at[pl.ds(0, far_slots)], far_pair_sems.at[0])

    for k in range(rounds):
        @pl.when(above_there[k])
        def _():
            scan_copy(k, 0).wait_send()

        @pl.when(below_there[k])
        def _():
            scan_copy(k, 1).wait_send()


def put_kernel(tiles_ref, offsets_ref, tiles_out, offsets_out, sems):
    copies = [
        pltpu.make_async_copy(tiles_ref, tiles_out, sems.at[0]),
        pltpu.make_async_copy(offsets_ref, offsets_out, sems.at[1]),
    ]
    for copy in copies:
        copy.start()
    for copy in copies:
        copy.wait()


def pair_sum_kernel(pairs, own, part_ref, landed, send_sems, recv_sems):
    row = lax.axis_index("rows")
    group = lax.axis_index("inner")
    core = lax.rem(group, 2)
    barrier = pltpu.get_barrier_semaphore()

    def place(ahead):
        return (row, 2 * lax.rem(group // 2 + ahead, pairs) + core)

    for ahead in range(1, pairs):
        pl.semaphore_signal(barrier, inc=1, device_id=place(ahead), device_id_type=MESH)
    pl.semaphore_wait(barrier, pairs - 1)
    copies = []
    for ahead in range(1, pairs):
        copy = pltpu.make_async_remote_copy(
            src_ref=part_ref.at[pl.ds(ahead * own, own)],
            dst_ref=landed.at[ahead - 1],
            send_sem=send_sems.at[ahead - 1],
            recv_sem=recv_sems.at[ahead - 1],
            device_id=place(ahead),
            device_id_type=MESH,
        )
        copy.start()
        copies.append(copy)
    for copy in copies:
        copy.wait()


def fused_body(rows, groups, r_tiles, r_cols, a_tiles, a_cols, c_cols, c_counts):
    local_rows, op_slots, tile, _ = a_tiles.shape
    row_count, r_slots = r_tiles.shape[:2]
    cap = c_cols.shape[1]
    tiles = local_rows * op_slots
    pairs = groups // 2
    own_cap = cap // groups
    half_cap = cap // 2
    width = -(-2 * tiles // 128) * 128
    chunks = []
    for size in [CHUNK] * (PASS_SLOTS // CHUNK) + list(LAST_CHUNKS):
        chunks.append((sum(before for _, before in chunks), size))
    list_slots = sum(size for _, size in chunks)
    pass_slots = PASS_SLOTS
    dims = (
        rows, groups, local_rows, op_slots, r_slots, cap, width, list_slots, pass_slots, tuple(chunks)
    )
    near_chunks = len(chunks)
    far_chunks = PASS_SLOTS // CHUNK
    early = min(EARLY, op_slots)
    near_slots = early + list_slots
    far_slots = early + pass_slots
    rounds = (rows - 1).bit_length()
    dtype = a_tiles.dtype
    out_dtype = jnp.bfloat16 if pairs == 1 else jnp.float32
    own = row_count * own_cap
    vmem = pl.BlockSpec(memory_space=pltpu.VMEM)
    anywhere = pl.BlockSpec(memory_space=pl.ANY)
    dma = pltpu.SemaphoreType.DMA
    block = (row_count, 128)
    part, offsets, flag = pl.pallas_call(
        functools.partial(fused_kernel, dims),
        out_shape=(
            jax.ShapeDtypeStruct((pairs * own, tile, tile), out_dtype),
            jax.ShapeDtypeStruct((1, row_count), jnp.int32),
            jax.ShapeDtypeStruct((1, 128), jnp.int32),
        ),
        in_specs=[anywhere] * 6,
        out_specs=(vmem, vmem, anywhere),
        scratch_shapes=[
            pltpu.VMEM((1, 128), jnp.int32),
            pltpu.VMEM(r_cols.shape, jnp.int32),
            pltpu.VMEM(c_cols.shape, jnp.int32),
            pltpu.VMEM((1, row_count), jnp.int32),
            pltpu.VMEM((op_slots, a_cols.shape[0]), jnp.int32),
            pltpu.VMEM(block, jnp.int32),
            pltpu.VMEM((5,) + block, jnp.int32),
            pltpu.VMEM((2, 8, width), jnp.int32),
            pltpu.VMEM((2 * tiles + 1, tile, tile), dtype),
            pltpu.VMEM((2 * row_count * r_slots, tile, tile), dtype),
            pltpu.VMEM((list_slots, tile, tile), dtype),
            pltpu.VMEM((2 * (near_slots + far_slots) + 1, tile, tile), dtype),
            pltpu.VMEM((row_count * half_cap, tile, tile), jnp.float32),
            pltpu.VMEM((3 * row_count, width), jnp.int32),
            pltpu.SMEM((3 * row_count, width), jnp.int32),
            pltpu.SMEM((8, width), jnp.int32),
            pltpu.VMEM((groups, 8, 128), jnp.int32),
            pltpu.VMEM((rounds, 8, 128), jnp.int32),
            pltpu.VMEM((rounds, 2, 8, 128), jnp.int32),
            dma((6,)),
            dma((2, 3)),
            dma((2, 2)),
            dma((2,)),
            dma((2,)),
            dma((near_chunks,)),
            dma((1,)),
            dma((2,)),
            dma((far_chunks + 1,)),
            dma((1,)),
            dma((2,)),
            dma((2,)),
            dma((2,)),
            dma((2, rounds, 2)),
        ],
        compiler_params=pltpu.CompilerParams(collective_id=40, has_side_effects=True),
        name="fused",
    )(
        r_cols,
        c_cols,
        c_counts[None, :],
        a_cols.T,
        a_tiles.reshape(tiles, tile, tile),
        r_tiles.reshape(row_count * r_slots, tile, tile),
    )
    if pairs == 1:
        c_tiles = part
    else:
        landed = pl.pallas_call(
            functools.partial(pair_sum_kernel, pairs, own),
            out_shape=jax.ShapeDtypeStruct((pairs - 1, own, tile, tile), jnp.float32),
            in_specs=[anywhere],
            out_specs=anywhere,
            scratch_shapes=[dma((pairs - 1,)), dma((pairs - 1,))],
            compiler_params=pltpu.CompilerParams(collective_id=41, has_side_effects=True),
            name="pair_sums",
        )(part)
        c_tiles = part[:own]
        for ahead in range(pairs - 1):
            c_tiles = c_tiles + landed[ahead]
        c_tiles = c_tiles.astype(jnp.bfloat16)
    return c_tiles.reshape(row_count, own_cap, tile, tile), offsets[0], flag[0, 0]


def body(rows, groups, *args):
    if rows % 2 or groups % 2:
        return plain_body(rows, groups, *args)
    c_tiles, offsets, flag = fused_body(rows, groups, *args)

    def again(c_tiles, offsets, *args):
        return plain_body(rows, groups, *args)

    def keep(c_tiles, offsets, *args):
        return c_tiles, offsets

    c_tiles, offsets = lax.cond(flag > 0, again, keep, c_tiles, offsets, *args)
    vmem = pl.BlockSpec(memory_space=pltpu.VMEM)
    anywhere = pl.BlockSpec(memory_space=pl.ANY)
    c_tiles, offsets = pl.pallas_call(
        put_kernel,
        out_shape=(
            jax.ShapeDtypeStruct(c_tiles.shape, c_tiles.dtype),
            jax.ShapeDtypeStruct((1,) + offsets.shape, offsets.dtype),
        ),
        in_specs=[vmem, vmem],
        out_specs=(anywhere, anywhere),
        scratch_shapes=[pltpu.SemaphoreType.DMA((2,))],
        name="put",
    )(c_tiles, offsets[None, :])
    return c_tiles, offsets[0]


def solution(mesh):
    rows = mesh.shape["rows"]
    groups = mesh.shape["inner"]
    return jax.shard_map(
        functools.partial(body, rows, groups),
        mesh=mesh,
        in_specs=(
            P("rows", "inner", None, None),
            P("rows", "inner"),
            P(("rows", "inner"), None, None, None),
            P(),
            P("rows", None),
            P("rows"),
        ),
        out_specs=(P("rows", "inner", None, None), P("rows")),
        check_vma=False,
    )
```

```python
import functools

import jax
import jax.numpy as jnp
from jax import lax
from jax.experimental import pallas as pl
from jax.experimental.pallas import tpu as pltpu
from jax.sharding import PartitionSpec as P

MESH = pl.DeviceIdType.MESH
BATCH = 4


def plan_kernel(
    dims, r_cols_ref, c_cols_ref, counts_ref, columns_ref, code_ref, plan_ref,
    meta_ref, gathered, needs, send_sem, recv_sem,
):
    rows, groups, local_rows, op_slots, r_slots, cap, half = dims
    width = 2 * half
    count = rows * groups
    tiles = local_rows * op_slots
    row = lax.axis_index("rows")
    group = lax.axis_index("inner")
    me = row * groups + group

    barrier = pltpu.get_barrier_semaphore()

    def place(step):
        other = lax.rem(me + step, count)
        return (other // groups, lax.rem(other, groups))

    def greet(step, carry):
        pl.semaphore_signal(barrier, inc=1, device_id=place(step), device_id_type=MESH)
        return carry

    lax.fori_loop(1, count, greet, 0)
    row_count = r_cols_ref.shape[0]
    live = r_slots + cap
    lanes = lax.broadcasted_iota(jnp.int32, (row_count, width), 1)
    above = lax.broadcasted_iota(jnp.int32, (row_count, width), 0)
    small = (row_count, row_count)
    diagonal = lax.broadcasted_iota(jnp.int32, small, 0) == lax.broadcasted_iota(jnp.int32, small, 1)
    spread_counts = jnp.broadcast_to(counts_ref[...], small)
    own_counts = jnp.sum(jnp.where(diagonal, spread_counts, 0), axis=1, keepdims=True)
    meta_ref[...] = jnp.full(meta_ref.shape, -9, jnp.int32)
    meta_ref[:, 0:r_slots] = r_cols_ref[...]
    meta_ref[:, r_slots:live] = c_cols_ref[...]
    meta_ref[:, live : live + 1] = own_counts
    gathered[me] = meta_ref[...]
    pl.semaphore_wait(barrier, count - 1)

    def post(step, carry):
        pltpu.make_async_remote_copy(
            src_ref=meta_ref,
            dst_ref=gathered.at[me],
            send_sem=send_sem,
            recv_sem=recv_sem,
            device_id=place(step),
            device_id_type=MESH,
        ).start()
        return carry

    lax.fori_loop(1, count, post, 0)
    everyone = gathered.at[pl.ds(0, count - 1)]
    pltpu.make_async_copy(everyone, everyone, send_sem).wait()
    pltpu.make_async_copy(everyone, everyone, recv_sem).wait()

    def matches(block, columns, fine_rows):
        named = fine_rows == block[:, 0:1]
        for j in range(1, r_slots):
            named = named | (fine_rows == block[:, j : j + 1])
        slot = jnp.full((row_count, width), -1, jnp.int32)
        for s in range(cap):
            slot = jnp.where(columns == block[:, r_slots + s : r_slots + s + 1], s, slot)
        return jnp.where(named, slot, -1)

    shift = jnp.where(lanes < half, -groups, groups) * local_rows
    tile = jnp.where(lanes < half, lanes, lanes - half)
    lane_rows = jnp.where(tile < tiles, shift + tile // op_slots, -(1 << 24))
    low_lanes = lanes[0:1] < half

    def near_matches(device):
        before = columns_ref[pl.ds(jnp.maximum(device - groups, 0), 1), :]
        after = columns_ref[pl.ds(jnp.minimum(device + groups, count - 1), 1), :]
        columns = jnp.where(low_lanes, before, after)
        return matches(gathered[device], columns, lane_rows + device * local_rows)

    def wanted(found):
        return jnp.max((found >= 0).astype(jnp.int32), axis=0, keepdims=True)

    def gather_needs(device, carry):
        needs[pl.ds(device, 1), :] = wanted(near_matches(device))
        return carry

    lax.fori_loop(0, count, gather_needs, 0, unroll=4)
    every = needs[...]
    low_side = lax.broadcasted_iota(jnp.int32, every.shape, 1) < half
    low = jnp.sum(jnp.where(low_side, every, 0), axis=1, keepdims=True)
    high = jnp.sum(jnp.where(low_side, 0, every), axis=1, keepdims=True)
    most = jnp.max(jnp.maximum(low, high), axis=0, keepdims=True)

    down = lax.broadcasted_iota(jnp.int32, (width, width), 0)
    across = lax.broadcasted_iota(jnp.int32, (width, width), 1)
    same = (down < half) == (across < half)

    def ranks(need):
        spread = jnp.broadcast_to(need, (width, width))
        column = jnp.sum(jnp.where(down == across, spread, 0), axis=1, keepdims=True)
        before = jnp.sum(jnp.where((across < down) & same, spread, 0), axis=1, keepdims=True)
        along = jnp.sum(
            jnp.where((down < across) & same, jnp.broadcast_to(column, (width, width)), 0),
            axis=0,
            keepdims=True,
        )
        return column, before, along

    def send_list(device, high):
        column, before, _ = ranks(needs[pl.ds(device, 1), :])
        first = half if high else 0
        mine = (down >= half) if high else (down < half)
        chosen = mine & (column > 0) & (before == across)
        return jnp.sum(jnp.where(chosen, down - first, 0), axis=0, keepdims=True)

    left = jnp.maximum(row - 1, 0) * groups + group
    right = jnp.minimum(row + 1, rows - 1) * groups + group
    plan_ref[0:1, :] = send_list(left, True)
    plan_ref[1:2, :] = send_list(right, False)

    found = near_matches(me)
    _, _, along = ranks(wanted(found))
    slot_at = along + jnp.where(lanes[0:1] < half, tiles, 2 * tiles)
    code_ref[:, 0:width] = jnp.where(found >= 0, found + cap * slot_at, -1)
    fine = me * local_rows + jnp.where(lanes < tiles, lanes // op_slots, 0)
    fine = jnp.where(lanes < tiles, fine, -5)
    found = matches(gathered[me], columns_ref[pl.ds(me, 1), :], fine)
    code_ref[:, width:] = jnp.where(found >= 0, found + cap * lanes, -1)

    def earlier(index, total):
        block = gathered[index * groups]
        return total + jnp.sum(block[:, live : live + 1], axis=0, keepdims=True)

    first = lax.fori_loop(0, row, earlier, jnp.zeros((1, 1), jnp.int32))
    counts = jnp.broadcast_to(own_counts, (row_count, width))
    inner_sum = jnp.sum(jnp.where(above < lanes, counts, 0), axis=0, keepdims=True)
    plan_ref[2:3, :] = inner_sum + first
    level = jnp.zeros((1, 1), jnp.int32)
    for size in sizes_for(tiles)[:-1]:
        level = level + (most > size).astype(jnp.int32)
    plan_ref[3:4, :] = jnp.broadcast_to(level, (1, width))


def halo_kernel(rows, size, plan_ref, a_ref, out_ref, packed, send_sems, recv_sems):
    row = lax.axis_index("rows")
    group = lax.axis_index("inner")
    barrier = pltpu.get_barrier_semaphore()
    has_left = row > 0
    has_right = row < rows - 1

    @pl.when(has_left)
    def _():
        pl.semaphore_signal(barrier, inc=1, device_id=(row - 1, group), device_id_type=MESH)

    @pl.when(has_right)
    def _():
        pl.semaphore_signal(barrier, inc=1, device_id=(row + 1, group), device_id_type=MESH)

    def pack(index, carry):
        packed[0, index] = a_ref[plan_ref[0, index]]
        packed[1, index] = a_ref[plan_ref[1, index]]
        return carry

    lax.fori_loop(0, size, pack, 0, unroll=2)

    pl.semaphore_wait(barrier, has_left.astype(jnp.int32) + has_right.astype(jnp.int32))

    def copy(side, other):
        return pltpu.make_async_remote_copy(
            src_ref=packed.at[side],
            dst_ref=out_ref.at[1 - side, pl.ds(0, size)],
            send_sem=send_sems.at[side],
            recv_sem=recv_sems.at[1 - side],
            device_id=(other, group),
            device_id_type=MESH,
        )

    @pl.when(has_left)
    def _():
        copy(0, row - 1).start()

    @pl.when(has_right)
    def _():
        copy(1, row + 1).start()

    @pl.when(has_left)
    def _():
        copy(0, row - 1).wait_send()
        copy(1, row - 1).wait_recv()

    @pl.when(has_right)
    def _():
        copy(1, row + 1).wait_send()
        copy(0, row + 1).wait_recv()


def product_kernel(dims, code_ref, cols_ref, r_ref, a_ref, halo_ref, out_ref, tiles_ref, jobs, sems):
    rows, groups, local_rows, op_slots, r_slots, cap, half = dims
    width = 2 * half
    tiles = local_rows * op_slots
    row_count = cols_ref.shape[0]
    own_cap = cap // groups
    row = lax.axis_index("rows")
    group = lax.axis_index("inner")
    own = pltpu.make_async_copy(a_ref, tiles_ref.at[pl.ds(0, tiles)], sems.at[0])
    near = pltpu.make_async_copy(halo_ref, tiles_ref.at[pl.ds(tiles, 2 * tiles)], sems.at[1])
    own.start()
    near.start()
    last = groups * row_count * own_cap
    scale = 1 << (3 * tiles * cap - 1).bit_length()

    def clear(index, carry):
        out_ref[index] = jnp.zeros(out_ref.shape[1:], jnp.float32)
        return carry

    lax.fori_loop(0, last, clear, 0, unroll=4)

    def list_row(c, found):
        def list_slot(j, found):
            fine = cols_ref[c, j]
            side = fine // (local_rows * groups) - row
            base = jnp.where(side == 0, width, jnp.where(side < 0, 0, half))
            base = base + lax.rem(fine, local_rows) * op_slots
            for t in range(op_slots):
                code = code_ref[c, base + t]
                jobs[found] = (c * r_slots + j) * scale + code
                found = found + (code >= 0).astype(jnp.int32)
            return found

        return lax.fori_loop(0, r_slots, list_slot, found)

    found = lax.fori_loop(0, row_count, list_row, jnp.int32(0))
    for extra in range(BATCH):
        jobs[found + extra] = -1
    own.wait()
    near.wait()

    def batch(step, carry):
        results = []
        targets = []
        for extra in range(BATCH):
            job = jobs[step * BATCH + extra]
            valid = job >= 0
            job = jnp.maximum(job, 0)
            pair = job // scale
            code = lax.rem(job, scale)
            slot = lax.rem(code, cap)
            ahead = lax.rem(slot // own_cap + groups - group, groups)
            target = (ahead * row_count + pair // r_slots) * own_cap + lax.rem(slot, own_cap)
            targets.append(jnp.where(valid, target, last))
            results.append(
                jnp.dot(
                    r_ref[pair],
                    tiles_ref[code // cap],
                    preferred_element_type=jnp.float32,
                )
            )
        for extra in range(BATCH):
            target = targets[extra]
            out_ref[target] = out_ref[target] + results[extra]
        return carry

    lax.fori_loop(0, (found + BATCH - 1) // BATCH, batch, 0)


def sum_kernel(groups, own, part_ref, landed, send_sems, recv_sems):
    row = lax.axis_index("rows")
    group = lax.axis_index("inner")
    barrier = pltpu.get_barrier_semaphore()
    for ahead in range(1, groups):
        pl.semaphore_signal(
            barrier, inc=1, device_id=(row, lax.rem(group + ahead, groups)), device_id_type=MESH
        )
    pl.semaphore_wait(barrier, groups - 1)
    copies = []
    for ahead in range(1, groups):
        copy = pltpu.make_async_remote_copy(
            src_ref=part_ref.at[pl.ds(ahead * own, own)],
            dst_ref=landed.at[ahead - 1],
            send_sem=send_sems.at[ahead - 1],
            recv_sem=recv_sems.at[ahead - 1],
            device_id=(row, lax.rem(group + ahead, groups)),
            device_id_type=MESH,
        )
        copy.start()
        copies.append(copy)
    for copy in copies:
        copy.wait()


def sizes_for(tiles):
    steps = [16, 18, 20, 21, 22, 23, 24, 25, 26, 27, 28, 29, 30, 32, 36, 42]
    return [size for size in steps if size < tiles] + [tiles]


def plain_body(rows, groups, r_tiles, r_cols, a_tiles, a_cols, c_cols, c_counts):
    local_rows, op_slots, tile, _ = a_tiles.shape
    row_count, r_slots = r_tiles.shape[:2]
    cap = c_cols.shape[1]
    tiles = local_rows * op_slots
    half = -(-tiles // 64) * 64
    width = 2 * half
    count = rows * groups
    own_cap = cap // groups
    dims = (rows, groups, local_rows, op_slots, r_slots, cap, half)
    vmem = pl.BlockSpec(memory_space=pltpu.VMEM)
    smem = pl.BlockSpec(memory_space=pltpu.SMEM)
    anywhere = pl.BlockSpec(memory_space=pl.ANY)

    flat = a_cols.reshape(count, tiles)
    flat = jnp.pad(flat, ((0, 0), (0, half - tiles)), constant_values=-2)
    columns = jnp.concatenate([flat, flat], axis=1)

    code, plan = pl.pallas_call(
        functools.partial(plan_kernel, dims),
        out_shape=(
            jax.ShapeDtypeStruct((row_count, 2 * width), jnp.int32),
            jax.ShapeDtypeStruct((8, width), jnp.int32),
        ),
        in_specs=[vmem] * 4,
        out_specs=(vmem, vmem),
        scratch_shapes=[
            pltpu.VMEM((row_count, width), jnp.int32),
            pltpu.VMEM((count, row_count, width), jnp.int32),
            pltpu.VMEM((count, width), jnp.int32),
            pltpu.SemaphoreType.DMA,
            pltpu.SemaphoreType.DMA,
        ],
        compiler_params=pltpu.CompilerParams(collective_id=0, has_side_effects=True),
        name="plan",
    )(r_cols, c_cols, c_counts[None, :], columns)

    flat_a = a_tiles.reshape(tiles, tile, tile)
    sizes = sizes_for(tiles)

    def exchange(number, size, plan, flat_a):
        return pl.pallas_call(
            functools.partial(halo_kernel, rows, size),
            out_shape=jax.ShapeDtypeStruct((2, tiles, tile, tile), a_tiles.dtype),
            in_specs=[smem, vmem],
            out_specs=anywhere,
            scratch_shapes=[
                pltpu.VMEM((2, size, tile, tile), a_tiles.dtype),
                pltpu.SemaphoreType.DMA((2,)),
                pltpu.SemaphoreType.DMA((2,)),
            ],
            compiler_params=pltpu.CompilerParams(collective_id=number + 2, has_side_effects=True),
            name=f"halo{size}",
        )(plan, flat_a)

    halo = lax.switch(
        plan[3, 0],
        [functools.partial(exchange, number, size) for number, size in enumerate(sizes)],
        plan,
        flat_a,
    )

    slots = row_count * r_slots * op_slots + BATCH
    partial_value = pl.pallas_call(
        functools.partial(product_kernel, dims),
        out_shape=jax.ShapeDtypeStruct((row_count * cap + 1, tile, tile), jnp.float32),
        in_specs=[smem, smem, vmem, anywhere, anywhere],
        out_specs=vmem,
        scratch_shapes=[
            pltpu.VMEM((3 * tiles, tile, tile), a_tiles.dtype),
            pltpu.SMEM((slots,), jnp.int32),
            pltpu.SemaphoreType.DMA((2,)),
        ],
        name="products",
    )(
        code,
        r_cols,
        r_tiles.reshape(row_count * r_slots, tile, tile),
        flat_a,
        halo.reshape(2 * tiles, tile, tile),
    )

    own_count = row_count * own_cap
    landed = pl.pallas_call(
        functools.partial(sum_kernel, groups, own_count),
        out_shape=jax.ShapeDtypeStruct((groups - 1, own_count, tile, tile), jnp.float32),
        in_specs=[anywhere],
        out_specs=anywhere,
        scratch_shapes=[
            pltpu.SemaphoreType.DMA((groups - 1,)),
            pltpu.SemaphoreType.DMA((groups - 1,)),
        ],
        compiler_params=pltpu.CompilerParams(collective_id=1, has_side_effects=True),
        name="sums",
    )(partial_value)
    c_tiles = partial_value[:own_count]
    for ahead in range(groups - 1):
        c_tiles = c_tiles + landed[ahead]
    c_tiles = c_tiles.astype(jnp.bfloat16)
    return (c_tiles.reshape(row_count, own_cap, tile, tile), plan[2, :row_count])

EARLY = 7
SCAN_AT = (1, 2, 5)
PASS_SLOTS = 15
CHUNK = 3
LAST_CHUNKS = (3, 3, 3, 2)
JOBS = 4
REMOTE = 1 << 14


def fused_kernel(
    dims, r_cols_hbm, c_cols_hbm, counts_hbm, columns_hbm, a_ref, r_ref,
    out_ref, offsets_ref, flag_hbm,
    flag_ref, r_cols_ref, c_cols_ref, counts_ref, columns_ref,
    meta, close, placing, pair_a, pair_r, packed, landed, sums, tables, codes, picks,
    told, scan_out, scan_in,
    local_sems, close_sems, pair_sems, place_sems, early_sems, near_sems, near_send,
    near_pair_sems, far_sems, far_send, far_pair_sems, table_sems, told_sems, scan_sems,
):
    (rows, groups, local_rows, op_slots, r_slots, cap, width, list_slots, pass_slots, chunks) = dims
    pairs = groups // 2
    tiles = local_rows * op_slots
    span = 2 * local_rows
    own_cap = cap // groups
    half_cap = cap // 2
    both = 2 * r_slots
    row_count = r_cols_ref.shape[0]
    live = r_slots + cap
    early = min(EARLY, op_slots)
    near_slots = early + list_slots
    far_slots = early + pass_slots
    near_chunks = len(chunks)
    far_chunks = sum(start < pass_slots for start, _ in chunks)
    last_slots = chunks[-1][1]
    far_base = 2 * near_slots
    zero_near = 2 * (near_slots + far_slots)
    zero_own = 2 * tiles
    rounds = (rows - 1).bit_length()

    row = lax.axis_index("rows")
    group = lax.axis_index("inner")
    part = lax.rem(group, 2)
    first_group = group - part
    mate = first_group + 1 - part
    odd = lax.rem(row, 2)
    near = row + 1 - 2 * odd
    far = row - 1 + 2 * odd
    has_far = (far >= 0) & (far < rows)
    onward = near + 1 - 2 * odd
    has_onward = (onward >= 0) & (onward < rows)
    mate_place = (row, mate)

    barrier = pltpu.get_barrier_semaphore()

    def greet(place):
        pl.semaphore_signal(barrier, inc=1, device_id=place, device_id_type=MESH)

    for core in range(2):
        greet((near, first_group + core))

    @pl.when(has_far)
    def _():
        for core in range(2):
            greet((far, first_group + core))

    for ahead in range(1, groups):
        greet((row, lax.rem(group + ahead, groups)))

    small_copies = [
        pltpu.make_async_copy(src, dst, local_sems.at[2 + index])
        for index, (src, dst) in enumerate(
            [
                (r_cols_hbm, r_cols_ref),
                (c_cols_hbm, c_cols_ref),
                (counts_hbm, counts_ref),
                (columns_hbm, columns_ref),
            ]
        )
    ]
    for copy in small_copies:
        copy.start()
    own_a = pltpu.make_async_copy(
        a_ref, pair_a.at[pl.ds(part * tiles, tiles)], local_sems.at[0]
    )
    own_r = pltpu.make_async_copy(r_ref, pair_r.at[pl.ds(part * row_count * r_slots, row_count * r_slots)], local_sems.at[1])
    own_a.start()
    own_r.start()

    def remote(src, dst, send_sem, recv_sem, place):
        return pltpu.make_async_remote_copy(
            src_ref=src, dst_ref=dst, send_sem=send_sem, recv_sem=recv_sem,
            device_id=place, device_id_type=MESH,
        )

    def wait_bytes(view, sem):
        pltpu.make_async_copy(view, view, sem).wait()

    small = (row_count, row_count)
    diagonal = lax.broadcasted_iota(jnp.int32, small, 0) == lax.broadcasted_iota(jnp.int32, small, 1)
    meta[...] = jnp.full(meta.shape, -9, jnp.int32)
    pair_a[zero_own] = jnp.zeros(pair_a.shape[1:], pair_a.dtype)
    landed[zero_near] = jnp.zeros(landed.shape[1:], landed.dtype)
    for copy in small_copies:
        copy.wait()
    spread_counts = jnp.broadcast_to(counts_ref[...], small)
    own_counts = jnp.sum(jnp.where(diagonal, spread_counts, 0), axis=1, keepdims=True)
    meta[:, 0:r_slots] = r_cols_ref[...]
    meta[:, r_slots:live] = c_cols_ref[...]
    pl.semaphore_wait(barrier, groups + 1 + 2 * has_far.astype(jnp.int32))

    def start_close(target, first, which):
        for core in range(2):
            remote(
                meta, close.at[first + part], close_sems.at[0, which], close_sems.at[1, which],
                (target, first_group + core),
            ).start()

    @pl.when(has_far)
    def _():
        start_close(far, 2, 1)

    start_close(near, 0, 0)
    to_mate = remote(meta, close.at[4], close_sems.at[0, 2], close_sems.at[1, 2], mate_place)
    to_mate.start()
    mate_a = remote(
        a_ref, pair_a.at[pl.ds(part * tiles, tiles)], pair_sems.at[0, 0], pair_sems.at[1, 0], mate_place
    )
    mate_a.start()

    own_a.wait()
    early_copy = remote(
        pair_a.at[pl.ds(part * tiles, early)], landed.at[pl.ds(part * near_slots, early)],
        early_sems.at[0], early_sems.at[1], (near, group),
    )
    early_copy.start()
    mate_r = remote(r_ref, pair_r.at[pl.ds(part * row_count * r_slots, row_count * r_slots)], pair_sems.at[0, 1], pair_sems.at[1, 1], mate_place)
    mate_r.start()

    lanes = lax.broadcasted_iota(jnp.int32, (1, width), 1)
    real = lanes < op_slots * span
    lane_slot = lanes // span
    lane_fine = jnp.where(real, lax.rem(lanes, span), -(1 << 24))
    lane_core = lax.rem(lanes, span) // local_rows
    lane_local = lax.rem(lanes, local_rows)
    lane_tile = lane_core * tiles + lane_local * op_slots + lane_slot
    late = jnp.where((lane_local > 0) | (lane_slot >= early), 1, 0)

    def pair_columns(which_row):
        start = (which_row * groups + first_group) * local_rows
        block = start // 128
        values = columns_ref[:, pl.ds(pl.multiple_of(block * 128, 128), 128)]
        if width > 128:
            values = jnp.concatenate([values] * (width // 128), axis=1)
        offset = start - block * 128
        total = jnp.zeros((1, width), jnp.int32)
        for t in range(op_slots):
            moved = pltpu.roll(values[t : t + 1, :], lax.rem(t * span - offset + 128 * width, width), 1)
            total = jnp.where(lane_slot == t, moved, total)
        return jnp.where(real, total, -2)

    def pair_fine(which_row):
        return lane_fine + (which_row * groups + first_group) * local_rows

    def named_by(meta_low, meta_high, fine):
        named = fine == meta_low[:, 0:1]
        for j in range(1, r_slots):
            named = named | (fine == meta_low[:, j : j + 1])
        for j in range(r_slots):
            named = named | (fine == meta_high[:, j : j + 1])
        return named

    def need_by_core(meta_low, meta_high, columns, fine):
        named = named_by(meta_low, meta_high, fine)
        needs = []
        for core in range(2):
            wanted = jnp.zeros(named.shape, jnp.bool_)
            for s in range(cap):
                if s // own_cap % 2 == core:
                    wanted = wanted | (columns == meta_low[:, r_slots + s : r_slots + s + 1])
            needs.append(jnp.max((named & wanted).astype(jnp.int32), axis=0, keepdims=True))
        return needs

    def need_of(meta_low, meta_high, columns, fine):
        low, high = need_by_core(meta_low, meta_high, columns, fine)
        return jnp.maximum(low, high)

    def before(need):
        total = need
        step = 1
        while step < width:
            total = total + jnp.where(lanes >= step, pltpu.roll(total, step, 1), 0)
            step *= 2
        return total - need

    def landing(places, count, base, slots):
        fits = (places >= 0) & (places < 2 * count)
        at = lax.rem(places, 2) * slots + early + places // 2
        at = jnp.where(late > 0, jnp.where(fits, at, -1), lane_core * slots + lane_slot)
        return jnp.where(real & (at >= 0), REMOTE + base + at, -1)

    own_columns = pair_columns(row)
    own_fine = pair_fine(row)

    near_columns = pair_columns(near)
    near_fine = pair_fine(near)
    far_row = jnp.clip(far, 0, rows - 1)
    far_columns = pair_columns(far_row)
    far_fine = jnp.where(has_far, pair_fine(far_row), -(1 << 24))
    to_mate.wait_recv()
    mine, other = meta[...], close[4]
    my_low = jnp.where(part == 0, mine, other)
    my_high = jnp.where(part == 0, other, mine)
    near_named = named_by(my_low, my_high, near_fine)
    far_named = named_by(my_low, my_high, far_fine)
    crowded = jnp.zeros((1, 1), jnp.int32)
    for s in range(cap):
        column = my_low[:, r_slots + s : r_slots + s + 1]
        hits = (near_named & (near_columns == column)).astype(jnp.int32)
        hits = hits + (far_named & (far_columns == column)).astype(jnp.int32)
        held = jnp.sum(hits, axis=1, keepdims=True)
        crowded = jnp.maximum(crowded, jnp.max(held, axis=0, keepdims=True))

    wait_bytes(close.at[pl.ds(0, 2)], close_sems.at[1, 0])
    near_low, near_high = [
        need * late for need in need_by_core(close[0], close[1], own_columns, own_fine)
    ]

    @pl.when(has_far)
    def _():
        wait_bytes(close.at[pl.ds(2, 2)], close_sems.at[1, 1])

    @pl.when(jnp.logical_not(has_far))
    def _():
        close[2] = jnp.full(close.shape[1:], -9, jnp.int32)
        close[3] = jnp.full(close.shape[1:], -9, jnp.int32)

    need_far = need_of(close[2], close[3], own_columns, own_fine) * late
    need_only = jnp.maximum(near_low, near_high) * (1 - need_far)
    lone_low = need_only * (1 - near_high)
    lone_high = need_only * (1 - near_low)
    lists = jnp.concatenate([need_far, need_only, lone_low, lone_high], axis=0)
    ahead_in = before(lists)
    totals = jnp.sum(lists, axis=1, keepdims=True)
    far_before, only_before, low_before, high_before = [ahead_in[x : x + 1] for x in range(4)]
    far_total, only_total, low_total, high_total = [totals[x : x + 1] for x in range(4)]
    last_low = (lone_low > 0) & (low_before < last_slots)
    last_high = (lone_high > 0) & (high_before < last_slots)
    need_rest = jnp.where(last_low | last_high, 0, need_only)
    near_total = far_total + only_total
    near_total = near_total - jnp.minimum(low_total, last_slots) - jnp.minimum(high_total, last_slots)
    rest_before = only_before - jnp.minimum(low_before, last_slots)
    rest_before = rest_before - jnp.minimum(high_before, last_slots)
    places = jnp.where(
        need_far > 0, far_before, jnp.where(need_rest > 0, rest_before + far_total, -1)
    )
    last_first = list_slots - last_slots
    places = jnp.where(places < 2 * last_first, places, -1)
    places = jnp.where(last_low, 2 * (last_first + low_before), places)
    places = jnp.where(last_high, 2 * (last_first + high_before) + 1, places)
    pick_rows = -(-list_slots // 8) * 8
    slot_down = lax.broadcasted_iota(jnp.int32, (pick_rows, width), 0)
    chosen = jnp.broadcast_to(places, (pick_rows, width)) == 2 * slot_down + part
    picked = jnp.sum(
        jnp.where(chosen, jnp.broadcast_to(lane_tile, (pick_rows, width)), 0), axis=1, keepdims=True
    )
    across = lax.broadcasted_iota(jnp.int32, (pick_rows, width), 1)
    pick_row = jnp.sum(
        jnp.where(slot_down == across, jnp.broadcast_to(picked, (pick_rows, width)), 0),
        axis=0, keepdims=True,
    )
    tables[0:8, :] = jnp.broadcast_to(pick_row, (8, width))
    pick_copy = pltpu.make_async_copy(tables.at[pl.ds(0, 8)], picks, table_sems.at[0])
    pick_copy.start()
    placing[0] = jnp.broadcast_to(landing(places, list_slots, 0, near_slots), placing.shape[1:])
    place_copy = remote(placing.at[0], placing.at[1], place_sems.at[0], place_sems.at[1], (near, group))
    place_copy.start()
    over = jnp.maximum(near_total - 2 * (list_slots - last_slots), far_total - 2 * pass_slots)
    over = jnp.maximum(over, crowded - JOBS)
    over = (over > 0).astype(jnp.int32)
    if groups > 2:
        told[group] = jnp.broadcast_to(over, told.shape[1:])

        def tell(ahead):
            return remote(
                told.at[group], told.at[group], told_sems.at[0], told_sems.at[1],
                (row, lax.rem(group + ahead, groups)),
            )

        for ahead in range(1, groups):
            tell(ahead).start()
        wait_bytes(told.at[pl.ds(0, groups - 1)], told_sems.at[1])
        over = told[0]
        for other_group in range(1, groups):
            over = over + told[other_group]

    tile = pair_a.shape[1]
    total_count = jnp.sum(own_counts, axis=0, keepdims=True)

    def scan_copy(k, side):
        other = row + (1 << k) if side == 0 else row - (1 << k)
        return remote(
            scan_out.at[k], scan_in.at[k, side], scan_sems.at[0, k, side], scan_sems.at[1, k, side],
            (other, group),
        )

    scan_shape = scan_out.shape[1:]
    scan_lane = lax.broadcasted_iota(jnp.int32, scan_shape, 1)
    above_there = [row + (1 << k) < rows for k in range(rounds)]
    below_there = [row - (1 << k) >= 0 for k in range(rounds)]

    def scan_send(k, state):
        scan_out[k] = state

        @pl.when(above_there[k])
        def _():
            scan_copy(k, 0).start()

        @pl.when(below_there[k])
        def _():
            scan_copy(k, 1).start()

    def scan_take(k, state):
        @pl.when(below_there[k])
        def _():
            scan_copy(k, 0).wait_recv()

        @pl.when(above_there[k])
        def _():
            scan_copy(k, 1).wait_recv()

        below = jnp.where((scan_lane < 2) & below_there[k], scan_in[k, 0], 0)
        beyond = jnp.where((scan_lane == 2) & above_there[k], scan_in[k, 1], 0)
        return state + below + beyond

    state = jnp.where(
        scan_lane == 0, jnp.broadcast_to(total_count, scan_shape),
        jnp.where(scan_lane < 3, over, 0),
    )
    scan_send(0, state)
    scans = 0

    def scan_step():
        nonlocal state, scans
        state = scan_take(scans, state)
        scans += 1
        if scans < rounds:
            scan_send(scans, state)

    mate_a.wait_recv()
    pick_copy.wait()

    def near_view(index):
        start, size = chunks[index]
        return landed.at[pl.ds(part * near_slots + early + start, size)]

    def near_copy(index):
        return remote(
            packed.at[pl.ds(*chunks[index])], near_view(index),
            near_send.at[0], near_sems.at[index], (near, group),
        )

    def pack(index):
        start, size = chunks[index]
        for slot in range(start, start + size):
            packed[slot] = pair_a[picks[0, slot]]

    pack(0)
    for index in range(near_chunks):
        if index + 1 < near_chunks:
            pack(index + 1)
        near_copy(index).start()

    def mate_copy(view, sems):
        return remote(view, view, sems.at[0], sems.at[1], mate_place)

    early_view = landed.at[pl.ds(part * near_slots, early)]
    early_far_view = landed.at[pl.ds(far_base + part * far_slots, early)]

    def far_view(index):
        start, size = chunks[index]
        return landed.at[pl.ds(far_base + part * far_slots + early + start, size)]

    early_far = remote(early_view, early_far_view, far_send.at[0], far_sems.at[far_chunks], (onward, group))

    def far_copy(index):
        return remote(
            near_view(index), far_view(index), far_send.at[0], far_sems.at[index], (onward, group)
        )

    def take_far(index):
        @pl.when(has_far)
        def _():
            if index < 0:
                early_far.wait_recv()
                mate_copy(early_far_view, far_pair_sems).start()
            else:
                far_copy(index).wait_recv()
                mate_copy(far_view(index), far_pair_sems).start()

    early_copy.wait_recv()

    @pl.when(has_onward)
    def _():
        early_far.start()

    mate_copy(early_view, near_pair_sems).start()
    if scans < rounds:
        scan_step()
    far_need = need_of(my_low, my_high, far_columns, far_fine) * late
    far_places = jnp.where(far_need > 0, before(far_need), -1)
    far_at = landing(far_places, pass_slots, far_base, far_slots)
    place_copy.wait_recv()
    near_at = placing[1][0:1, :]

    above = (row_count, width)
    table_lanes = lax.broadcasted_iota(jnp.int32, above, 1)
    own_at, near_at, far_at = [jnp.broadcast_to(x, above) for x in (lane_tile, near_at, far_at)]
    slot_own, slot_near, slot_far = [], [], []
    for index in range(half_cap):
        even = (2 * (index // own_cap)) * own_cap + index % own_cap
        low = my_low[:, r_slots + even : r_slots + even + 1]
        high = my_low[:, r_slots + even + own_cap : r_slots + even + own_cap + 1]
        column = jnp.where(part == 0, low, high)
        slot_own.append(jnp.where(own_columns == column, own_at, -1))
        slot_near.append(jnp.where(near_columns == column, near_at, -1))
        slot_far.append(jnp.where(far_columns == column, far_at, -1))
    code = jnp.full(above, -1, jnp.int32)
    for j in range(both):
        block = my_low if j < r_slots else my_high
        named = block[:, j % r_slots : j % r_slots + 1]
        in_own = own_fine == named
        in_near = near_fine == named
        in_far = far_fine == named
        for index in range(half_cap):
            found = jnp.where(in_own, slot_own[index], -1)
            found = jnp.where(in_near, slot_near[index], found)
            found = jnp.where(in_far, slot_far[index], found)
            best = jnp.max(found, axis=1, keepdims=True)
            code = jnp.where(table_lanes == index * both + j, best, code)
    tables[0:row_count, :] = jnp.where((code >= 0) & (code < REMOTE), code, zero_own)
    away = code >= REMOTE
    rank = away.astype(jnp.int32)
    table_j = lax.rem(table_lanes, both)
    step = 1
    while step < both:
        rank = rank + jnp.where(table_j >= step, pltpu.roll(rank, step, 1), 0)
        step *= 2
    job = jnp.where(away, (code - REMOTE) * both + table_j, -1)
    rank = jnp.where(away, rank - 1 + (table_lanes // both) * JOBS, -1)
    short = jnp.full(above, -1, jnp.int32)
    for at in range(half_cap * JOBS):
        best = jnp.max(jnp.where(rank == at, job, -1), axis=1, keepdims=True)
        short = jnp.where(table_lanes == at, best, short)
    job_j = lax.rem(jnp.maximum(short, 0), both)
    job_c = lax.broadcasted_iota(jnp.int32, above, 0)
    job_r = (job_j // r_slots) * (row_count * r_slots) + job_c * r_slots + lax.rem(job_j, r_slots)
    tables[row_count : 2 * row_count, :] = jnp.where(short >= 0, short // both, zero_near)
    tables[2 * row_count : 3 * row_count, :] = job_r
    code_copy = pltpu.make_async_copy(tables, codes, table_sems.at[1])
    code_copy.start()

    code_copy.wait()
    own_r.wait()
    mate_r.wait_recv()

    def own_stage(c, carry):
        for index in range(0, half_cap, 2):
            total = None
            for j in range(0, both, 2):
                left = jnp.concatenate(
                    [pair_r[x // r_slots * row_count * r_slots + c * r_slots + x % r_slots] for x in (j, j + 1)], axis=1
                )
                right = jnp.concatenate(
                    [
                        jnp.concatenate(
                            [pair_a[codes[c, slot * both + x]] for slot in (index, index + 1)], axis=1
                        )
                        for x in (j, j + 1)
                    ],
                    axis=0,
                )
                term = jnp.dot(left, right, preferred_element_type=jnp.float32)
                total = term if total is None else total + term
            sums[c * half_cap + index] = total[:, :tile]
            sums[c * half_cap + index + 1] = total[:, tile:]
        return carry

    def share(index):
        return min(index * row_count // (near_chunks - 1), row_count)

    lag = 3
    for index in range(near_chunks - 1):
        near_copy(index).wait_recv()
        if index < far_chunks:
            @pl.when(has_onward)
            def _():
                far_copy(index).start()
        mate_copy(near_view(index), near_pair_sems).start()
        if -1 <= index - lag < far_chunks:
            take_far(index - lag)
        lax.fori_loop(
            share(index), share(index + 1), own_stage, 0
        )
        if index in SCAN_AT and scans < rounds:
            scan_step()
    for index in range(max(near_chunks - 1 - lag, -1), far_chunks):
        take_far(index)
    while scans < rounds:
        scan_step()

    flags = jnp.where((scan_lane == 1) | (scan_lane == 2), state, 0)
    flags = jnp.max(jnp.max(flags, axis=1, keepdims=True), axis=0, keepdims=True)
    flag_ref[...] = jnp.broadcast_to((flags > 0).astype(jnp.int32), flag_ref.shape)
    flag_copy = pltpu.make_async_copy(flag_ref, flag_hbm, table_sems.at[0])
    flag_copy.start()
    reached = jnp.where(scan_lane == 0, state, 0)
    reached = jnp.max(jnp.max(reached, axis=1, keepdims=True), axis=0, keepdims=True)
    earlier = lax.broadcasted_iota(jnp.int32, small, 0) < lax.broadcasted_iota(jnp.int32, small, 1)
    counts = jnp.broadcast_to(own_counts, small)
    inner_sum = jnp.sum(jnp.where(earlier, counts, 0), axis=0, keepdims=True)
    offsets_ref[...] = inner_sum + (reached - total_count)

    near_copy(near_chunks - 1).wait_recv()
    wait_bytes(landed.at[pl.ds(0, near_slots - last_slots)], near_pair_sems.at[1])

    @pl.when(has_far)
    def _():
        wait_bytes(landed.at[pl.ds(0, far_slots)], far_pair_sems.at[1])

    ahead_of = [lax.rem(index // own_cap + pairs - group // 2, pairs) for index in range(half_cap)]

    def near_stage(c, carry):
        for index in range(half_cap):
            jobs = range(index * JOBS, (index + 1) * JOBS)
            left = jnp.concatenate([pair_r[codes[2 * row_count + c, x]] for x in jobs], axis=1)
            right = jnp.concatenate([landed[codes[row_count + c, x]] for x in jobs], axis=0)
            total = sums[c * half_cap + index] + jnp.dot(
                left, right, preferred_element_type=jnp.float32
            )
            place = ahead_of[index] * row_count * own_cap + c * own_cap + index % own_cap
            out_ref[place] = total.astype(out_ref.dtype)
        return carry

    lax.fori_loop(0, row_count, near_stage, 0, unroll=8)

    flag_copy.wait()
    wait_bytes(close.at[pl.ds(0, 2)], close_sems.at[0, 0])
    to_mate.wait_send()
    mate_a.wait_send()
    mate_r.wait_send()
    early_copy.wait_send()
    place_copy.wait_send()
    wait_bytes(packed, near_send.at[0])
    if groups > 2:
        wait_bytes(told.at[pl.ds(0, groups - 1)], told_sems.at[0])
    wait_bytes(landed.at[pl.ds(0, near_slots - last_slots)], near_pair_sems.at[0])

    @pl.when(has_onward)
    def _():
        wait_bytes(landed.at[pl.ds(0, far_slots)], far_send.at[0])

    @pl.when(has_far)
    def _():
        wait_bytes(close.at[pl.ds(2, 2)], close_sems.at[0, 1])
        wait_bytes(landed.at[pl.ds(0, far_slots)], far_pair_sems.at[0])

    for k in range(rounds):
        @pl.when(above_there[k])
        def _():
            scan_copy(k, 0).wait_send()

        @pl.when(below_there[k])
        def _():
            scan_copy(k, 1).wait_send()


def put_kernel(tiles_ref, offsets_ref, tiles_out, offsets_out, sems):
    copies = [
        pltpu.make_async_copy(tiles_ref, tiles_out, sems.at[0]),
        pltpu.make_async_copy(offsets_ref, offsets_out, sems.at[1]),
    ]
    for copy in copies:
        copy.start()
    for copy in copies:
        copy.wait()


def pair_sum_kernel(pairs, own, part_ref, landed, send_sems, recv_sems):
    row = lax.axis_index("rows")
    group = lax.axis_index("inner")
    core = lax.rem(group, 2)
    barrier = pltpu.get_barrier_semaphore()

    def place(ahead):
        return (row, 2 * lax.rem(group // 2 + ahead, pairs) + core)

    for ahead in range(1, pairs):
        pl.semaphore_signal(barrier, inc=1, device_id=place(ahead), device_id_type=MESH)
    pl.semaphore_wait(barrier, pairs - 1)
    copies = []
    for ahead in range(1, pairs):
        copy = pltpu.make_async_remote_copy(
            src_ref=part_ref.at[pl.ds(ahead * own, own)],
            dst_ref=landed.at[ahead - 1],
            send_sem=send_sems.at[ahead - 1],
            recv_sem=recv_sems.at[ahead - 1],
            device_id=place(ahead),
            device_id_type=MESH,
        )
        copy.start()
        copies.append(copy)
    for copy in copies:
        copy.wait()


def fused_body(rows, groups, r_tiles, r_cols, a_tiles, a_cols, c_cols, c_counts):
    local_rows, op_slots, tile, _ = a_tiles.shape
    row_count, r_slots = r_tiles.shape[:2]
    cap = c_cols.shape[1]
    tiles = local_rows * op_slots
    pairs = groups // 2
    own_cap = cap // groups
    half_cap = cap // 2
    width = -(-2 * tiles // 128) * 128
    chunks = []
    for size in [CHUNK] * (PASS_SLOTS // CHUNK) + list(LAST_CHUNKS):
        chunks.append((sum(before for _, before in chunks), size))
    list_slots = sum(size for _, size in chunks)
    pass_slots = PASS_SLOTS
    dims = (
        rows, groups, local_rows, op_slots, r_slots, cap, width, list_slots, pass_slots, tuple(chunks)
    )
    near_chunks = len(chunks)
    far_chunks = PASS_SLOTS // CHUNK
    early = min(EARLY, op_slots)
    near_slots = early + list_slots
    far_slots = early + pass_slots
    rounds = (rows - 1).bit_length()
    dtype = a_tiles.dtype
    out_dtype = jnp.bfloat16 if pairs == 1 else jnp.float32
    own = row_count * own_cap
    vmem = pl.BlockSpec(memory_space=pltpu.VMEM)
    anywhere = pl.BlockSpec(memory_space=pl.ANY)
    dma = pltpu.SemaphoreType.DMA
    block = (row_count, 128)
    part, offsets, flag = pl.pallas_call(
        functools.partial(fused_kernel, dims),
        out_shape=(
            jax.ShapeDtypeStruct((pairs * own, tile, tile), out_dtype),
            jax.ShapeDtypeStruct((1, row_count), jnp.int32),
            jax.ShapeDtypeStruct((1, 128), jnp.int32),
        ),
        in_specs=[anywhere] * 6,
        out_specs=(vmem, vmem, anywhere),
        scratch_shapes=[
            pltpu.VMEM((1, 128), jnp.int32),
            pltpu.VMEM(r_cols.shape, jnp.int32),
            pltpu.VMEM(c_cols.shape, jnp.int32),
            pltpu.VMEM((1, row_count), jnp.int32),
            pltpu.VMEM((op_slots, a_cols.shape[0]), jnp.int32),
            pltpu.VMEM(block, jnp.int32),
            pltpu.VMEM((5,) + block, jnp.int32),
            pltpu.VMEM((2, 8, width), jnp.int32),
            pltpu.VMEM((2 * tiles + 1, tile, tile), dtype),
            pltpu.VMEM((2 * row_count * r_slots, tile, tile), dtype),
            pltpu.VMEM((list_slots, tile, tile), dtype),
            pltpu.VMEM((2 * (near_slots + far_slots) + 1, tile, tile), dtype),
            pltpu.VMEM((row_count * half_cap, tile, tile), jnp.float32),
            pltpu.VMEM((3 * row_count, width), jnp.int32),
            pltpu.SMEM((3 * row_count, width), jnp.int32),
            pltpu.SMEM((8, width), jnp.int32),
            pltpu.VMEM((groups, 8, 128), jnp.int32),
            pltpu.VMEM((rounds, 8, 128), jnp.int32),
            pltpu.VMEM((rounds, 2, 8, 128), jnp.int32),
            dma((6,)),
            dma((2, 3)),
            dma((2, 2)),
            dma((2,)),
            dma((2,)),
            dma((near_chunks,)),
            dma((1,)),
            dma((2,)),
            dma((far_chunks + 1,)),
            dma((1,)),
            dma((2,)),
            dma((2,)),
            dma((2,)),
            dma((2, rounds, 2)),
        ],
        compiler_params=pltpu.CompilerParams(collective_id=40, has_side_effects=True),
        name="fused",
    )(
        r_cols,
        c_cols,
        c_counts[None, :],
        a_cols.T,
        a_tiles.reshape(tiles, tile, tile),
        r_tiles.reshape(row_count * r_slots, tile, tile),
    )
    if pairs == 1:
        c_tiles = part
    else:
        landed = pl.pallas_call(
            functools.partial(pair_sum_kernel, pairs, own),
            out_shape=jax.ShapeDtypeStruct((pairs - 1, own, tile, tile), jnp.float32),
            in_specs=[anywhere],
            out_specs=anywhere,
            scratch_shapes=[dma((pairs - 1,)), dma((pairs - 1,))],
            compiler_params=pltpu.CompilerParams(collective_id=41, has_side_effects=True),
            name="pair_sums",
        )(part)
        c_tiles = part[:own]
        for ahead in range(pairs - 1):
            c_tiles = c_tiles + landed[ahead]
        c_tiles = c_tiles.astype(jnp.bfloat16)
    return c_tiles.reshape(row_count, own_cap, tile, tile), offsets[0], flag[0, 0]


def body(rows, groups, *args):
    if rows % 2 or groups % 2:
        return plain_body(rows, groups, *args)
    c_tiles, offsets, flag = fused_body(rows, groups, *args)

    def again(c_tiles, offsets, *args):
        return plain_body(rows, groups, *args)

    def keep(c_tiles, offsets, *args):
        return c_tiles, offsets

    c_tiles, offsets = lax.cond(flag > 0, again, keep, c_tiles, offsets, *args)
    vmem = pl.BlockSpec(memory_space=pltpu.VMEM)
    anywhere = pl.BlockSpec(memory_space=pl.ANY)
    c_tiles, offsets = pl.pallas_call(
        put_kernel,
        out_shape=(
            jax.ShapeDtypeStruct(c_tiles.shape, c_tiles.dtype),
            jax.ShapeDtypeStruct((1,) + offsets.shape, offsets.dtype),
        ),
        in_specs=[vmem, vmem],
        out_specs=(anywhere, anywhere),
        scratch_shapes=[pltpu.SemaphoreType.DMA((2,))],
        name="put",
    )(c_tiles, offsets[None, :])
    return c_tiles, offsets[0]


def solution(mesh):
    rows = mesh.shape["rows"]
    groups = mesh.shape["inner"]
    return jax.shard_map(
        functools.partial(body, rows, groups),
        mesh=mesh,
        in_specs=(
            P("rows", "inner", None, None),
            P("rows", "inner"),
            P(("rows", "inner"), None, None, None),
            P(),
            P("rows", None),
            P("rows"),
        ),
        out_specs=(P("rows", "inner", None, None), P("rows")),
        check_vma=False,
    )
```
